16 devices in a mesh: dp: 2 (over z), tp: 8 (over y, x, core).
Axes of the slice: x: 2, y: 2, z: 2, core: 2. Of those that a mesh axis runs over, the one named last changes fastest.
Arguments:
- y_one: float32 [16, 256, 1280], P('dp'), parts along dimension 0
- y_two: float32 [16, 256, 1280], P('dp'), parts along dimension 0
- dy_one: float32 [16, 256, 1280], P('dp'), parts along dimension 0
- dy_two: float32 [16, 256, 1280], P('dp'), parts along dimension 0
- saved_one: float32 [1, 16, 256, 1280], P(None, 'dp'), parts along dimension 1
- saved_two: float32 [1, 16, 256, 1280], P(None, 'dp'), parts along dimension 1
- w_qkv: bfloat16 [3, 1280, 3, 16, 80], P(None, None, None, 'tp')
- w_o: bfloat16 [3, 16, 80, 1280], P(None, 'tp')
- w_in: bfloat16 [3, 1280, 5120], P(None, None, 'tp')
- w_out: bfloat16 [3, 5120, 1280], P(None, 'tp')
Outputs:
- output 1: float32 [16, 256, 1280], P('dp'), parts along dimension 0
- output 2: float32 [16, 256, 1280], P('dp'), parts along dimension 0
- output 3: float32 [16, 256, 1280], P('dp'), parts along dimension 0
- output 4: float32 [16, 256, 1280], P('dp'), parts along dimension 0
- output 5: float32 [6, 1280, 3, 16, 80], P('dp', None, None, 'tp'), parts along dimension 0
- output 6: float32 [6, 16, 80, 1280], P('dp', 'tp'), parts along dimension 0
- output 7: float32 [6, 1280, 5120], P('dp', None, 'tp'), parts along dimension 0
- output 8: float32 [6, 5120, 1280], P('dp', 'tp'), parts along dimension 0
There are 2 independent parts. The reference program is written for one: setup_inputs(seed, part) draws one part's arguments, and reference() takes and returns one part's arrays. A program takes and returns all parts, laid end to end along the dimension named above; an argument that names none is the same for every part.
All inputs are finite; a program needn't handle non-finite values.
Results may differ from the reference program's by a relative error of at most 0.0121767.
Values are sent between devices in bfloat16 or wider.
A program may use at most 1 GiB of HBM per device.

```python
import jax
import jax.numpy as jnp
from jax import lax

SEQS = 8
SEQ = 256
HIDDEN = 1280
HEADS = 16
FF = 5120
PAIRS = 1

LAYERS = 2 * PAIRS + 1
HEAD = HIDDEN // HEADS
EPS = 1e-6


def setup_inputs(seed: int = 0, part: int = 0) -> dict:
    base_keys = jax.random.split(jax.random.key(seed), 2)
    act_keys = jax.random.split(jax.random.fold_in(base_keys[0], part), 6)
    w_keys = jax.random.split(base_keys[1], 4)
    state_shape = (SEQS, SEQ, HIDDEN)
    saved_shape = (PAIRS, SEQS, SEQ, HIDDEN)
    qk_gain = jnp.array([2.0 ** 0.5, 2.0 ** 0.5, 1.0], jnp.float32).reshape(1, 1, 3, 1, 1)
    wo_gain = 0.3 * (SEQ / 55.0) ** 0.5
    w_qkv = jax.random.normal(w_keys[0], (LAYERS, HIDDEN, 3, HEADS, HEAD), jnp.float32) * (HIDDEN ** -0.5) * qk_gain
    w_o = jax.random.normal(w_keys[1], (LAYERS, HEADS, HEAD, HIDDEN), jnp.float32) * (HIDDEN ** -0.5 * wo_gain)
    w_in = jax.random.normal(w_keys[2], (LAYERS, HIDDEN, FF), jnp.float32) * (HIDDEN ** -0.5)
    w_out = jax.random.normal(w_keys[3], (LAYERS, FF, HIDDEN), jnp.float32) * (0.45 * FF ** -0.5)
    return {
        "y_one": jax.random.normal(act_keys[0], state_shape, jnp.float32),
        "y_two": jax.random.normal(act_keys[1], state_shape, jnp.float32),
        "dy_one": jax.random.normal(act_keys[2], state_shape, jnp.float32),
        "dy_two": jax.random.normal(act_keys[3], state_shape, jnp.float32),
        "saved_one": jax.random.normal(act_keys[4], saved_shape, jnp.float32),
        "saved_two": jax.random.normal(act_keys[5], saved_shape, jnp.float32),
        "w_qkv": w_qkv.astype(jnp.bfloat16),
        "w_o": w_o.astype(jnp.bfloat16),
        "w_in": w_in.astype(jnp.bfloat16),
        "w_out": w_out.astype(jnp.bfloat16),
    }


def rms_norm(state):
    return state * lax.rsqrt(jnp.mean(state * state, axis=-1, keepdims=True) + EPS)


def to_bf(values):
    return values.astype(jnp.bfloat16).astype(jnp.float32)


def attend_one(qkv_one):
    q_one, k_one, v_one = qkv_one
    scores = jnp.einsum("qne,kne->nqk", q_one, k_one) * HEAD ** -0.5
    attn_probs = jax.nn.softmax(scores, axis=-1)
    return jnp.einsum("nqk,kne->qne", to_bf(attn_probs), v_one)


def branch_f(state, w_qkv, w_o):
    normed = to_bf(rms_norm(state))
    qkv_all = to_bf(jnp.einsum("bsh,hkne->kbsne", normed, w_qkv))
    heads_out = lax.map(jax.checkpoint(attend_one), (qkv_all[0], qkv_all[1], qkv_all[2]))
    return jnp.einsum("bsne,neh->bsh", to_bf(heads_out), w_o)


def branch_g(state, w_in, w_out):
    normed = to_bf(rms_norm(state))
    hidden = jnp.einsum("bsh,hf->bsf", normed, w_in)
    return jnp.einsum("bsf,fh->bsh", to_bf(jax.nn.gelu(hidden, approximate=True)), w_out)


def reversible_back(block_w, y_one, y_two, d_one, d_two):
    w_qkv, w_o, w_in, w_out = block_w
    g_val, g_pull = jax.vjp(branch_g, y_one, w_in, w_out)
    x_two = y_two - g_val
    g_dx, g_win, g_wout = g_pull(d_two)
    d_one = d_one + g_dx
    f_val, f_pull = jax.vjp(branch_f, x_two, w_qkv, w_o)
    x_one = y_one - f_val
    f_dx, f_wqkv, f_wo = f_pull(d_one)
    return x_one, x_two, d_one, d_two + f_dx, (f_wqkv, f_wo, g_win, g_wout)


def plain_back(block_w, x_one, x_two, d_one, d_two):
    w_qkv, w_o, w_in, w_out = block_w
    f_pull = jax.vjp(branch_f, x_two, w_qkv, w_o)[1]
    f_dx, f_wqkv, f_wo = f_pull(d_one)
    g_pull = jax.vjp(branch_g, x_one, w_in, w_out)[1]
    g_dx, g_win, g_wout = g_pull(d_two)
    return d_one + g_dx, d_two + f_dx, (f_wqkv, f_wo, g_win, g_wout)


def reference(y_one, y_two, dy_one, dy_two, saved_one, saved_two, w_qkv, w_o, w_in, w_out):
    weights = tuple(weight.astype(jnp.float32) for weight in (w_qkv, w_o, w_in, w_out))
    top_w = tuple(weight[LAYERS - 1] for weight in weights)
    x_one, x_two, d_one, d_two, top_grads = reversible_back(top_w, y_one, y_two, dy_one, dy_two)
    paired = tuple(weight[: 2 * PAIRS].reshape((PAIRS, 2) + weight.shape[1:]) for weight in weights)
    rev_w = tuple(weight[:, 0] for weight in paired)
    plain_w = tuple(weight[:, 1] for weight in paired)

    def pair_step(carry_in, scan_in):
        rev_block_w, plain_block_w, s_one, s_two = scan_in
        d_mid_one, d_mid_two, plain_grads = plain_back(plain_block_w, s_one, s_two, carry_in[2], carry_in[3])
        carry_out = reversible_back(rev_block_w, s_one, s_two, d_mid_one, d_mid_two)
        return carry_out[:4], (carry_out[4], plain_grads)

    final_state, scan_grads = lax.scan(pair_step, (x_one, x_two, d_one, d_two), (rev_w, plain_w, saved_one, saved_two), reverse=True)
    grad_out = tuple(
        jnp.concatenate([jnp.stack([rev_g, plain_g], axis=1).reshape((2 * PAIRS,) + rev_g.shape[1:]), top_g[None]], axis=0)
        for rev_g, plain_g, top_g in zip(scan_grads[0], scan_grads[1], top_grads)
    )
    return (final_state[0], final_state[1], final_state[2], final_state[3], grad_out[0], grad_out[1], grad_out[2], grad_out[3])
```

```python
import jax
import jax.numpy as jnp
from jax import lax
from jax.sharding import PartitionSpec as P

EPS = 1e-6
BF = jnp.bfloat16
F32 = jnp.float32


def rms_norm(state):
    return state * lax.rsqrt(jnp.mean(state * state, axis=-1, keepdims=True) + EPS)


def rms_vjp(state, cot):
    rinv = lax.rsqrt(jnp.mean(state * state, axis=-1, keepdims=True) + EPS)
    normed = state * rinv
    return rinv * (cot - normed * jnp.mean(cot * normed, axis=-1, keepdims=True))


def gelu_tanh(hidden):
    return jax.nn.gelu(hidden, approximate=True)


def mm(spec, left, right):
    return jnp.einsum(spec, left, right, preferred_element_type=F32)


def attn_forward(normed, w_qkv):
    head_dim = w_qkv.shape[-1]
    qkv_all = mm("bsh,hkne->kbsne", normed, w_qkv).astype(BF)
    scores = mm("bqne,bkne->bnqk", qkv_all[0], qkv_all[1]) * head_dim ** -0.5
    attn_probs = jax.nn.softmax(scores, axis=-1)
    probs_bf = attn_probs.astype(BF)
    heads_out = mm("bnqk,bkne->bqne", probs_bf, qkv_all[2]).astype(BF)
    return qkv_all, attn_probs, probs_bf, heads_out


def attn_backward(normed, w_qkv, w_o, attn_cache, d_bf):
    qkv_all, attn_probs, probs_bf, heads_out = attn_cache
    head_dim = w_qkv.shape[-1]
    d_wo = mm("bqne,bqh->neh", heads_out, d_bf)
    d_heads = mm("bqh,neh->bqne", d_bf, w_o).astype(BF)
    d_v = mm("bnqk,bqne->bkne", probs_bf, d_heads)
    d_probs = mm("bqne,bkne->bnqk", d_heads, qkv_all[2])
    d_scores = attn_probs * (d_probs - jnp.sum(d_probs * attn_probs, axis=-1, keepdims=True)) * head_dim ** -0.5
    ds_bf = d_scores.astype(BF)
    d_q = mm("bnqk,bkne->bqne", ds_bf, qkv_all[1])
    d_k = mm("bnqk,bqne->bkne", ds_bf, qkv_all[0])
    d_qkv = jnp.stack([d_q.astype(BF), d_k.astype(BF), d_v.astype(BF)], axis=2)
    d_wqkv = mm("bsh,bskne->hkne", normed, d_qkv)
    d_normed = mm("bskne,hkne->bsh", d_qkv, w_qkv)
    return d_normed, d_wqkv, d_wo


def mlp_forward(normed, w_in):
    hidden = mm("bsh,hf->bsf", normed, w_in)
    gelu_out, gelu_pull = jax.vjp(gelu_tanh, hidden)
    return gelu_out.astype(BF), gelu_pull


def mlp_backward(normed, w_in, w_out, act_bf, gelu_pull, d_bf):
    d_wout = mm("bsf,bsh->fh", act_bf, d_bf)
    d_act = mm("bsh,fh->bsf", d_bf, w_out)
    d_hidden = gelu_pull(d_act)[0].astype(BF)
    d_win = mm("bsh,bsf->hf", normed, d_hidden)
    d_normed = mm("bsf,hf->bsh", d_hidden, w_in)
    return d_normed, d_win, d_wout


def scatter_sum(part):
    return lax.psum_scatter(part, "tp", scatter_dimension=0, tiled=True)


def gather(shard):
    return lax.all_gather(shard, "tp", axis=0, tiled=True)


def solution(mesh):
    act_spec = P("dp", None, None)
    saved_spec = P(None, "dp", None, None)
    weight_specs = (P(None, None, None, "tp", None), P(None, "tp", None, None), P(None, None, "tp"), P(None, "tp", None))
    grad_specs = (P("dp", None, None, "tp", None), P("dp", "tp", None, None), P("dp", None, "tp"), P("dp", "tp", None))
    n_tp = mesh.shape["tp"]

    def per_device(y_one, y_two, dy_one, dy_two, saved_one, saved_two, w_qkv, w_o, w_in, w_out):
        rank = lax.axis_index("tp")
        rows = y_one.shape[0] // n_tp

        def shard(full):
            return lax.dynamic_slice_in_dim(full, rank * rows, rows, axis=0)

        n_layers = w_qkv.shape[0]
        grads = [None] * n_layers
        top = n_layers - 1
        in_bf = rms_norm(y_one).astype(BF)
        act_bf, pull = mlp_forward(in_bf, w_in[top])
        g_sum = scatter_sum(mm("bsf,fh->bsh", act_bf, w_out[top]))
        x_two = shard(y_two) - g_sum
        f_in = gather(rms_norm(x_two).astype(BF))
        g_back, d_win, d_wout = mlp_backward(in_bf, w_in[top], w_out[top], act_bf, pull, dy_two.astype(BF))
        d_one = shard(dy_one) + rms_vjp(shard(y_one), scatter_sum(g_back.astype(BF)).astype(F32))
        d_one_bf = gather(d_one.astype(BF))
        cache = attn_forward(f_in, w_qkv[top])
        f_back, d_wqkv, d_wo = attn_backward(f_in, w_qkv[top], w_o[top], cache, d_one_bf)
        d_two = shard(dy_two) + rms_vjp(x_two, scatter_sum(f_back.astype(BF)).astype(F32))
        d_two_bf = gather(d_two.astype(BF))
        grads[top] = (d_wqkv, d_wo, d_win, d_wout)
        for pair_idx in reversed(range(saved_one.shape[0])):
            s_one, s_two = saved_one[pair_idx], saved_two[pair_idx]
            hi, lo = 2 * pair_idx + 1, 2 * pair_idx
            s1_bf = rms_norm(s_one).astype(BF)
            s2_bf = rms_norm(s_two).astype(BF)
            cache = attn_forward(s2_bf, w_qkv[hi])
            f_back, d_wqkv, d_wo = attn_backward(s2_bf, w_qkv[hi], w_o[hi], cache, d_one_bf)
            act_bf, pull = mlp_forward(s1_bf, w_in[hi])
            g_back_hi, d_win, d_wout = mlp_backward(s1_bf, w_in[hi], w_out[hi], act_bf, pull, d_two_bf)
            grads[hi] = (d_wqkv, d_wo, d_win, d_wout)
            d_two = d_two + rms_vjp(shard(s_two), scatter_sum(f_back.astype(BF)).astype(F32))
            d_two_bf = gather(d_two.astype(BF))
            act_bf, pull = mlp_forward(s1_bf, w_in[lo])
            g_sum = scatter_sum(mm("bsf,fh->bsh", act_bf, w_out[lo]))
            x_two = shard(s_two) - g_sum
            x_two_full = gather(x_two)
            f_in = rms_norm(x_two_full).astype(BF)
            g_back, d_win, d_wout = mlp_backward(s1_bf, w_in[lo], w_out[lo], act_bf, pull, d_two_bf)
            d_one = d_one + rms_vjp(shard(s_one), scatter_sum((g_back + g_back_hi).astype(BF)).astype(F32))
            d_one_bf = gather(d_one.astype(BF))
            cache = attn_forward(f_in, w_qkv[lo])
            if pair_idx == 0:
                heads_all = lax.all_gather(cache[3], "tp", axis=0, tiled=False)
                wo_all = lax.all_gather(w_o[lo], "tp", axis=0, tiled=False)
                x_one_full = s_one - mm("dbqne,dneh->bqh", heads_all, wo_all)
            f_back, d_wqkv, d_wo = attn_backward(f_in, w_qkv[lo], w_o[lo], cache, d_one_bf)
            d_two = d_two + rms_vjp(x_two, scatter_sum(f_back.astype(BF)).astype(F32))
            grads[lo] = (d_wqkv, d_wo, d_win, d_wout)
            if pair_idx:
                d_two_bf = gather(d_two.astype(BF))
        stacked = tuple(jnp.stack([entry[slot] for entry in grads]) for slot in range(4))
        return (x_one_full, x_two_full, gather(d_one), gather(d_two)) + stacked

    return jax.shard_map(
        per_device,
        mesh=mesh,
        in_specs=(act_spec,) * 4 + (saved_spec,) * 2 + weight_specs,
        out_specs=(act_spec,) * 4 + grad_specs,
        check_vma=False,
    )
```

```python
import jax
import jax.numpy as jnp
from jax import lax
from jax.sharding import PartitionSpec as P

EPS = 1e-6
BF = jnp.bfloat16
F32 = jnp.float32


def rms_norm(state):
    return state * lax.rsqrt(jnp.mean(state * state, axis=-1, keepdims=True) + EPS)


def rms_vjp(state, cot):
    rinv = lax.rsqrt(jnp.mean(state * state, axis=-1, keepdims=True) + EPS)
    normed = state * rinv
    return rinv * (cot - normed * jnp.mean(cot * normed, axis=-1, keepdims=True))


def gelu_tanh(hidden):
    return jax.nn.gelu(hidden, approximate=True)


def mm(spec, left, right):
    return jnp.einsum(spec, left, right, preferred_element_type=F32)


def attn_forward(normed, w_qkv):
    head_dim = w_qkv.shape[-1]
    qkv_all = mm("bsh,hkne->kbsne", normed, w_qkv).astype(BF)
    scores = mm("bqne,bkne->bnqk", qkv_all[0], qkv_all[1]) * head_dim ** -0.5
    attn_probs = jax.nn.softmax(scores, axis=-1)
    probs_bf = attn_probs.astype(BF)
    heads_out = mm("bnqk,bkne->bqne", probs_bf, qkv_all[2]).astype(BF)
    return qkv_all, attn_probs, probs_bf, heads_out


def attn_backward(normed, w_qkv, w_o, attn_cache, d_bf):
    qkv_all, attn_probs, probs_bf, heads_out = attn_cache
    head_dim = w_qkv.shape[-1]
    d_wo = mm("bqne,bqh->neh", heads_out, d_bf)
    d_heads = mm("bqh,neh->bqne", d_bf, w_o).astype(BF)
    d_v = mm("bnqk,bqne->bkne", probs_bf, d_heads)
    d_probs = mm("bqne,bkne->bnqk", d_heads, qkv_all[2])
    d_scores = attn_probs * (d_probs - jnp.sum(d_probs * attn_probs, axis=-1, keepdims=True)) * head_dim ** -0.5
    ds_bf = d_scores.astype(BF)
    d_q = mm("bnqk,bkne->bqne", ds_bf, qkv_all[1])
    d_k = mm("bnqk,bqne->bkne", ds_bf, qkv_all[0])
    d_qkv = jnp.stack([d_q.astype(BF), d_k.astype(BF), d_v.astype(BF)], axis=2)
    d_wqkv = mm("bsh,bskne->hkne", normed, d_qkv)
    d_normed = mm("bskne,hkne->bsh", d_qkv, w_qkv)
    return d_normed, d_wqkv, d_wo


def mlp_forward(normed, w_in):
    hidden = mm("bsh,hf->bsf", normed, w_in)
    gelu_out, gelu_pull = jax.vjp(gelu_tanh, hidden)
    return gelu_out.astype(BF), gelu_pull


def mlp_backward(normed, w_in, w_out, act_bf, gelu_pull, d_bf):
    d_wout = mm("bsf,bsh->fh", act_bf, d_bf)
    d_act = mm("bsh,fh->bsf", d_bf, w_out)
    d_hidden = gelu_pull(d_act)[0].astype(BF)
    d_win = mm("bsh,bsf->hf", normed, d_hidden)
    d_normed = mm("bsf,hf->bsh", d_hidden, w_in)
    return d_normed, d_win, d_wout


def flip_pairs(n_tp, bit):
    return [(idx, idx ^ bit) for idx in range(n_tp)]


def scatter_sum(part):
    n_tp = part.shape[0]
    rank = lax.axis_index("tp")
    core, x_pos, y_pos = rank % 2, (rank // 2) % 2, rank // 4
    width = part.shape[-1] // 2
    halves = []
    for half in range(2):
        cols = part[..., half * width:(half + 1) * width].reshape(2, 2, 2, part.shape[1], width)
        sent = lax.dynamic_index_in_dim(cols, 1 - core, axis=2, keepdims=False)
        kept = lax.dynamic_index_in_dim(cols, core, axis=2, keepdims=False)
        summed = kept + lax.ppermute(sent, "tp", flip_pairs(n_tp, 1))
        order = ((1, x_pos, 2), (0, y_pos, 4)) if half == 0 else ((0, y_pos, 4), (0, x_pos, 2))
        for axis, pos, bit in order:
            sent = lax.dynamic_index_in_dim(summed, 1 - pos, axis=axis, keepdims=False)
            kept = lax.dynamic_index_in_dim(summed, pos, axis=axis, keepdims=False)
            summed = kept + lax.ppermute(sent, "tp", flip_pairs(n_tp, bit))
        halves.append(summed)
    return jnp.concatenate(halves, axis=-1)[None]


def gather(shard):
    return lax.all_gather(shard, "tp", axis=0, tiled=True)


def solution(mesh):
    act_spec = P("dp", None, None)
    saved_spec = P(None, "dp", None, None)
    weight_specs = (P(None, None, None, "tp", None), P(None, "tp", None, None), P(None, None, "tp"), P(None, "tp", None))
    grad_specs = (P("dp", None, None, "tp", None), P("dp", "tp", None, None), P("dp", None, "tp"), P("dp", "tp", None))
    n_tp = mesh.shape["tp"]

    def per_device(y_one, y_two, dy_one, dy_two, saved_one, saved_two, w_qkv, w_o, w_in, w_out):
        rank = lax.axis_index("tp")
        rows = y_one.shape[0] // n_tp

        def shard(full):
            return lax.dynamic_slice_in_dim(full, rank * rows, rows, axis=0)

        n_layers = w_qkv.shape[0]
        grads = [None] * n_layers
        top = n_layers - 1
        in_bf = rms_norm(y_one).astype(BF)
        act_bf, pull = mlp_forward(in_bf, w_in[top])
        g_sum = scatter_sum(mm("bsf,fh->bsh", act_bf, w_out[top]))
        x_two = shard(y_two) - g_sum
        f_in = gather(rms_norm(x_two).astype(BF))
        g_back, d_win, d_wout = mlp_backward(in_bf, w_in[top], w_out[top], act_bf, pull, dy_two.astype(BF))
        d_one = shard(dy_one) + rms_vjp(shard(y_one), scatter_sum(g_back.astype(BF)).astype(F32))
        d_one_bf = gather(d_one.astype(BF))
        cache = attn_forward(f_in, w_qkv[top])
        f_back, d_wqkv, d_wo = attn_backward(f_in, w_qkv[top], w_o[top], cache, d_one_bf)
        d_two = shard(dy_two) + rms_vjp(x_two, scatter_sum(f_back.astype(BF)).astype(F32))
        d_two_bf = gather(d_two.astype(BF))
        grads[top] = (d_wqkv, d_wo, d_win, d_wout)
        for pair_idx in reversed(range(saved_one.shape[0])):
            s_one, s_two = saved_one[pair_idx], saved_two[pair_idx]
            hi, lo = 2 * pair_idx + 1, 2 * pair_idx
            s1_bf = rms_norm(s_one).astype(BF)
            s2_bf = rms_norm(s_two).astype(BF)
            cache = attn_forward(s2_bf, w_qkv[hi])
            f_back, d_wqkv, d_wo = attn_backward(s2_bf, w_qkv[hi], w_o[hi], cache, d_one_bf)
            act_bf, pull = mlp_forward(s1_bf, w_in[hi])
            g_back_hi, d_win, d_wout = mlp_backward(s1_bf, w_in[hi], w_out[hi], act_bf, pull, d_two_bf)
            grads[hi] = (d_wqkv, d_wo, d_win, d_wout)
            d_two = d_two + rms_vjp(shard(s_two), scatter_sum(f_back.astype(BF)).astype(F32))
            d_two_bf = gather(d_two.astype(BF))
            act_bf, pull = mlp_forward(s1_bf, w_in[lo])
            g_sum = scatter_sum(mm("bsf,fh->bsh", act_bf, w_out[lo]))
            x_two = shard(s_two) - g_sum
            x_two_full = gather(x_two)
            f_in = rms_norm(x_two_full).astype(BF)
            g_back, d_win, d_wout = mlp_backward(s1_bf, w_in[lo], w_out[lo], act_bf, pull, d_two_bf)
            d_one = d_one + rms_vjp(shard(s_one), scatter_sum((g_back + g_back_hi).astype(BF)).astype(F32))
            d_one_bf = gather(d_one.astype(BF))
            cache = attn_forward(f_in, w_qkv[lo])
            if pair_idx == 0:
                heads_all = lax.all_gather(cache[3], "tp", axis=0, tiled=False)
                wo_all = lax.all_gather(w_o[lo], "tp", axis=0, tiled=False)
                x_one_full = s_one - mm("dbqne,dneh->bqh", heads_all, wo_all)
            f_back, d_wqkv, d_wo = attn_backward(f_in, w_qkv[lo], w_o[lo], cache, d_one_bf)
            d_two = d_two + rms_vjp(x_two, scatter_sum(f_back.astype(BF)).astype(F32))
            grads[lo] = (d_wqkv, d_wo, d_win, d_wout)
            if pair_idx:
                d_two_bf = gather(d_two.astype(BF))
        stacked = tuple(jnp.stack([entry[slot] for entry in grads]) for slot in range(4))
        return (x_one_full, x_two_full, gather(d_one), gather(d_two)) + stacked

    return jax.shard_map(
        per_device,
        mesh=mesh,
        in_specs=(act_spec,) * 4 + (saved_spec,) * 2 + weight_specs,
        out_specs=(act_spec,) * 4 + grad_specs,
        check_vma=False,
    )
```

```python
import functools

import jax
import jax.numpy as jnp
from jax import lax
from jax.experimental import pallas as pl
from jax.experimental.pallas import tpu as pltpu
from jax.sharding import PartitionSpec as P

EPS = 1e-6
BF = jnp.bfloat16
F32 = jnp.float32
GELU_C = 0.7978845608028654
GELU_A = 0.044715


def rms_norm(state):
    return state * lax.rsqrt(jnp.mean(state * state, axis=-1, keepdims=True) + EPS)


def rms_vjp(state, cot):
    rinv = lax.rsqrt(jnp.mean(state * state, axis=-1, keepdims=True) + EPS)
    normed = state * rinv
    return rinv * (cot - normed * jnp.mean(cot * normed, axis=-1, keepdims=True))


def dot(left, right, dims=((1,), (0,))):
    return lax.dot_general(left, right, (dims, ((), ())), preferred_element_type=F32)


def dot_nt(left, right):
    return dot(left, right, ((1,), (1,)))


def dot_tn(left, right):
    return dot(left, right, ((0,), (0,)))


def gelu_val(hid):
    return hid * (0.5 * (1.0 + jnp.tanh(GELU_C * (hid + GELU_A * (hid * hid * hid)))))


def gelu_grad(hid):
    sq = hid * hid
    th = jnp.tanh(GELU_C * (hid + GELU_A * (sq * hid)))
    return 0.5 * (1.0 + th) + hid * (0.5 * (1.0 - th * th)) * (GELU_C * (1.0 + 3.0 * GELU_A * sq))


def seq_index(step, rank):
    return (2 * (step % 4) + 1 - step // 4) ^ rank


def seq_call(body, rank, ins, outs, parts, flops, name):
    def spec(kind, shape):
        if kind == "row":
            return pl.BlockSpec((1,) + tuple(shape[1:]), lambda g, rk: (seq_index(g, rk[0]), 0, 0))
        if kind == "col":
            return pl.BlockSpec((shape[0], shape[1] // 8), lambda g, rk: (0, seq_index(g, rk[0])))
        return pl.BlockSpec(tuple(shape), lambda g, rk: (0,) * len(shape))

    in_specs = [spec(kind, arr.shape) for kind, arr in ins]
    out_specs = [spec(kind, shape) for kind, shape, _ in outs]
    out_shape = [jax.ShapeDtypeStruct(shape, dtype) for _, shape, dtype in outs]
    for rows, width, dtype in parts:
        block = (1, rows, width // 2)
        for first in (True, False):
            for _ in range(2):
                if first:
                    out_specs.append(pl.BlockSpec(block, lambda g, rk: (jnp.minimum(g, 3), 0, 0)))
                else:
                    out_specs.append(pl.BlockSpec(block, lambda g, rk: (jnp.maximum(g - 4, 0), 0, 0)))
                out_shape.append(jax.ShapeDtypeStruct((4, rows, width // 2), dtype))
    n_in, n_out = len(ins), len(outs)

    def kernel(rank_ref, *refs):
        step = pl.program_id(0)
        in_refs, out_refs, part_refs = refs[:n_in], refs[n_in:n_in + n_out], refs[n_in + n_out:]
        for value in body(in_refs, out_refs):
            send_l, send_r, keep_l, keep_r = part_refs[:4]
            part_refs = part_refs[4:]
            half = value.shape[-1] // 2

            @pl.when(step < 4)
            def _():
                send_l[0] = value[:, :half].astype(send_l.dtype)
                send_r[0] = value[:, half:].astype(send_r.dtype)

            @pl.when(step >= 4)
            def _():
                keep_l[0] = value[:, :half].astype(keep_l.dtype)
                keep_r[0] = value[:, half:].astype(keep_r.dtype)

    nbytes = sum(arr.size * arr.dtype.itemsize for _, arr in ins) + sum(o.size * o.dtype.itemsize for o in out_shape)
    return pl.pallas_call(
        kernel,
        grid_spec=pltpu.PrefetchScalarGridSpec(
            num_scalar_prefetch=1, grid=(8,), in_specs=in_specs, out_specs=out_specs
        ),
        out_shape=out_shape,
        compiler_params=pltpu.CompilerParams(dimension_semantics=("arbitrary",), vmem_limit_bytes=56 * 1024 * 1024),
        cost_estimate=pl.CostEstimate(flops=flops, bytes_accessed=nbytes, transcendentals=0),
        name=name,
    )(rank, *[arr for _, arr in ins])


def mlp_top(rank, x, w_in, w_out, d):
    seqs, rows, width = x.shape
    inner = w_in.shape[1]

    def body(in_refs, out_refs):
        x_ref, win_ref, wout_ref, d_ref = in_refs
        a_ref, act_ref, dh_ref, dbf_ref = out_refs
        a = rms_norm(x_ref[0]).astype(BF)
        a_ref[0] = a
        d_bf = d_ref[0].astype(BF)
        dbf_ref[0] = d_bf
        hid = dot(a, win_ref[...])
        act_ref[0] = gelu_val(hid).astype(BF)
        dh = (dot_nt(d_bf, wout_ref[...]) * gelu_grad(hid)).astype(BF)
        dh_ref[0] = dh
        yield dot_nt(dh, win_ref[...])

    outs = [("row", (seqs, rows, width), BF), ("row", (seqs, rows, inner), BF), ("row", (seqs, rows, inner), BF), ("row", (seqs, rows, width), BF)]
    return seq_call(
        body, rank, [("row", x), ("all", w_in), ("all", w_out), ("row", d)], outs, [(rows, width, BF)], 6 * seqs * rows * width * inner, "mlp_top"
    )


def mlp_out(rank, act, w_out):
    seqs, rows, inner = act.shape

    def body(in_refs, out_refs):
        yield dot(in_refs[0][0], in_refs[1][...])

    return seq_call(body, rank, [("row", act), ("all", w_out)], [], [(rows, w_out.shape[1], F32)], 2 * act.size * w_out.shape[1], "mlp_out")


def mlp_pair_fwd(rank, x, w_hi, w_lo):
    seqs, rows, width = x.shape
    inner = w_hi.shape[1]

    def body(in_refs, out_refs):
        x_ref, whi_ref, wlo_ref = in_refs
        a_ref, hhi_ref, acthi_ref, hlo_ref, actlo_ref = out_refs
        a = rms_norm(x_ref[0]).astype(BF)
        a_ref[0] = a
        for w_ref, h_ref, act_ref in ((wlo_ref, hlo_ref, actlo_ref), (whi_ref, hhi_ref, acthi_ref)):
            hid = dot(a, w_ref[...])
            h_ref[0] = hid
            act_ref[0] = gelu_val(hid).astype(BF)
        return ()

    mid = (seqs, rows, inner)
    outs = [("row", x.shape, BF), ("row", mid, F32), ("row", mid, BF), ("row", mid, F32), ("row", mid, BF)]
    return seq_call(body, rank, [("row", x), ("all", w_hi), ("all", w_lo)], outs, [], 4 * seqs * rows * width * inner, "mlp_pair_fwd")


def mlp_dhid(rank, d, w_out, hid):
    seqs, rows, width = d.shape
    inner = w_out.shape[0]

    def body(in_refs, out_refs):
        d_ref, w_ref, h_ref = in_refs
        out_refs[0][0] = (dot_nt(d_ref[0], w_ref[...]) * gelu_grad(h_ref[0])).astype(BF)
        return ()

    return seq_call(
        body, rank, [("row", d), ("all", w_out), ("row", hid)], [("row", hid.shape, BF)], [], 2 * seqs * rows * width * inner, "mlp_dhid"
    )[0]


def mlp_pair_back(rank, d, w_out, hid, dh_hi, w_hi, w_lo):
    seqs, rows, width = d.shape
    inner = w_out.shape[0]

    def body(in_refs, out_refs):
        d_ref, w_ref, h_ref, dhhi_ref, whi_ref, wlo_ref = in_refs
        dh = (dot_nt(d_ref[0], w_ref[...]) * gelu_grad(h_ref[0])).astype(BF)
        out_refs[0][0] = dh
        yield dot_nt(dhhi_ref[0], whi_ref[...]) + dot_nt(dh, wlo_ref[...])

    return seq_call(
        body,
        rank,
        [("row", d), ("all", w_out), ("row", hid), ("row", dh_hi), ("all", w_hi), ("all", w_lo)],
        [("row", hid.shape, BF)],
        [(rows, width, BF)],
        6 * seqs * rows * width * inner,
        "mlp_pair_back",
    )


def attn(rank, head_dim, w_qkv, w_o, x=None, norm=False, qkv=None, d=None):
    seqs, rows, width = (x if x is not None else d).shape
    cols, inner = w_qkv.shape[0], w_o.shape[0]
    heads = inner // head_dim
    scale = head_dim ** -0.5
    forward, backward = x is not None, d is not None
    ins, outs = [("all", w_qkv)], []
    if forward:
        ins.append(("row", x))
        if norm:
            outs.append(("row", x.shape, BF))
        outs.append(("col", (inner, seqs * rows), BF))
        if not backward:
            outs.append(("col", (cols, seqs * rows), BF))
    else:
        ins.append(("col", qkv))
    if backward:
        ins += [("all", w_o), ("row", d)]
        outs.append(("col", (cols, seqs * rows), BF))

    def body(in_refs, out_refs):
        in_refs, out_refs = list(in_refs), list(out_refs)
        wqkv_ref = in_refs.pop(0)
        if forward:
            x_ref = in_refs.pop(0)
            if norm:
                a = rms_norm(x_ref[0]).astype(BF)
                out_refs.pop(0)[0] = a
            else:
                a = x_ref[0]
            o_ref = out_refs.pop(0)
            qkv_t = dot_nt(wqkv_ref[...], a).astype(BF)
            if not backward:
                out_refs.pop(0)[...] = qkv_t
        else:
            qkv_t = in_refs.pop(0)[...]
        if backward:
            wo_ref, d_ref = in_refs
            dqkv_ref = out_refs.pop(0)
            dheads = dot_nt(wo_ref[...], d_ref[0]).astype(BF)
        pieces = [[], [], []]
        for n in range(heads):
            lo = n * head_dim
            q_t, k_t, v_t = (qkv_t[part * inner + lo:part * inner + lo + head_dim] for part in range(3))
            scores = dot_tn(k_t, q_t) * scale
            expd = jnp.exp(scores - jnp.max(scores, axis=0, keepdims=True))
            probs = expd / jnp.sum(expd, axis=0, keepdims=True)
            probs_bf = probs.astype(BF)
            if forward:
                o_ref[pl.ds(lo, head_dim), :] = dot(v_t, probs_bf).astype(BF)
            if backward:
                dhead = dheads[lo:lo + head_dim]
                d_v = dot_nt(dhead, probs_bf)
                d_probs = dot_tn(v_t, dhead)
                d_scores = (probs * (d_probs - jnp.sum(d_probs * probs, axis=0, keepdims=True)) * scale).astype(BF)
                for part, piece in enumerate((dot(k_t, d_scores), dot_nt(q_t, d_scores), d_v)):
                    pieces[part].append(piece.astype(BF))
        if backward:
            dqkv = jnp.concatenate(pieces[0] + pieces[1] + pieces[2], axis=0)
            dqkv_ref[...] = dqkv
            yield dot_tn(dqkv, wqkv_ref[...])

    flops = 2 * seqs * rows * (width * (cols * (forward + backward) + inner * backward) + rows * inner * (2 * forward + 5 * backward))
    return seq_call(body, rank, ins, outs, [(rows, width, BF)] if backward else [], flops, "attn_" + "f" * forward + "b" * backward)


def weight_grad(stack, layers, layer, left, right, transposed, name):
    tokens, n_cols = right.shape
    n_rows = left.shape[0] if transposed else left.shape[1]
    tile = 512

    def kernel(left_ref, right_ref, *refs):
        out_ref = refs[-1]
        prod = (dot if transposed else dot_tn)(left_ref[...], right_ref[...])

        @pl.when(pl.program_id(0) == 0)
        def _():
            out_ref[0] = prod

        @pl.when(pl.program_id(0) > 0)
        def _():
            out_ref[0] += prod

    in_specs = [
        pl.BlockSpec((n_rows, tile), lambda k: (0, k)) if transposed else pl.BlockSpec((tile, n_rows), lambda k: (k, 0)),
        pl.BlockSpec((tile, n_cols), lambda k: (k, 0)),
    ]
    args = [left, right]
    if stack is not None:
        in_specs.append(pl.BlockSpec(memory_space=pl.ANY))
        args.append(stack)
    return pl.pallas_call(
        kernel,
        grid=(tokens // tile,),
        in_specs=in_specs,
        out_specs=pl.BlockSpec((1, n_rows, n_cols), lambda k: (layer, 0, 0)),
        out_shape=jax.ShapeDtypeStruct((layers, n_rows, n_cols), F32),
        input_output_aliases={2: 0} if stack is not None else {},
        compiler_params=pltpu.CompilerParams(dimension_semantics=("arbitrary",), vmem_limit_bytes=56 * 1024 * 1024),
        cost_estimate=pl.CostEstimate(
            flops=2 * tokens * n_rows * n_cols, bytes_accessed=2 * tokens * (n_rows + n_cols) + 4 * n_rows * n_cols, transcendentals=0
        ),
        name=name,
    )(*args)


def permute(array, bit):
    return lax.ppermute(array, "tp", [(idx, idx ^ bit) for idx in range(8)])


def scatter_sum(parts):
    halves = []
    for send, keep, order in ((parts[0], parts[2], (2, 4)), (parts[1], parts[3], (4, 2))):
        summed = keep + permute(send, 1)
        summed = summed.reshape((2, 2) + summed.shape[1:])
        away, here = (summed[:, 1], summed[:, 0]) if order[0] == 2 else (summed[1], summed[0])
        summed = here + permute(away, order[0])
        halves.append(summed[0].astype(F32) + permute(summed[1], order[1]).astype(F32))
    return jnp.concatenate(halves, axis=-1)[None]


def gather(shard):
    return lax.all_gather(shard, "tp", axis=0, tiled=True)


def solution(mesh):
    act_spec = P("dp", None, None)
    saved_spec = P(None, "dp", None, None)
    weight_specs = (P(None, None, None, "tp", None), P(None, "tp", None, None), P(None, None, "tp"), P(None, "tp", None))
    grad_specs = (P("dp", None, None, "tp", None), P("dp", "tp", None, None), P("dp", None, "tp"), P("dp", "tp", None))

    def per_device(y_one, y_two, dy_one, dy_two, saved_one, saved_two, w_qkv, w_o, w_in, w_out):
        index = lax.axis_index("tp")
        rank = index.astype(jnp.int32).reshape((1,))
        n_layers, width, _, n_heads, head_dim = w_qkv.shape
        tokens = y_one.shape[0] * y_one.shape[1]
        qkv_w = w_qkv.transpose(0, 2, 3, 4, 1).reshape(n_layers, 3 * n_heads * head_dim, width)
        o_w = w_o.reshape(n_layers, n_heads * head_dim, width)

        def shard(full):
            return lax.dynamic_slice_in_dim(full, index, 1, axis=0)

        def flat(full):
            return full.reshape(tokens, full.shape[-1])

        stacks = [None] * 4

        def attn_grads(layer, a, o_t, dqkv_t, d_bf):
            stacks[0] = weight_grad(stacks[0], n_layers, layer, dqkv_t, flat(a), True, "dw_qkv")
            stacks[1] = weight_grad(stacks[1], n_layers, layer, o_t, flat(d_bf), True, "dw_o")

        def mlp_grads(layer, a, act, dh, d_bf):
            stacks[2] = weight_grad(stacks[2], n_layers, layer, flat(a), flat(dh), False, "dw_in")
            stacks[3] = weight_grad(stacks[3], n_layers, layer, flat(act), flat(d_bf), False, "dw_out")

        top = n_layers - 1
        g_a, g_act, g_dh, d_two_bf, *g_back = mlp_top(rank, y_one, w_in[top], w_out[top], dy_two)
        d_one = shard(dy_one) + rms_vjp(shard(y_one), scatter_sum(g_back))
        d_one_bf = gather(d_one.astype(BF))
        x_two = shard(y_two) - scatter_sum(mlp_out(rank, g_act, w_out[top]))
        f_a = gather(rms_norm(x_two).astype(BF))
        mlp_grads(top, g_a, g_act, g_dh, d_two_bf)
        o_t, dqkv_t, *f_back = attn(rank, head_dim, qkv_w[top], o_w[top], x=f_a, d=d_one_bf)
        attn_grads(top, f_a, o_t, dqkv_t, d_one_bf)
        d_two = shard(dy_two) + rms_vjp(x_two, scatter_sum(f_back))
        for pair_idx in reversed(range(saved_one.shape[0])):
            s_one, s_two = saved_one[pair_idx], saved_two[pair_idx]
            hi, lo = 2 * pair_idx + 1, 2 * pair_idx
            f_a, o_t, dqkv_t, *f_back = attn(rank, head_dim, qkv_w[hi], o_w[hi], x=s_two, norm=True, d=d_one_bf)
            attn_grads(hi, f_a, o_t, dqkv_t, d_one_bf)
            g_a, h_hi, act_hi, h_lo, act_lo = mlp_pair_fwd(rank, s_one, w_in[hi], w_in[lo])
            x_two = shard(s_two) - scatter_sum(mlp_out(rank, act_lo, w_out[lo]))
            x_two_full = gather(x_two)
            d_two_bf = gather(d_two.astype(BF))
            dh_hi = mlp_dhid(rank, d_two_bf, w_out[hi], h_hi)
            mlp_grads(hi, g_a, act_hi, dh_hi, d_two_bf)
            d_two = d_two + rms_vjp(shard(s_two), scatter_sum(f_back))
            d_two_bf = gather(d_two.astype(BF))
            dh_lo, *g_back = mlp_pair_back(rank, d_two_bf, w_out[lo], h_lo, dh_hi, w_in[hi], w_in[lo])
            mlp_grads(lo, g_a, act_lo, dh_lo, d_two_bf)
            d_one = d_one + rms_vjp(shard(s_one), scatter_sum(g_back))
            d_one_bf = gather(d_one.astype(BF))
            f_a, o_t, qkv_t = attn(rank, head_dim, qkv_w[lo], o_w[lo], x=x_two_full, norm=True)
            if pair_idx == 0:
                o_all = gather(o_t)
                wo_all = gather(o_w[lo])
                x_one_full = s_one - lax.dot_general(o_all, wo_all, (((0,), (0,)), ((), ())), preferred_element_type=F32).reshape(s_one.shape)
            dqkv_t, *f_back = attn(rank, head_dim, qkv_w[lo], o_w[lo], qkv=qkv_t, d=d_one_bf)
            attn_grads(lo, f_a, o_t, dqkv_t, d_one_bf)
            d_two = d_two + rms_vjp(x_two, scatter_sum(f_back))
        grad_qkv = stacks[0].reshape(n_layers, 3, n_heads, head_dim, width).transpose(0, 4, 1, 2, 3)
        grad_o = stacks[1].reshape(w_o.shape)
        return (x_one_full, x_two_full, gather(d_one), gather(d_two), grad_qkv, grad_o, stacks[2], stacks[3])

    return jax.shard_map(
        per_device,
        mesh=mesh,
        in_specs=(act_spec,) * 4 + (saved_spec,) * 2 + weight_specs,
        out_specs=(act_spec,) * 4 + grad_specs,
        check_vma=False,
    )
```

```python
import jax
import jax.numpy as jnp
from jax import lax
from jax.experimental import pallas as pl
from jax.experimental.pallas import tpu as pltpu
from jax.sharding import PartitionSpec as P

EPS = 1e-6
BF = jnp.bfloat16
F32 = jnp.float32
GELU_C = 0.7978845608028654
GELU_A = 0.044715


def rms_norm(state):
    return state * lax.rsqrt(jnp.mean(state * state, axis=-1, keepdims=True) + EPS)


def rms_vjp(state, cot):
    rinv = lax.rsqrt(jnp.mean(state * state, axis=-1, keepdims=True) + EPS)
    normed = state * rinv
    return rinv * (cot - normed * jnp.mean(cot * normed, axis=-1, keepdims=True))


def dot(left, right, dims=((1,), (0,))):
    return lax.dot_general(left, right, (dims, ((), ())), preferred_element_type=F32)


def dot_nt(left, right):
    return dot(left, right, ((1,), (1,)))


def dot_tn(left, right):
    return dot(left, right, ((0,), (0,)))


def gelu_val(hid):
    return hid * (0.5 * (1.0 + jnp.tanh(GELU_C * (hid + GELU_A * (hid * hid * hid)))))


def gelu_grad(hid):
    sq = hid * hid
    th = jnp.tanh(GELU_C * (hid + GELU_A * (sq * hid)))
    return 0.5 * (1.0 + th) + hid * (0.5 * (1.0 - th * th)) * (GELU_C * (1.0 + 3.0 * GELU_A * sq))


MIB = 1024 * 1024


def seq_call(body, rank, ins, outs, parts, flops, name, after=()):
    n_in, n_out = len(ins), len(outs)
    seqs = 8

    def run(parity, previous, after):
        steps = seqs if parity is None else seqs // 2

        def seq(g, rk):
            return g if parity is None else (2 * g + parity) ^ rk[0]

        def spec(kind, shape, layer=0):
            if kind == "row":
                return pl.BlockSpec((None,) + tuple(shape[1:]), lambda g, rk: (seq(g, rk), 0, 0))
            if kind == "col":
                return pl.BlockSpec((shape[0], shape[1] // seqs), lambda g, rk: (0, seq(g, rk)))
            if kind == "layer":
                return pl.BlockSpec((None,) + tuple(shape[1:]), lambda g, rk: (layer, 0, 0))
            return pl.BlockSpec(tuple(shape), lambda g, rk: (0,) * len(shape))

        hidden = list(previous) + list(after)
        in_specs = [spec(kind, arr.shape, *layer) for kind, arr, *layer in ins] + [pl.BlockSpec(memory_space=pl.ANY)] * len(hidden)
        out_specs = [spec(kind, shape) for kind, shape, _ in outs]
        out_shape = [jax.ShapeDtypeStruct(shape, dtype) for _, shape, dtype in outs]
        for rows, width, dtype in parts:
            for _ in range(2):
                out_specs.append(pl.BlockSpec((None, rows, width // 2), lambda g, rk: (g, 0, 0)))
                out_shape.append(jax.ShapeDtypeStruct((steps, rows, width // 2), dtype))

        out_specs.append(pl.BlockSpec((8, 128), lambda g, rk: (0, 0)))
        out_shape.append(jax.ShapeDtypeStruct((8, 128), F32))

        def kernel(rank_ref, *refs):
            refs[-1][...] = jnp.zeros((8, 128), F32)
            in_refs = refs[:n_in]
            out_refs = refs[n_in + len(hidden):n_in + len(hidden) + n_out]
            part_refs = refs[n_in + len(hidden) + n_out:]
            for index, value in enumerate(body(in_refs, out_refs)):
                left, right = part_refs[2 * index:2 * index + 2]
                half = value.shape[-1] // 2
                left[...] = value[:, :half].astype(left.dtype)
                right[...] = value[:, half:].astype(right.dtype)

        vmem = 0
        for block, dtype in [(sp.block_shape, arr.dtype) for sp, (_, arr, *_) in zip(in_specs, ins)] + [
            (sp.block_shape, o.dtype) for sp, o in zip(out_specs, out_shape)
        ]:
            count = 1
            for dim in block:
                count *= dim or 1
            vmem += 2 * count * jnp.dtype(dtype).itemsize
        share = 1 if parity is None else 2
        nbytes = sum(o.size * o.dtype.itemsize for o in out_shape) // share
        return pl.pallas_call(
            kernel,
            grid_spec=pltpu.PrefetchScalarGridSpec(
                num_scalar_prefetch=1, grid=(steps,), in_specs=in_specs, out_specs=out_specs
            ),
            out_shape=out_shape,
            input_output_aliases={1 + n_in + index: index for index in range(len(previous))},
            compiler_params=pltpu.CompilerParams(dimension_semantics=("arbitrary",), vmem_limit_bytes=min(vmem + 14 * MIB, 60 * MIB)),
            cost_estimate=pl.CostEstimate(flops=flops // share, bytes_accessed=nbytes, transcendentals=0),
            name=name,
        )(rank, *[arr for _, arr, *_ in ins], *hidden)

    if not parts:
        return list(run(None, (), after))
    sent = list(run(1, (), after))
    kept = list(run(0, sent[:n_out], [sent[-1]]))
    return kept[:n_out] + [sent[n_out], sent[n_out + 1], kept[n_out], kept[n_out + 1], kept[-1]]


def mlp_top(rank, x, w_in, w_out, layer, d):
    seqs, rows, width = x.shape
    inner = w_in.shape[2]

    def body(in_refs, out_refs):
        x_ref, win_ref, wout_ref, d_ref = in_refs
        a_ref, act_ref, dh_ref, dbf_ref = out_refs
        a = rms_norm(x_ref[...]).astype(BF)
        a_ref[...] = a
        d_bf = d_ref[...].astype(BF)
        dbf_ref[...] = d_bf
        hid = dot(a, win_ref[...])
        act_ref[...] = gelu_val(hid).astype(BF)
        dh = (dot_nt(d_bf, wout_ref[...]) * gelu_grad(hid)).astype(BF)
        dh_ref[...] = dh
        yield dot_nt(dh, win_ref[...])

    outs = [("row", (seqs, rows, width), BF), ("row", (seqs, rows, inner), BF), ("row", (seqs, rows, inner), BF), ("row", (seqs, rows, width), BF)]
    ins = [("row", x), ("layer", w_in, layer), ("layer", w_out, layer), ("row", d)]
    return seq_call(body, rank, ins, outs, [(rows, width, BF)], 6 * seqs * rows * width * inner, "mlp_top")


def mlp_out(rank, act, w_out, layer, after=()):
    rows, width = act.shape[1], w_out.shape[2]

    def body(in_refs, out_refs):
        yield dot(in_refs[0][...], in_refs[1][...])

    return seq_call(body, rank, [("row", act), ("layer", w_out, layer)], [], [(rows, width, F32)], 2 * act.size * width, "mlp_out", after)


def mlp_pair_fwd(rank, x, w_in, hi, lo, after=()):
    seqs, rows, width = x.shape
    inner = w_in.shape[2]

    def body(in_refs, out_refs):
        x_ref, whi_ref, wlo_ref = in_refs
        a_ref, hhi_ref, acthi_ref, hlo_ref, actlo_ref = out_refs
        a = rms_norm(x_ref[...]).astype(BF)
        a_ref[...] = a
        for w_ref, h_ref, act_ref in ((wlo_ref, hlo_ref, actlo_ref), (whi_ref, hhi_ref, acthi_ref)):
            hid = dot(a, w_ref[...])
            h_ref[...] = hid
            act_ref[...] = gelu_val(hid).astype(BF)
        return ()

    mid = (seqs, rows, inner)
    outs = [("row", x.shape, BF), ("row", mid, F32), ("row", mid, BF), ("row", mid, F32), ("row", mid, BF)]
    ins = [("row", x), ("layer", w_in, hi), ("layer", w_in, lo)]
    return seq_call(body, rank, ins, outs, [], 4 * seqs * rows * width * inner, "mlp_pair_fwd", after)


def mlp_dhid(rank, d, w_out, layer, hid, after=()):
    seqs, rows, width = d.shape
    inner = w_out.shape[1]

    def body(in_refs, out_refs):
        d_ref, w_ref, h_ref = in_refs
        out_refs[0][...] = (dot_nt(d_ref[...], w_ref[...]) * gelu_grad(h_ref[...])).astype(BF)
        return ()

    ins = [("row", d), ("layer", w_out, layer), ("row", hid)]
    return seq_call(body, rank, ins, [("row", hid.shape, BF)], [], 2 * seqs * rows * width * inner, "mlp_dhid", after)


def mlp_pair_back(rank, d, w_out, hid, dh_hi, w_in, hi, lo, after=()):
    seqs, rows, width = d.shape
    inner = w_out.shape[1]

    def body(in_refs, out_refs):
        d_ref, w_ref, h_ref, dhhi_ref, whi_ref, wlo_ref = in_refs
        dh = (dot_nt(d_ref[...], w_ref[...]) * gelu_grad(h_ref[...])).astype(BF)
        out_refs[0][...] = dh
        yield dot_nt(dhhi_ref[...], whi_ref[...]) + dot_nt(dh, wlo_ref[...])

    ins = [("row", d), ("layer", w_out, lo), ("row", hid), ("row", dh_hi), ("layer", w_in, hi), ("layer", w_in, lo)]
    return seq_call(body, rank, ins, [("row", hid.shape, BF)], [(rows, width, BF)], 6 * seqs * rows * width * inner, "mlp_pair_back", after)


def attn(rank, head_dim, w_qkv, w_o, layer, x=None, minus=None, norm=False, qkv=None, d=None, after=()):
    seqs, rows, width = (x if x is not None else d).shape
    cols, inner = w_qkv.shape[1], w_o.shape[1]
    heads = inner // head_dim
    scale = head_dim ** -0.5
    forward, backward = x is not None, d is not None
    ins, outs = [("layer", w_qkv, layer)], []
    if forward:
        ins.append(("row", x))
        if minus is not None:
            ins.append(("row", minus))
            outs.append(("row", x.shape, F32))
        if norm:
            outs.append(("row", x.shape, BF))
        outs.append(("col", (inner, seqs * rows), BF))
        if not backward:
            outs.append(("col", (cols, seqs * rows), BF))
    else:
        ins.append(("col", qkv))
    if backward:
        ins += [("layer", w_o, layer), ("row", d)]
        outs.append(("col", (cols, seqs * rows), BF))

    def body(in_refs, out_refs):
        in_refs, out_refs = list(in_refs), list(out_refs)
        wqkv_ref = in_refs.pop(0)
        if forward:
            value = in_refs.pop(0)[...]
            if minus is not None:
                value = value - in_refs.pop(0)[...]
                out_refs.pop(0)[...] = value
            if norm:
                value = rms_norm(value).astype(BF)
                out_refs.pop(0)[...] = value
            o_ref = out_refs.pop(0)
            qkv_t = dot_nt(wqkv_ref[...], value).astype(BF)
            if not backward:
                out_refs.pop(0)[...] = qkv_t
        else:
            qkv_t = in_refs.pop(0)[...]
        if backward:
            wo_ref, d_ref = in_refs
            dqkv_ref = out_refs.pop(0)
            dheads = dot_nt(wo_ref[...], d_ref[...]).astype(BF)
        pieces = [[], [], []]
        for n in range(heads):
            lo = n * head_dim
            q_t, k_t, v_t = (qkv_t[part * inner + lo:part * inner + lo + head_dim] for part in range(3))
            scores = dot_tn(k_t, q_t) * scale
            expd = jnp.exp(scores - jnp.max(scores, axis=0, keepdims=True))
            probs = expd / jnp.sum(expd, axis=0, keepdims=True)
            probs_bf = probs.astype(BF)
            if forward:
                o_ref[pl.ds(lo, head_dim), :] = dot(v_t, probs_bf).astype(BF)
            if backward:
                dhead = dheads[lo:lo + head_dim]
                d_v = dot_nt(dhead, probs_bf)
                d_probs = dot_tn(v_t, dhead)
                d_scores = (probs * (d_probs - jnp.sum(d_probs * probs, axis=0, keepdims=True)) * scale).astype(BF)
                for part, piece in enumerate((dot(k_t, d_scores), dot_nt(q_t, d_scores), d_v)):
                    pieces[part].append(piece.astype(BF))
        if backward:
            dqkv = jnp.concatenate(pieces[0] + pieces[1] + pieces[2], axis=0)
            dqkv_ref[...] = dqkv
            yield dot_tn(dqkv, wqkv_ref[...])

    flops = 2 * seqs * rows * (width * (cols * (forward + backward) + inner * backward) + rows * inner * (2 * forward + 5 * backward))
    return seq_call(body, rank, ins, outs, [(rows, width, BF)] if backward else [], flops, "attn_" + "f" * forward + "b" * backward, after)


def attn_value(rank, base, o_all, wo_all, after=()):
    def body(in_refs, out_refs):
        base_ref, o_ref, w_ref = in_refs
        out_refs[0][...] = base_ref[...] - dot_tn(o_ref[...], w_ref[...])
        return ()

    ins = [("row", base), ("col", o_all), ("all", wo_all)]
    return seq_call(body, rank, ins, [("row", base.shape, F32)], [], 2 * base.size * wo_all.shape[0], "attn_value", after)


def weight_grads(stacks, layers, layer, jobs, name, after=()):
    steps = 5
    in_specs, out_specs, out_shape, args, flops, vmem = [], [], [], [], 0, 0
    for left, right, split in jobs:
        tokens, n_cols = right.shape
        if split == "rows":
            n_rows = left.shape[1]
            in_specs.append(pl.BlockSpec((tokens, n_rows // steps), lambda g: (0, g)))
            in_specs.append(pl.BlockSpec((tokens, n_cols), lambda g: (0, 0)))
            out_specs.append(pl.BlockSpec((None, n_rows // steps, n_cols), lambda g: (layer, g, 0)))
        else:
            n_rows = left.shape[0]
            in_specs.append(pl.BlockSpec((n_rows, tokens), lambda g: (0, 0)))
            in_specs.append(pl.BlockSpec((tokens, n_cols // steps), lambda g: (0, g)))
            out_specs.append(pl.BlockSpec((None, n_rows, n_cols // steps), lambda g: (layer, 0, g)))
        out_shape.append(jax.ShapeDtypeStruct((layers, n_rows, n_cols), F32))
        args += [left, right]
        flops += 2 * tokens * n_rows * n_cols
        vmem += 4 * (left.size + right.size) + 2 * n_rows * n_cols
    n_jobs = len(jobs)
    aliases = {}
    if stacks[0] is not None:
        aliases = {len(args) + index: index for index in range(n_jobs)}
        args += stacks
    args += list(after)
    in_specs += [pl.BlockSpec(memory_space=pl.ANY)] * (len(args) - 2 * n_jobs)
    out_specs.append(pl.BlockSpec((8, 128), lambda g: (0, 0)))
    out_shape.append(jax.ShapeDtypeStruct((8, 128), F32))

    def kernel(*refs):
        outs = refs[len(args):]
        for index, (_, _, split) in enumerate(jobs):
            left_ref, right_ref = refs[2 * index:2 * index + 2]
            outs[index][...] = (dot_tn if split == "rows" else dot)(left_ref[...], right_ref[...])
        outs[-1][...] = jnp.zeros((8, 128), F32)

    *stacks, token = pl.pallas_call(
        kernel,
        grid=(steps,),
        in_specs=in_specs,
        out_specs=out_specs,
        out_shape=out_shape,
        input_output_aliases=aliases,
        compiler_params=pltpu.CompilerParams(dimension_semantics=("arbitrary",), vmem_limit_bytes=min(vmem + 10 * MIB, 60 * MIB)),
        cost_estimate=pl.CostEstimate(flops=flops, bytes_accessed=vmem, transcendentals=0),
        name=name,
    )(*args)
    return stacks, token


def permute(array, bit):
    return lax.ppermute(array, "tp", [(idx, idx ^ bit) for idx in range(8)])


def tie(value, tokens):
    return lax.optimization_barrier((value, *tokens))[0] if tokens else value


def sum_cores(parts):
    halves = []
    for send, keep, order in ((parts[0], parts[2], (2, 4)), (parts[1], parts[3], (4, 2))):
        grid = (2, 2) + keep.shape[1:]
        halves.append((keep.reshape(grid), permute(send, 1).reshape(grid), order))
    return halves


def sum_first(halves, begin=()):
    moving, sent = [], []
    for keep, recv, order in halves:
        recv = tie(recv, begin)
        pick = (lambda arr, pos: arr[:, pos]) if order[0] == 2 else (lambda arr, pos: arr[pos])
        away = pick(keep, 1) + pick(recv, 1)
        sent.append(away)
        moving.append((pick(keep, 0) + pick(recv, 0), permute(away, order[0]), order))
    return moving, sent


def sum_last(moving, fill=(), last=()):
    halves, sent = [], []
    for here, recv, order in moving:
        recv = tie(recv, fill)
        away = here[1] + recv[1]
        sent.append(away)
        final = tie(permute(away, order[1]), last)
        halves.append((here[0] + recv[0]).astype(F32) + final.astype(F32))
    return jnp.concatenate(halves, axis=-1)[None], sent


def gather(shard):
    return lax.all_gather(shard, "tp", axis=0, tiled=True)


def solution(mesh):
    act_spec = P("dp", None, None)
    saved_spec = P(None, "dp", None, None)
    weight_specs = (P(None, None, None, "tp", None), P(None, "tp", None, None), P(None, None, "tp"), P(None, "tp", None))
    grad_specs = (P("dp", None, None, "tp", None), P("dp", "tp", None, None), P("dp", None, "tp"), P("dp", "tp", None))

    def per_device(y_one, y_two, dy_one, dy_two, saved_one, saved_two, w_qkv, w_o, w_in, w_out):
        index = lax.axis_index("tp")
        rank = index.astype(jnp.int32).reshape((1,))
        n_layers, width, _, n_heads, head_dim = w_qkv.shape
        tokens = y_one.shape[0] * y_one.shape[1]
        qkv_w = w_qkv.transpose(0, 2, 3, 4, 1).reshape(n_layers, 3 * n_heads * head_dim, width)
        o_w = w_o.reshape(n_layers, n_heads * head_dim, width)

        def shard(full):
            return lax.dynamic_slice_in_dim(full, index, 1, axis=0)

        def flat(full):
            return full.reshape(tokens, full.shape[-1])

        stacks = {"attn": [None] * 2, "in": [None], "out": [None]}

        def attn_grads(layer, a, o_t, dqkv_t, d_bf, after=()):
            jobs = [(dqkv_t, flat(a), "cols"), (o_t, flat(d_bf), "cols")]
            stacks["attn"], token = weight_grads(stacks["attn"], n_layers, layer, jobs, "dw_attn", after)
            return token

        def mlp_grads(layer, a, act, dh, d_bf, after=()):
            stacks["in"], first = weight_grads(stacks["in"], n_layers, layer, [(flat(a), flat(dh), "rows")], "dw_in", after)
            stacks["out"], second = weight_grads(stacks["out"], n_layers, layer, [(flat(act), flat(d_bf), "rows")], "dw_out", [first])
            return first, second

        top, hi, lo = 2, 1, 0
        s_one, s_two = saved_one[0], saved_two[0]
        wo_all = gather(o_w[lo])
        top_a, top_act, top_dh, d_two_bf, *part_g, tok_top = mlp_top(rank, y_one, w_in, w_out, top, dy_two)
        sum_g, sent = sum_first(sum_cores(part_g))
        *part_out, tok_out = mlp_out(rank, top_act, w_out, top, [tok_top, *sent])
        sum_out = sum_cores(part_out)
        back, _ = sum_last(sum_g, [tok_out] + [recv for _, recv, _ in sum_out])
        d_one = shard(dy_one) + rms_vjp(shard(y_one), back)
        d_one_bf = gather(d_one.astype(BF))
        sum_out, sent = sum_first(sum_out, [back])
        s_a, h_hi, act_hi, h_lo, act_lo, tok_fwd = mlp_pair_fwd(rank, s_one, w_in, hi, lo, [tok_out, *sent])
        tok_in, tok_dw = mlp_grads(top, top_a, top_act, top_dh, d_two_bf, [tok_fwd])
        value, _ = sum_last(sum_out, [tok_in], [tok_dw])
        x_two_top = shard(y_two) - value
        f_top = gather(rms_norm(x_two_top).astype(BF))
        *part_out, tok_out = mlp_out(rank, act_lo, w_out, lo, [tok_dw])
        sum_out, sent = sum_first(sum_cores(part_out), [x_two_top])
        f_hi, o_hi, dqkv_hi, *part_hi, tok_hi = attn(
            rank, head_dim, qkv_w, o_w, hi, x=s_two, norm=True, d=d_one_bf, after=[tok_out, wo_all, *sent]
        )
        sum_hi = sum_cores(part_hi)
        received = [recv for _, recv, _ in sum_hi]
        o_top, dqkv_top, *part_top, tok_top = attn(rank, head_dim, qkv_w, o_w, top, x=f_top, d=d_one_bf, after=[tok_hi, *received])
        g_sum, _ = sum_last(sum_out, [tok_hi], [tok_top])
        sum_top, sent = sum_first(sum_cores(part_top))
        tok_dw_hi = attn_grads(hi, f_hi, o_hi, dqkv_hi, d_one_bf, [tok_top, *sent])
        g_full = gather(g_sum)
        x_two = shard(s_two) - g_sum
        back, sent = sum_last(sum_top, [tok_dw_hi])
        d_two = shard(dy_two) + rms_vjp(x_two_top, back)
        sum_hi, sent_hi = sum_first(sum_hi, sent)
        d_two_hi_bf = gather(tie(d_two, [g_sum]).astype(BF))
        tok_dw_top = attn_grads(top, f_top, o_top, dqkv_top, d_one_bf, [tok_dw_hi, *sent_hi])
        back, _ = sum_last(sum_hi, [tok_dw_top])
        d_two = d_two + rms_vjp(shard(s_two), back)
        d_two_lo_bf = gather(d_two.astype(BF))
        x_two_full, f_lo, o_lo, qkv_lo, tok_f = attn(rank, head_dim, qkv_w, o_w, lo, x=s_two, minus=g_full, norm=True, after=[tok_dw_top])
        o_all = gather(o_lo)
        dh_hi, tok_dh = mlp_dhid(rank, d_two_hi_bf, w_out, hi, h_hi, [tok_f])
        _, tok_dw = mlp_grads(hi, s_a, act_hi, dh_hi, d_two_hi_bf, [tok_dh])
        dh_lo, *part_g, tok_g = mlp_pair_back(rank, d_two_lo_bf, w_out, h_lo, dh_hi, w_in, hi, lo, [tok_dw])
        sum_g, sent = sum_first(sum_cores(part_g))
        tok_in, tok_dw = mlp_grads(lo, s_a, act_lo, dh_lo, d_two_lo_bf, [tok_g, *sent])
        back, _ = sum_last(sum_g, [tok_in])
        d_one = d_one + rms_vjp(shard(s_one), back)
        d_one_bf = gather(tie(d_one.astype(BF), [o_all]))
        x_one_full, tok_x = attn_value(rank, s_one, o_all, wo_all, [tok_dw])
        dqkv_lo, *part_lo, tok_b = attn(rank, head_dim, qkv_w, o_w, lo, qkv=qkv_lo, d=d_one_bf, after=[tok_x])
        sum_lo, sent = sum_first(sum_cores(part_lo))
        tok_dw = attn_grads(lo, f_lo, o_lo, dqkv_lo, d_one_bf, [tok_b, *sent])
        back, _ = sum_last(sum_lo, [tok_dw])
        d_two = d_two + rms_vjp(x_two, back)
        grad_qkv = stacks["attn"][0].reshape(n_layers, 3, n_heads, head_dim, width).transpose(0, 4, 1, 2, 3)
        grad_o = stacks["attn"][1].reshape(w_o.shape)
        return (x_one_full, x_two_full, gather(d_one), gather(d_two), grad_qkv, grad_o, stacks["in"][0], stacks["out"][0])

    return jax.shard_map(
        per_device,
        mesh=mesh,
        in_specs=(act_spec,) * 4 + (saved_spec,) * 2 + weight_specs,
        out_specs=(act_spec,) * 4 + grad_specs,
        check_vma=False,
    )
```

```python
import jax
import jax.numpy as jnp
from jax import lax
from jax.experimental import pallas as pl
from jax.experimental.pallas import tpu as pltpu
from jax.sharding import PartitionSpec as P

EPS = 1e-6
BF = jnp.bfloat16
F32 = jnp.float32
GELU_C = 0.7978845608028654
GELU_A = 0.044715


def rms_norm(state):
    return state * lax.rsqrt(jnp.mean(state * state, axis=-1, keepdims=True) + EPS)


def rms_vjp(state, cot):
    rinv = lax.rsqrt(jnp.mean(state * state, axis=-1, keepdims=True) + EPS)
    normed = state * rinv
    return rinv * (cot - normed * jnp.mean(cot * normed, axis=-1, keepdims=True))


def dot(left, right, dims=((1,), (0,))):
    return lax.dot_general(left, right, (dims, ((), ())), preferred_element_type=F32)


def dot_nt(left, right):
    return dot(left, right, ((1,), (1,)))


def dot_tn(left, right):
    return dot(left, right, ((0,), (0,)))


def gelu_val(hid):
    return hid * (0.5 * (1.0 + jnp.tanh(GELU_C * (hid + GELU_A * (hid * hid * hid)))))


def gelu_grad(hid):
    sq = hid * hid
    th = jnp.tanh(GELU_C * (hid + GELU_A * (sq * hid)))
    return 0.5 * (1.0 + th) + hid * (0.5 * (1.0 - th * th)) * (GELU_C * (1.0 + 3.0 * GELU_A * sq))


MIB = 1024 * 1024


def seq_call(body, rank, ins, outs, parts, flops, after=()):
    n_in, n_out = len(ins), len(outs)
    seqs = 8

    def run(parity, previous, after):
        steps = seqs if parity is None else seqs // 2

        def seq(g, rk):
            return g if parity is None else (2 * g + parity) ^ rk[0]

        def spec(kind, shape, layer=0):
            if kind == "row":
                return pl.BlockSpec((None,) + tuple(shape[1:]), lambda g, rk: (seq(g, rk), 0, 0))
            if kind == "col":
                return pl.BlockSpec((shape[0], shape[1] // seqs), lambda g, rk: (0, seq(g, rk)))
            if kind == "layer":
                return pl.BlockSpec((None,) + tuple(shape[1:]), lambda g, rk: (layer, 0, 0))
            return pl.BlockSpec(tuple(shape), lambda g, rk: (0,) * len(shape))

        hidden = list(previous) + list(after)
        in_specs = [spec(kind, arr.shape, *layer) for kind, arr, *layer in ins] + [pl.BlockSpec(memory_space=pl.ANY)] * len(hidden)
        out_specs = [spec(kind, shape) for kind, shape, _ in outs]
        out_shape = [jax.ShapeDtypeStruct(shape, dtype) for _, shape, dtype in outs]
        for rows, width, dtype in parts:
            for _ in range(2):
                out_specs.append(pl.BlockSpec((None, rows, width // 2), lambda g, rk: (g, 0, 0)))
                out_shape.append(jax.ShapeDtypeStruct((steps, rows, width // 2), dtype))

        out_specs.append(pl.BlockSpec((8, 128), lambda g, rk: (0, 0)))
        out_shape.append(jax.ShapeDtypeStruct((8, 128), F32))

        def kernel(rank_ref, *refs):
            refs[-1][...] = jnp.zeros((8, 128), F32)
            in_refs = refs[:n_in]
            out_refs = refs[n_in + len(hidden):n_in + len(hidden) + n_out]
            part_refs = refs[n_in + len(hidden) + n_out:]
            for index, value in enumerate(body(in_refs, out_refs)):
                left, right = part_refs[2 * index:2 * index + 2]
                half = value.shape[-1] // 2
                left[...] = value[:, :half].astype(left.dtype)
                right[...] = value[:, half:].astype(right.dtype)

        share = 1 if parity is None else 2
        nbytes = sum(o.size * o.dtype.itemsize for o in out_shape) // share
        return pl.pallas_call(
        kernel,
        grid_spec=pltpu.PrefetchScalarGridSpec(
            num_scalar_prefetch=1, grid=(steps,), in_specs=in_specs, out_specs=out_specs
        ),
        out_shape=out_shape,
        input_output_aliases={1 + n_in + index: index for index in range(len(previous))},
        compiler_params=pltpu.CompilerParams(dimension_semantics=("arbitrary",), vmem_limit_bytes=60 * MIB),
        cost_estimate=pl.CostEstimate(flops=flops // share, bytes_accessed=nbytes, transcendentals=0),
        )(rank, *[arr for _, arr, *_ in ins], *hidden)

    if not parts:
        return list(run(None, (), after))
    sent = list(run(1, (), after))
    kept = list(run(0, sent[:n_out], [sent[-1]]))
    return kept[:n_out] + [sent[n_out], sent[n_out + 1], kept[n_out], kept[n_out + 1], kept[-1]]


def mlp_fwd(rank, x, w_in, layer):
    seqs, rows, width = x.shape
    inner = w_in.shape[2]

    def body(in_refs, out_refs):
        x_ref, win_ref = in_refs
        a_ref, h_ref, act_ref = out_refs
        a = rms_norm(x_ref[...]).astype(BF)
        a_ref[...] = a
        hid = dot(a, win_ref[...])
        h_ref[...] = hid
        act_ref[...] = gelu_val(hid).astype(BF)
        return ()

    mid = (seqs, rows, inner)
    outs = [("row", x.shape, BF), ("row", mid, F32), ("row", mid, BF)]
    return seq_call(body, rank, [("row", x), ("layer", w_in, layer)], outs, [], 2 * seqs * rows * width * inner)


def mlp_back(rank, d, w_out, hid, w_in, layer, after=()):
    seqs, rows, width = d.shape
    inner = w_out.shape[1]

    def body(in_refs, out_refs):
        d_ref, wout_ref, h_ref, win_ref = in_refs
        dbf_ref, dh_ref = out_refs
        d_bf = d_ref[...].astype(BF)
        dbf_ref[...] = d_bf
        dh = (dot_nt(d_bf, wout_ref[...]) * gelu_grad(h_ref[...])).astype(BF)
        dh_ref[...] = dh
        yield dot_nt(dh, win_ref[...])

    ins = [("row", d), ("layer", w_out, layer), ("row", hid), ("layer", w_in, layer)]
    outs = [("row", d.shape, BF), ("row", hid.shape, BF)]
    return seq_call(body, rank, ins, outs, [(rows, width, BF)], 4 * seqs * rows * width * inner, after)


def mlp_out(rank, act, w_out, layer, after=()):
    rows, width = act.shape[1], w_out.shape[2]

    def body(in_refs, out_refs):
        yield dot(in_refs[0][...], in_refs[1][...])

    return seq_call(body, rank, [("row", act), ("layer", w_out, layer)], [], [(rows, width, F32)], 2 * act.size * width, after)


def mlp_pair_fwd(rank, x, w_in, hi, lo, after=()):
    seqs, rows, width = x.shape
    inner = w_in.shape[2]

    def body(in_refs, out_refs):
        x_ref, whi_ref, wlo_ref = in_refs
        a_ref, hhi_ref, acthi_ref, hlo_ref, actlo_ref = out_refs
        a = rms_norm(x_ref[...]).astype(BF)
        a_ref[...] = a
        for w_ref, h_ref, act_ref in ((wlo_ref, hlo_ref, actlo_ref), (whi_ref, hhi_ref, acthi_ref)):
            hid = dot(a, w_ref[...])
            h_ref[...] = hid
            act_ref[...] = gelu_val(hid).astype(BF)
        return ()

    mid = (seqs, rows, inner)
    outs = [("row", x.shape, BF), ("row", mid, F32), ("row", mid, BF), ("row", mid, F32), ("row", mid, BF)]
    ins = [("row", x), ("layer", w_in, hi), ("layer", w_in, lo)]
    return seq_call(body, rank, ins, outs, [], 4 * seqs * rows * width * inner, after)


def mlp_dhid(rank, d, w_out, layer, hid, after=()):
    seqs, rows, width = d.shape
    inner = w_out.shape[1]

    def body(in_refs, out_refs):
        d_ref, w_ref, h_ref = in_refs
        out_refs[0][...] = (dot_nt(d_ref[...], w_ref[...]) * gelu_grad(h_ref[...])).astype(BF)
        return ()

    ins = [("row", d), ("layer", w_out, layer), ("row", hid)]
    return seq_call(body, rank, ins, [("row", hid.shape, BF)], [], 2 * seqs * rows * width * inner, after)


def mlp_pair_back(rank, d, w_out, hid, dh_hi, w_in, hi, lo, after=()):
    seqs, rows, width = d.shape
    inner = w_out.shape[1]

    def body(in_refs, out_refs):
        d_ref, w_ref, h_ref, dhhi_ref, whi_ref, wlo_ref = in_refs
        dh = (dot_nt(d_ref[...], w_ref[...]) * gelu_grad(h_ref[...])).astype(BF)
        out_refs[0][...] = dh
        yield dot_nt(dhhi_ref[...], whi_ref[...]) + dot_nt(dh, wlo_ref[...])

    ins = [("row", d), ("layer", w_out, lo), ("row", hid), ("row", dh_hi), ("layer", w_in, hi), ("layer", w_in, lo)]
    return seq_call(body, rank, ins, [("row", hid.shape, BF)], [(rows, width, BF)], 6 * seqs * rows * width * inner, after)


def attn(rank, head_dim, w_qkv, w_o, layer, x=None, minus=None, norm=False, qkv=None, d=None, after=()):
    seqs, rows, width = (x if x is not None else d).shape
    cols, inner = w_qkv.shape[1], w_o.shape[1]
    heads = inner // head_dim
    scale = head_dim ** -0.5
    forward, backward = x is not None, d is not None
    ins, outs = [("layer", w_qkv, layer)], []
    if forward:
        ins.append(("row", x))
        if minus is not None:
            ins.append(("row", minus))
            outs.append(("row", x.shape, F32))
        if norm:
            outs.append(("row", x.shape, BF))
        outs.append(("col", (inner, seqs * rows), BF))
        if not backward:
            outs.append(("col", (cols, seqs * rows), BF))
    else:
        ins.append(("col", qkv))
    if backward:
        ins += [("layer", w_o, layer), ("row", d)]
        outs.append(("col", (cols, seqs * rows), BF))

    def body(in_refs, out_refs):
        in_refs, out_refs = list(in_refs), list(out_refs)
        wqkv_ref = in_refs.pop(0)
        if forward:
            value = in_refs.pop(0)[...]
            if minus is not None:
                value = value - in_refs.pop(0)[...]
                out_refs.pop(0)[...] = value
            if norm:
                value = rms_norm(value).astype(BF)
                out_refs.pop(0)[...] = value
            o_ref = out_refs.pop(0)
            qkv_t = dot_nt(wqkv_ref[...], value).astype(BF)
            if not backward:
                out_refs.pop(0)[...] = qkv_t
        else:
            qkv_t = in_refs.pop(0)[...]
        if backward:
            wo_ref, d_ref = in_refs
            dqkv_ref = out_refs.pop(0)
            dheads = dot_nt(wo_ref[...], d_ref[...]).astype(BF)
        pieces = [[], [], []]
        for n in range(heads):
            lo = n * head_dim
            q_t, k_t, v_t = (qkv_t[part * inner + lo:part * inner + lo + head_dim] for part in range(3))
            scores = dot_tn(k_t, q_t) * scale
            expd = jnp.exp(scores - jnp.max(scores, axis=0, keepdims=True))
            probs = expd / jnp.sum(expd, axis=0, keepdims=True)
            probs_bf = probs.astype(BF)
            if forward:
                o_ref[pl.ds(lo, head_dim), :] = dot(v_t, probs_bf).astype(BF)
            if backward:
                dhead = dheads[lo:lo + head_dim]
                d_v = dot_nt(dhead, probs_bf)
                d_probs = dot_tn(v_t, dhead)
                d_scores = (probs * (d_probs - jnp.sum(d_probs * probs, axis=0, keepdims=True)) * scale).astype(BF)
                for part, piece in enumerate((dot(k_t, d_scores), dot_nt(q_t, d_scores), d_v)):
                    pieces[part].append(piece.astype(BF))
        if backward:
            dqkv = jnp.concatenate(pieces[0] + pieces[1] + pieces[2], axis=0)
            dqkv_ref[...] = dqkv
            yield dot_tn(dqkv, wqkv_ref[...])

    flops = 2 * seqs * rows * (width * (cols * (forward + backward) + inner * backward) + rows * inner * (2 * forward + 5 * backward))
    return seq_call(body, rank, ins, outs, [(rows, width, BF)] if backward else [], flops, after)


def attn_value(rank, base, o_all, wo_all, after=()):
    def body(in_refs, out_refs):
        base_ref, o_ref, w_ref = in_refs
        out_refs[0][...] = base_ref[...] - dot_tn(o_ref[...], w_ref[...])
        return ()

    ins = [("row", base), ("col", o_all), ("all", wo_all)]
    return seq_call(body, rank, ins, [("row", base.shape, F32)], [], 2 * base.size * wo_all.shape[0], after)


def emit(rank, array, after=()):
    def body(in_refs, out_refs):
        out_refs[0][...] = in_refs[0][...]
        return ()

    return seq_call(body, rank, [("row", array)], [("row", array.shape, array.dtype)], [], 16 * array.size, after)


def weight_grads(stacks, layers, layer, jobs, after=()):
    steps = 5
    in_specs, out_specs, out_shape, args, flops, vmem = [], [], [], [], 0, 0
    for left, right, split in jobs:
        tokens, n_cols = right.shape
        if split == "rows":
            n_rows = left.shape[1]
            in_specs.append(pl.BlockSpec((tokens, n_rows // steps), lambda g: (0, g)))
            in_specs.append(pl.BlockSpec((tokens, n_cols), lambda g: (0, 0)))
            out_specs.append(pl.BlockSpec((None, n_rows // steps, n_cols), lambda g: (layer, g, 0)))
        else:
            n_rows = left.shape[0]
            in_specs.append(pl.BlockSpec((n_rows, tokens), lambda g: (0, 0)))
            in_specs.append(pl.BlockSpec((tokens, n_cols // steps), lambda g: (0, g)))
            out_specs.append(pl.BlockSpec((None, n_rows, n_cols // steps), lambda g: (layer, 0, g)))
        out_shape.append(jax.ShapeDtypeStruct((layers, n_rows, n_cols), F32))
        args += [left, right]
        flops += 2 * tokens * n_rows * n_cols
        vmem += 4 * (left.size + right.size) + 2 * n_rows * n_cols
    n_jobs = len(jobs)
    aliases = {}
    if stacks[0] is not None:
        aliases = {len(args) + index: index for index in range(n_jobs)}
        args += stacks
    args += list(after)
    in_specs += [pl.BlockSpec(memory_space=pl.ANY)] * (len(args) - 2 * n_jobs)
    out_specs.append(pl.BlockSpec((8, 128), lambda g: (0, 0)))
    out_shape.append(jax.ShapeDtypeStruct((8, 128), F32))

    def kernel(*refs):
        outs = refs[len(args):]
        for index, (_, _, split) in enumerate(jobs):
            left_ref, right_ref = refs[2 * index:2 * index + 2]
            outs[index][...] = (dot_tn if split == "rows" else dot)(left_ref[...], right_ref[...])
        outs[-1][...] = jnp.zeros((8, 128), F32)

    call = pl.pallas_call(
        kernel,
        grid=(steps,),
        in_specs=in_specs,
        out_specs=out_specs,
        out_shape=out_shape,
        input_output_aliases=aliases,
        compiler_params=pltpu.CompilerParams(dimension_semantics=("arbitrary",), vmem_limit_bytes=60 * MIB),
        cost_estimate=pl.CostEstimate(flops=flops, bytes_accessed=vmem, transcendentals=0),
    )
    *stacks, token = call(*args)
    return stacks, token


def permute(array, bit):
    return lax.ppermute(array, "tp", [(idx, idx ^ bit) for idx in range(8)])


def tie(value, tokens):
    return lax.optimization_barrier((value, *tokens))[0] if tokens else value


def sum_cores(parts):
    halves = []
    for send, keep, order in ((parts[0], parts[2], (2, 4)), (parts[1], parts[3], (4, 2))):
        grid = (2, 2) + keep.shape[1:]
        halves.append((keep.reshape(grid), permute(send, 1).reshape(grid), order))
    return halves


def sum_first(halves, begin=()):
    moving, sent = [], []
    for keep, recv, order in halves:
        recv = tie(recv, begin)
        pick = (lambda arr, pos: arr[:, pos]) if order[0] == 2 else (lambda arr, pos: arr[pos])
        away = pick(keep, 1) + pick(recv, 1)
        sent.append(away)
        moving.append((pick(keep, 0) + pick(recv, 0), permute(away, order[0]), order))
    return moving, sent


def received(halves):
    return [recv for _, recv, _ in halves]


def sum_second(moving, fill=()):
    value, sent, final = [], [], []
    for here, recv, order in moving:
        recv = tie(recv, fill)
        sent.append(here[1] + recv[1])
        value.append(here[0] + recv[0])
        final.append(permute(sent[-1], order[1]))
    return value, sent, final


def sum_end(value, final, fill=()):
    halves = [here.astype(F32) + tie(recv, fill).astype(F32) for here, recv in zip(value, final)]
    return jnp.concatenate(halves, axis=-1)[None]


def gather(shard):
    return lax.all_gather(shard, "tp", axis=0, tiled=True)


def solution(mesh):
    act_spec = P("dp", None, None)
    saved_spec = P(None, "dp", None, None)
    weight_specs = (P(None, None, None, "tp", None), P(None, "tp", None, None), P(None, None, "tp"), P(None, "tp", None))
    grad_specs = (P("dp", None, None, "tp", None), P("dp", "tp", None, None), P("dp", None, "tp"), P("dp", "tp", None))

    def per_device(y_one, y_two, dy_one, dy_two, saved_one, saved_two, w_qkv, w_o, w_in, w_out):
        index = lax.axis_index("tp")
        rank = index.astype(jnp.int32).reshape((1,))
        n_layers, width, _, n_heads, head_dim = w_qkv.shape
        tokens = y_one.shape[0] * y_one.shape[1]
        qkv_w = w_qkv.transpose(0, 2, 3, 4, 1).reshape(n_layers, 3 * n_heads * head_dim, width)
        o_w = w_o.reshape(n_layers, n_heads * head_dim, width)

        def shard(full):
            return lax.dynamic_slice_in_dim(full, index, 1, axis=0)

        def flat(full):
            return full.reshape(tokens, full.shape[-1])

        stacks = {"attn": [None] * 2, "in": [None], "out": [None]}

        def attn_grads(layer, a, o_t, dqkv_t, d_bf, after=()):
            jobs = [(dqkv_t, flat(a), "cols"), (o_t, flat(d_bf), "cols")]
            stacks["attn"], token = weight_grads(stacks["attn"], n_layers, layer, jobs, after)
            return token

        def mlp_grads(layer, a, act, dh, d_bf, after=()):
            stacks["in"], first = weight_grads(stacks["in"], n_layers, layer, [(flat(a), flat(dh), "rows")], after)
            stacks["out"], second = weight_grads(stacks["out"], n_layers, layer, [(flat(act), flat(d_bf), "rows")], [first])
            return first, second

        top, hi, lo = 2, 1, 0
        s_one, s_two = saved_one[0], saved_two[0]
        wo_all = gather(o_w[lo])
        top_a, h_top, top_act, tok = mlp_fwd(rank, y_one, w_in, top)
        *parts, tok = mlp_out(rank, top_act, w_out, top, [tok])
        sum_out, sent = sum_first(sum_cores(parts))
        d_two_bf, top_dh, *parts, tok = mlp_back(rank, dy_two, w_out, h_top, w_in, top, [tok, *sent])
        sum_g = sum_cores(parts)
        s_a, h_hi, act_hi, h_lo, act_lo, tok = mlp_pair_fwd(rank, s_one, w_in, hi, lo, [tok, *received(sum_g)])
        value, sent, final = sum_second(sum_out, [tok])
        sum_g, sent_g = sum_first(sum_g, sent)
        tok_in, tok = mlp_grads(top, top_a, top_act, top_dh, d_two_bf, [tok, *sent, *sent_g])
        x_two_top = shard(y_two) - sum_end(value, final, [tok_in])
        f_top = gather(rms_norm(x_two_top).astype(BF))
        value, sent, final = sum_second(sum_g, [tok])
        *parts, tok = mlp_out(rank, act_lo, w_out, lo, [tok, *sent])
        back = sum_end(value, final, [tok])
        d_one = shard(dy_one) + rms_vjp(shard(y_one), back)
        d_one_bf = gather(d_one.astype(BF))
        sum_out, sent = sum_first(sum_cores(parts), [back])
        f_hi, o_hi, qkv_hi, tok = attn(rank, head_dim, qkv_w, o_w, hi, x=s_two, norm=True, after=[tok, wo_all, *sent])
        value, sent, final = sum_second(sum_out, [tok])
        o_top, qkv_top, tok = attn(rank, head_dim, qkv_w, o_w, top, x=f_top, after=[tok, *sent])
        g_sum = sum_end(value, final, [tok])
        g_full = gather(g_sum)
        x_two = shard(s_two) - g_sum
        dqkv_top, *parts, tok = attn(rank, head_dim, qkv_w, o_w, top, qkv=qkv_top, d=d_one_bf, after=[tok, g_sum])
        sum_top, sent = sum_first(sum_cores(parts))
        dqkv_hi, *parts, tok = attn(rank, head_dim, qkv_w, o_w, hi, qkv=qkv_hi, d=d_one_bf, after=[tok, *sent])
        sum_hi = sum_cores(parts)
        value, sent, final = sum_second(sum_top, [tok, *received(sum_hi)])
        sum_hi, sent_hi = sum_first(sum_hi, sent)
        tok = attn_grads(top, f_top, o_top, dqkv_top, d_one_bf, [tok, *sent, *sent_hi])
        d_two = shard(dy_two) + rms_vjp(x_two_top, sum_end(value, final, [tok]))
        d_two_hi_bf = gather(d_two.astype(BF))
        value, sent, final = sum_second(sum_hi, [tok])
        tok = attn_grads(hi, f_hi, o_hi, dqkv_hi, d_one_bf, [tok, *sent])
        d_two = d_two + rms_vjp(shard(s_two), sum_end(value, final, [tok]))
        d_two_lo_bf = gather(d_two.astype(BF))
        x_two_full, f_lo, o_lo, qkv_lo, tok = attn(rank, head_dim, qkv_w, o_w, lo, x=s_two, minus=g_full, norm=True, after=[tok])
        o_all = gather(o_lo)
        dh_hi, tok = mlp_dhid(rank, d_two_hi_bf, w_out, hi, h_hi, [tok])
        _, tok = mlp_grads(hi, s_a, act_hi, dh_hi, d_two_hi_bf, [tok])
        dh_lo, *parts, tok = mlp_pair_back(rank, d_two_lo_bf, w_out, h_lo, dh_hi, w_in, hi, lo, [tok])
        sum_g, sent = sum_first(sum_cores(parts))
        tok_in, tok = mlp_grads(lo, s_a, act_lo, dh_lo, d_two_lo_bf, [tok, *sent])
        value, sent, final = sum_second(sum_g, [tok_in])
        d_one = d_one + rms_vjp(shard(s_one), sum_end(value, final))
        d_one_bf = gather(tie(d_one.astype(BF), [o_all]))
        x_one_full, tok = attn_value(rank, s_one, o_all, wo_all, [tok])
        dqkv_lo, *parts, tok = attn(rank, head_dim, qkv_w, o_w, lo, qkv=qkv_lo, d=d_one_bf, after=[tok])
        sum_lo, sent = sum_first(sum_cores(parts))
        tok = attn_grads(lo, f_lo, o_lo, dqkv_lo, d_one_bf, [tok, *sent])
        value, sent, final = sum_second(sum_lo, [tok])
        d_two = d_two + rms_vjp(x_two, sum_end(value, final))
        d_one_full, _ = emit(rank, gather(d_one), [tok])
        grad_qkv = stacks["attn"][0].reshape(n_layers, 3, n_heads, head_dim, width).transpose(0, 4, 1, 2, 3)
        grad_o = stacks["attn"][1].reshape(w_o.shape)
        return (x_one_full, x_two_full, d_one_full, gather(d_two), grad_qkv, grad_o, stacks["in"][0], stacks["out"][0])

    return jax.shard_map(
        per_device,
        mesh=mesh,
        in_specs=(act_spec,) * 4 + (saved_spec,) * 2 + weight_specs,
        out_specs=(act_spec,) * 4 + grad_specs,
        check_vma=False,
    )
```

```python
import jax
import jax.numpy as jnp
from jax import lax
from jax.experimental import pallas as pl
from jax.experimental.pallas import tpu as pltpu
from jax.sharding import PartitionSpec as P

EPS = 1e-6
BF = jnp.bfloat16
F32 = jnp.float32
GELU_C = 0.7978845608028654
GELU_A = 0.044715


def rms_norm(state):
    return state * lax.rsqrt(jnp.mean(state * state, axis=-1, keepdims=True) + EPS)


def rms_vjp(state, cot):
    rinv = lax.rsqrt(jnp.mean(state * state, axis=-1, keepdims=True) + EPS)
    normed = state * rinv
    return rinv * (cot - normed * jnp.mean(cot * normed, axis=-1, keepdims=True))


def dot(left, right, dims=((1,), (0,))):
    return lax.dot_general(left, right, (dims, ((), ())), preferred_element_type=F32)


def dot_nt(left, right):
    return dot(left, right, ((1,), (1,)))


def dot_tn(left, right):
    return dot(left, right, ((0,), (0,)))


def gelu_both(hid):
    sq = hid * hid
    th = jnp.tanh(GELU_C * (hid + GELU_A * (sq * hid)))
    cdf = 0.5 * (1.0 + th)
    return hid * cdf, cdf + hid * (0.5 * (1.0 - th * th)) * (GELU_C * (1.0 + 3.0 * GELU_A * sq))


MIB = 1024 * 1024


def seq_call(body, rank, ins, outs, parts, flops, after=()):
    n_in, n_out = len(ins), len(outs)
    seqs = 8

    def run(parity, previous, after):
        steps = seqs if parity is None else seqs // 2

        def seq(g, rk):
            return g if parity is None else (2 * g + parity) ^ rk[0]

        def spec(kind, shape, layer=0):
            if kind == "row":
                return pl.BlockSpec((None,) + tuple(shape[1:]), lambda g, rk: (seq(g, rk), 0, 0))
            if kind == "col":
                return pl.BlockSpec((shape[0], shape[1] // seqs), lambda g, rk: (0, seq(g, rk)))
            if kind == "layer":
                return pl.BlockSpec((None,) + tuple(shape[1:]), lambda g, rk: (layer, 0, 0))
            return pl.BlockSpec(tuple(shape), lambda g, rk: (0,) * len(shape))

        hidden = list(previous) + list(after)
        in_specs = [spec(kind, arr.shape, *layer) for kind, arr, *layer in ins] + [pl.BlockSpec(memory_space=pl.ANY)] * len(hidden)
        out_specs = [spec(kind, shape) for kind, shape, _ in outs]
        out_shape = [jax.ShapeDtypeStruct(shape, dtype) for _, shape, dtype in outs]
        for rows, width, dtype in parts:
            for _ in range(2):
                out_specs.append(pl.BlockSpec((None, rows, width // 2), lambda g, rk: (g, 0, 0)))
                out_shape.append(jax.ShapeDtypeStruct((steps, rows, width // 2), dtype))

        out_specs.append(pl.BlockSpec((8, 128), lambda g, rk: (0, 0)))
        out_shape.append(jax.ShapeDtypeStruct((8, 128), F32))

        def kernel(rank_ref, *refs):
            refs[-1][...] = jnp.zeros((8, 128), F32)
            in_refs = refs[:n_in]
            out_refs = refs[n_in + len(hidden):n_in + len(hidden) + n_out]
            part_refs = refs[n_in + len(hidden) + n_out:]
            for index, value in enumerate(body(in_refs, out_refs)):
                left, right = part_refs[2 * index:2 * index + 2]
                half = value.shape[-1] // 2
                left[...] = value[:, :half].astype(left.dtype)
                right[...] = value[:, half:].astype(right.dtype)

        share = 1 if parity is None else 2
        nbytes = sum(o.size * o.dtype.itemsize for o in out_shape) // share
        return pl.pallas_call(
        kernel,
        grid_spec=pltpu.PrefetchScalarGridSpec(
            num_scalar_prefetch=1, grid=(steps,), in_specs=in_specs, out_specs=out_specs
        ),
        out_shape=out_shape,
        input_output_aliases={1 + n_in + index: index for index in range(len(previous))},
        compiler_params=pltpu.CompilerParams(dimension_semantics=("arbitrary",), vmem_limit_bytes=60 * MIB),
        cost_estimate=pl.CostEstimate(flops=flops // share, bytes_accessed=nbytes, transcendentals=0),
        )(rank, *[arr for _, arr, *_ in ins], *hidden)

    if not parts:
        return list(run(None, (), after))
    sent = list(run(1, (), after))
    kept = list(run(0, sent[:n_out], [sent[-1]]))
    return kept[:n_out] + [sent[n_out], sent[n_out + 1], kept[n_out], kept[n_out + 1], kept[-1]]


def mlp_fwd(rank, x, w_in, layer):
    seqs, rows, width = x.shape
    inner = w_in.shape[2]

    def body(in_refs, out_refs):
        x_ref, win_ref = in_refs
        a_ref, slope_ref, act_ref = out_refs
        a = rms_norm(x_ref[...]).astype(BF)
        a_ref[...] = a
        hid = dot(a, win_ref[...])
        act, slope_ref[...] = gelu_both(hid)
        act_ref[...] = act.astype(BF)
        return ()

    mid = (seqs, rows, inner)
    outs = [("row", x.shape, BF), ("row", mid, F32), ("row", mid, BF)]
    return seq_call(body, rank, [("row", x), ("layer", w_in, layer)], outs, [], 2 * seqs * rows * width * inner)


def mlp_back(rank, d, w_out, slope, w_in, layer, after=()):
    seqs, rows, width = d.shape
    inner = w_out.shape[1]

    def body(in_refs, out_refs):
        d_ref, wout_ref, slope_ref, win_ref = in_refs
        dbf_ref, dh_ref = out_refs
        d_bf = d_ref[...].astype(BF)
        dbf_ref[...] = d_bf
        dh = (dot_nt(d_bf, wout_ref[...]) * slope_ref[...]).astype(BF)
        dh_ref[...] = dh
        yield dot_nt(dh, win_ref[...])

    ins = [("row", d), ("layer", w_out, layer), ("row", slope), ("layer", w_in, layer)]
    outs = [("row", d.shape, BF), ("row", slope.shape, BF)]
    return seq_call(body, rank, ins, outs, [(rows, width, BF)], 4 * seqs * rows * width * inner, after)


def mlp_out(rank, act, w_out, layer, after=()):
    rows, width = act.shape[1], w_out.shape[2]

    def body(in_refs, out_refs):
        yield dot(in_refs[0][...], in_refs[1][...])

    return seq_call(body, rank, [("row", act), ("layer", w_out, layer)], [], [(rows, width, F32)], 2 * act.size * width, after)


def mlp_pair_fwd(rank, x, w_in, hi, lo, after=()):
    seqs, rows, width = x.shape
    inner = w_in.shape[2]

    def body(in_refs, out_refs):
        x_ref, whi_ref, wlo_ref = in_refs
        a_ref, shi_ref, acthi_ref, slo_ref, actlo_ref = out_refs
        a = rms_norm(x_ref[...]).astype(BF)
        a_ref[...] = a
        for w_ref, slope_ref, act_ref in ((wlo_ref, slo_ref, actlo_ref), (whi_ref, shi_ref, acthi_ref)):
            hid = dot(a, w_ref[...])
            act, slope_ref[...] = gelu_both(hid)
            act_ref[...] = act.astype(BF)
        return ()

    mid = (seqs, rows, inner)
    outs = [("row", x.shape, BF), ("row", mid, F32), ("row", mid, BF), ("row", mid, F32), ("row", mid, BF)]
    ins = [("row", x), ("layer", w_in, hi), ("layer", w_in, lo)]
    return seq_call(body, rank, ins, outs, [], 4 * seqs * rows * width * inner, after)


def mlp_dhid(rank, d, w_out, layer, slope, after=()):
    seqs, rows, width = d.shape
    inner = w_out.shape[1]

    def body(in_refs, out_refs):
        d_ref, w_ref, slope_ref = in_refs
        out_refs[0][...] = (dot_nt(d_ref[...], w_ref[...]) * slope_ref[...]).astype(BF)
        return ()

    ins = [("row", d), ("layer", w_out, layer), ("row", slope)]
    return seq_call(body, rank, ins, [("row", slope.shape, BF)], [], 2 * seqs * rows * width * inner, after)


def mlp_pair_back(rank, d, w_out, slope, dh_hi, w_in, hi, lo, after=()):
    seqs, rows, width = d.shape
    inner = w_out.shape[1]

    def body(in_refs, out_refs):
        d_ref, w_ref, slope_ref, dshi_ref, whi_ref, wlo_ref = in_refs
        dh = (dot_nt(d_ref[...], w_ref[...]) * slope_ref[...]).astype(BF)
        out_refs[0][...] = dh
        yield dot_nt(dshi_ref[...], whi_ref[...]) + dot_nt(dh, wlo_ref[...])

    ins = [("row", d), ("layer", w_out, lo), ("row", slope), ("row", dh_hi), ("layer", w_in, hi), ("layer", w_in, lo)]
    return seq_call(body, rank, ins, [("row", slope.shape, BF)], [(rows, width, BF)], 6 * seqs * rows * width * inner, after)


def attn(rank, head_dim, w_qkv, w_o, layer, x=None, minus=None, norm=False, qkv=None, d=None, after=()):
    seqs, rows, width = (x if x is not None else d).shape
    cols, inner = w_qkv.shape[1], w_o.shape[1]
    heads = inner // head_dim
    scale = head_dim ** -0.5
    forward, backward = x is not None, d is not None
    ins, outs = [("layer", w_qkv, layer)], []
    if forward:
        ins.append(("row", x))
        if minus is not None:
            ins.append(("row", minus))
            outs.append(("row", x.shape, F32))
        if norm:
            outs.append(("row", x.shape, BF))
        outs.append(("col", (inner, seqs * rows), BF))
        if not backward:
            outs.append(("col", (cols, seqs * rows), BF))
    else:
        ins.append(("col", qkv))
    if backward:
        ins += [("layer", w_o, layer), ("row", d)]
        outs.append(("col", (cols, seqs * rows), BF))

    def body(in_refs, out_refs):
        in_refs, out_refs = list(in_refs), list(out_refs)
        wqkv_ref = in_refs.pop(0)
        if forward:
            value = in_refs.pop(0)[...]
            if minus is not None:
                value = value - in_refs.pop(0)[...]
                out_refs.pop(0)[...] = value
            if norm:
                value = rms_norm(value).astype(BF)
                out_refs.pop(0)[...] = value
            o_ref = out_refs.pop(0)
            qkv_t = dot_nt(wqkv_ref[...], value).astype(BF)
            if not backward:
                out_refs.pop(0)[...] = qkv_t
        else:
            qkv_t = in_refs.pop(0)[...]
        if backward:
            wo_ref, d_ref = in_refs
            dqkv_ref = out_refs.pop(0)
            dheads = dot_nt(wo_ref[...], d_ref[...]).astype(BF)
        pieces = [[], [], []]
        for n in range(heads):
            lo = n * head_dim
            q_t, k_t, v_t = (qkv_t[part * inner + lo:part * inner + lo + head_dim] for part in range(3))
            scores = dot_tn(k_t, q_t) * scale
            expd = jnp.exp(scores - jnp.max(scores, axis=0, keepdims=True))
            probs = expd / jnp.sum(expd, axis=0, keepdims=True)
            probs_bf = probs.astype(BF)
            if forward:
                o_ref[pl.ds(lo, head_dim), :] = dot(v_t, probs_bf).astype(BF)
            if backward:
                dhead = dheads[lo:lo + head_dim]
                d_v = dot_nt(dhead, probs_bf)
                d_probs = dot_tn(v_t, dhead)
                d_scores = (probs * (d_probs - jnp.sum(d_probs * probs, axis=0, keepdims=True)) * scale).astype(BF)
                for part, piece in enumerate((dot(k_t, d_scores), dot_nt(q_t, d_scores), d_v)):
                    pieces[part].append(piece.astype(BF))
        if backward:
            dqkv = jnp.concatenate(pieces[0] + pieces[1] + pieces[2], axis=0)
            dqkv_ref[...] = dqkv
            yield dot_tn(dqkv, wqkv_ref[...])

    flops = 2 * seqs * rows * (width * (cols * (forward + backward) + inner * backward) + rows * inner * (2 * forward + 5 * backward))
    return seq_call(body, rank, ins, outs, [(rows, width, BF)] if backward else [], flops, after)


def attn_value(rank, base, o_all, wo_all, after=()):
    def body(in_refs, out_refs):
        base_ref, o_ref, w_ref = in_refs
        out_refs[0][...] = base_ref[...] - dot_tn(o_ref[...], w_ref[...])
        return ()

    ins = [("row", base), ("col", o_all), ("all", wo_all)]
    return seq_call(body, rank, ins, [("row", base.shape, F32)], [], 2 * base.size * wo_all.shape[0], after)


def emit(rank, array, after=()):
    def body(in_refs, out_refs):
        out_refs[0][...] = in_refs[0][...]
        return ()

    return seq_call(body, rank, [("row", array)], [("row", array.shape, array.dtype)], [], 16 * array.size, after)


def weight_grads(stacks, layers, layer, jobs, after=()):
    steps = 5
    in_specs, out_specs, out_shape, args, flops, vmem = [], [], [], [], 0, 0
    for left, right, split in jobs:
        tokens, n_cols = right.shape
        if split == "rows":
            n_rows = left.shape[1]
            in_specs.append(pl.BlockSpec((tokens, n_rows // steps), lambda g: (0, g)))
            in_specs.append(pl.BlockSpec((tokens, n_cols), lambda g: (0, 0)))
            out_specs.append(pl.BlockSpec((None, n_rows // steps, n_cols), lambda g: (layer, g, 0)))
        else:
            n_rows = left.shape[0]
            in_specs.append(pl.BlockSpec((n_rows, tokens), lambda g: (0, 0)))
            in_specs.append(pl.BlockSpec((tokens, n_cols // steps), lambda g: (0, g)))
            out_specs.append(pl.BlockSpec((None, n_rows, n_cols // steps), lambda g: (layer, 0, g)))
        out_shape.append(jax.ShapeDtypeStruct((layers, n_rows, n_cols), F32))
        args += [left, right]
        flops += 2 * tokens * n_rows * n_cols
        vmem += 4 * (left.size + right.size) + 2 * n_rows * n_cols
    n_jobs = len(jobs)
    aliases = {}
    if stacks[0] is not None:
        aliases = {len(args) + index: index for index in range(n_jobs)}
        args += stacks
    args += list(after)
    in_specs += [pl.BlockSpec(memory_space=pl.ANY)] * (len(args) - 2 * n_jobs)
    out_specs.append(pl.BlockSpec((8, 128), lambda g: (0, 0)))
    out_shape.append(jax.ShapeDtypeStruct((8, 128), F32))

    def kernel(*refs):
        outs = refs[len(args):]
        for index, (_, _, split) in enumerate(jobs):
            left_ref, right_ref = refs[2 * index:2 * index + 2]
            outs[index][...] = (dot_tn if split == "rows" else dot)(left_ref[...], right_ref[...])
        outs[-1][...] = jnp.zeros((8, 128), F32)

    call = pl.pallas_call(
        kernel,
        grid=(steps,),
        in_specs=in_specs,
        out_specs=out_specs,
        out_shape=out_shape,
        input_output_aliases=aliases,
        compiler_params=pltpu.CompilerParams(dimension_semantics=("arbitrary",), vmem_limit_bytes=60 * MIB),
        cost_estimate=pl.CostEstimate(flops=flops, bytes_accessed=vmem, transcendentals=0),
    )
    *stacks, token = call(*args)
    return stacks, token


def permute(array, bit):
    return lax.ppermute(array, "tp", [(idx, idx ^ bit) for idx in range(8)])


def tie(value, tokens):
    return lax.optimization_barrier((value, *tokens))[0] if tokens else value


def sum_cores(parts):
    halves = []
    for send, keep, order in ((parts[0], parts[2], (2, 4)), (parts[1], parts[3], (4, 2))):
        grid = (2, 2) + keep.shape[1:]
        halves.append((keep.reshape(grid), permute(send, 1).reshape(grid), order))
    return halves


def sum_first(halves, begin=()):
    moving, sent = [], []
    for keep, recv, order in halves:
        recv = tie(recv, begin)
        pick = (lambda arr, pos: arr[:, pos]) if order[0] == 2 else (lambda arr, pos: arr[pos])
        away = pick(keep, 1) + pick(recv, 1)
        sent.append(away)
        moving.append((pick(keep, 0) + pick(recv, 0), permute(away, order[0]), order))
    return moving, sent


def received(halves):
    return [recv for _, recv, _ in halves]


def sum_second(moving, fill=()):
    value, sent, final = [], [], []
    for here, recv, order in moving:
        recv = tie(recv, fill)
        sent.append(here[1] + recv[1])
        value.append(here[0] + recv[0])
        final.append(permute(sent[-1], order[1]))
    return value, sent, final


def sum_end(value, final, fill=()):
    halves = [here.astype(F32) + tie(recv, fill).astype(F32) for here, recv in zip(value, final)]
    return jnp.concatenate(halves, axis=-1)[None]


def gather(shard):
    return lax.all_gather(shard, "tp", axis=0, tiled=True)


def solution(mesh):
    act_spec = P("dp", None, None)
    saved_spec = P(None, "dp", None, None)
    weight_specs = (P(None, None, None, "tp", None), P(None, "tp", None, None), P(None, None, "tp"), P(None, "tp", None))
    grad_specs = (P("dp", None, None, "tp", None), P("dp", "tp", None, None), P("dp", None, "tp"), P("dp", "tp", None))

    def per_device(y_one, y_two, dy_one, dy_two, saved_one, saved_two, w_qkv, w_o, w_in, w_out):
        index = lax.axis_index("tp")
        rank = index.astype(jnp.int32).reshape((1,))
        n_layers, width, _, n_heads, head_dim = w_qkv.shape
        tokens = y_one.shape[0] * y_one.shape[1]
        qkv_w = w_qkv.transpose(0, 2, 3, 4, 1).reshape(n_layers, 3 * n_heads * head_dim, width)
        o_w = w_o.reshape(n_layers, n_heads * head_dim, width)

        def shard(full):
            return lax.dynamic_slice_in_dim(full, index, 1, axis=0)

        def flat(full):
            return full.reshape(tokens, full.shape[-1])

        stacks = {"attn": [None] * 2, "in": [None], "out": [None]}

        def attn_grads(layer, a, o_t, dqkv_t, d_bf, after=()):
            jobs = [(dqkv_t, flat(a), "cols"), (o_t, flat(d_bf), "cols")]
            stacks["attn"], token = weight_grads(stacks["attn"], n_layers, layer, jobs, after)
            return token

        def mlp_grad(which, layer, left, right, after):
            stacks[which], token = weight_grads(
                stacks[which], n_layers, layer, [(flat(left), flat(right), "rows")], after
            )
            return token

        top, hi, lo = 2, 1, 0
        s_one, s_two = saved_one[0], saved_two[0]
        wo_all = gather(o_w[lo])
        top_a, s_top, top_act, tok = mlp_fwd(rank, y_one, w_in, top)
        *parts, tok = mlp_out(rank, top_act, w_out, top, [tok])
        sum_out, sent = sum_first(sum_cores(parts))
        d_two_bf, top_dh, *parts, tok = mlp_back(rank, dy_two, w_out, s_top, w_in, top, [tok, *sent])
        sum_g = sum_cores(parts)
        tok_in = mlp_grad("in", top, top_a, top_dh, [tok, *received(sum_g)])
        value, sent, final = sum_second(sum_out, [tok_in])
        sum_g, sent_g = sum_first(sum_g, sent)
        tok = mlp_grad("out", top, top_act, d_two_bf, [tok_in, *sent, *sent_g])
        x_two_top = shard(y_two) - sum_end(value, final, [tok])
        f_top = gather(rms_norm(x_two_top).astype(BF))
        s_a, sl_hi, act_hi, sl_lo, act_lo, tok = mlp_pair_fwd(rank, s_one, w_in, hi, lo, [tok])
        value, sent, final = sum_second(sum_g, [tok])
        *parts, tok = mlp_out(rank, act_lo, w_out, lo, [tok, *sent])
        back = sum_end(value, final, [tok])
        d_one = shard(dy_one) + rms_vjp(shard(y_one), back)
        d_one_bf = gather(d_one.astype(BF))
        sum_out, sent = sum_first(sum_cores(parts), [back])
        f_hi, o_hi, qkv_hi, tok = attn(rank, head_dim, qkv_w, o_w, hi, x=s_two, norm=True, after=[tok, wo_all, *sent])
        o_top, qkv_top, tok = attn(rank, head_dim, qkv_w, o_w, top, x=f_top, after=[tok])
        value, sent, final = sum_second(sum_out, [tok])
        dqkv_top, *parts, tok = attn(rank, head_dim, qkv_w, o_w, top, qkv=qkv_top, d=d_one_bf, after=[tok, *sent])
        g_sum = sum_end(value, final, [tok])
        g_full = gather(g_sum)
        x_two = shard(s_two) - g_sum
        sum_top, sent = sum_first(sum_cores(parts))
        dqkv_hi, *parts, tok = attn(rank, head_dim, qkv_w, o_w, hi, qkv=qkv_hi, d=d_one_bf, after=[tok, *sent])
        sum_hi = sum_cores(parts)
        value, sent, final = sum_second(sum_top, [tok, *received(sum_hi)])
        sum_hi, sent_hi = sum_first(sum_hi, sent)
        tok = attn_grads(top, f_top, o_top, dqkv_top, d_one_bf, [tok, *sent, *sent_hi])
        d_two = shard(dy_two) + rms_vjp(x_two_top, sum_end(value, final, [tok]))
        d_two_hi_bf = gather(d_two.astype(BF))
        value, sent, final = sum_second(sum_hi, [tok])
        tok = attn_grads(hi, f_hi, o_hi, dqkv_hi, d_one_bf, [tok, *sent])
        d_two = d_two + rms_vjp(shard(s_two), sum_end(value, final, [tok]))
        d_two_lo_bf = gather(d_two.astype(BF))
        x_two_full, f_lo, o_lo, qkv_lo, tok = attn(rank, head_dim, qkv_w, o_w, lo, x=s_two, minus=g_full, norm=True, after=[tok])
        o_all = gather(o_lo)
        dh_hi, tok = mlp_dhid(rank, d_two_hi_bf, w_out, hi, sl_hi, [tok])
        tok = mlp_grad("in", hi, s_a, dh_hi, [tok])
        tok = mlp_grad("out", hi, act_hi, d_two_hi_bf, [tok])
        dh_lo, *parts, tok = mlp_pair_back(rank, d_two_lo_bf, w_out, sl_lo, dh_hi, w_in, hi, lo, [tok])
        sum_g, sent = sum_first(sum_cores(parts))
        tok_in = mlp_grad("in", lo, s_a, dh_lo, [tok, *sent])
        tok = mlp_grad("out", lo, act_lo, d_two_lo_bf, [tok_in])
        value, sent, final = sum_second(sum_g, [tok_in])
        d_one = d_one + rms_vjp(shard(s_one), sum_end(value, final))
        d_one_bf = gather(tie(d_one.astype(BF), [o_all]))
        x_one_full, tok = attn_value(rank, s_one, o_all, wo_all, [tok])
        dqkv_lo, *parts, tok = attn(rank, head_dim, qkv_w, o_w, lo, qkv=qkv_lo, d=d_one_bf, after=[tok])
        sum_lo, sent = sum_first(sum_cores(parts))
        tok = attn_grads(lo, f_lo, o_lo, dqkv_lo, d_one_bf, [tok, *sent])
        value, sent, final = sum_second(sum_lo, [tok])
        d_two = d_two + rms_vjp(x_two, sum_end(value, final))
        d_one_full, _ = emit(rank, gather(d_one), [tok])
        grad_qkv = stacks["attn"][0].reshape(n_layers, 3, n_heads, head_dim, width).transpose(0, 4, 1, 2, 3)
        grad_o = stacks["attn"][1].reshape(w_o.shape)
        return (x_one_full, x_two_full, d_one_full, gather(d_two), grad_qkv, grad_o, stacks["in"][0], stacks["out"][0])

    return jax.shard_map(
        per_device,
        mesh=mesh,
        in_specs=(act_spec,) * 4 + (saved_spec,) * 2 + weight_specs,
        out_specs=(act_spec,) * 4 + grad_specs,
        check_vma=False,
    )
```

```python
import jax
import jax.numpy as jnp
from jax import lax
from jax.experimental import pallas as pl
from jax.experimental.pallas import tpu as pltpu
from jax.sharding import PartitionSpec as P

EPS = 1e-6
BF = jnp.bfloat16
F32 = jnp.float32
GELU_C = 0.7978845608028654
GELU_A = 0.044715


def rms_norm(state):
    return state * lax.rsqrt(jnp.mean(state * state, axis=-1, keepdims=True) + EPS)


def rms_vjp(state, cot):
    rinv = lax.rsqrt(jnp.mean(state * state, axis=-1, keepdims=True) + EPS)
    normed = state * rinv
    return rinv * (cot - normed * jnp.mean(cot * normed, axis=-1, keepdims=True))


def dot(left, right, dims=((1,), (0,))):
    return lax.dot_general(left, right, (dims, ((), ())), preferred_element_type=F32)


def dot_nt(left, right):
    return dot(left, right, ((1,), (1,)))


def dot_tn(left, right):
    return dot(left, right, ((0,), (0,)))


def gelu_both(hid):
    sq = hid * hid
    th = jnp.tanh(GELU_C * (hid + GELU_A * (sq * hid)))
    cdf = 0.5 * (1.0 + th)
    return hid * cdf, cdf + hid * (0.5 * (1.0 - th * th)) * (GELU_C * (1.0 + 3.0 * GELU_A * sq))


MIB = 1024 * 1024


def seq_call(body, rank, ins, outs, parts, flops, after=()):
    n_in, n_out = len(ins), len(outs)
    seqs = 8

    def run(parity, previous, after):
        steps = seqs if parity is None else seqs // 2

        def seq(g, rk):
            return g if parity is None else (2 * g + parity) ^ rk[0]

        def spec(kind, shape, layer=0):
            if kind == "row":
                return pl.BlockSpec((None,) + tuple(shape[1:]), lambda g, rk: (seq(g, rk), 0, 0))
            if kind == "col":
                return pl.BlockSpec((shape[0], shape[1] // seqs), lambda g, rk: (0, seq(g, rk)))
            if kind == "layer":
                return pl.BlockSpec((None,) + tuple(shape[1:]), lambda g, rk: (layer, 0, 0))
            return pl.BlockSpec(tuple(shape), lambda g, rk: (0,) * len(shape))

        hidden = list(previous) + list(after)
        in_specs = [spec(kind, arr.shape, *layer) for kind, arr, *layer in ins] + [pl.BlockSpec(memory_space=pl.ANY)] * len(hidden)
        out_specs = [spec(kind, shape) for kind, shape, _ in outs]
        out_shape = [jax.ShapeDtypeStruct(shape, dtype) for _, shape, dtype in outs]
        for rows, width, dtype in parts:
            for _ in range(2):
                out_specs.append(pl.BlockSpec((None, rows, width // 2), lambda g, rk: (g, 0, 0)))
                out_shape.append(jax.ShapeDtypeStruct((steps, rows, width // 2), dtype))

        out_specs.append(pl.BlockSpec((8, 128), lambda g, rk: (0, 0)))
        out_shape.append(jax.ShapeDtypeStruct((8, 128), F32))

        def kernel(rank_ref, *refs):
            refs[-1][...] = jnp.zeros((8, 128), F32)
            in_refs = refs[:n_in]
            out_refs = refs[n_in + len(hidden):n_in + len(hidden) + n_out]
            part_refs = refs[n_in + len(hidden) + n_out:]
            for index, value in enumerate(body(in_refs, out_refs)):
                left, right = part_refs[2 * index:2 * index + 2]
                half = value.shape[-1] // 2
                left[...] = value[:, :half].astype(left.dtype)
                right[...] = value[:, half:].astype(right.dtype)

        share = 1 if parity is None else 2
        nbytes = sum(o.size * o.dtype.itemsize for o in out_shape) // share
        return pl.pallas_call(
        kernel,
        grid_spec=pltpu.PrefetchScalarGridSpec(
            num_scalar_prefetch=1, grid=(steps,), in_specs=in_specs, out_specs=out_specs
        ),
        out_shape=out_shape,
        input_output_aliases={1 + n_in + index: index for index in range(len(previous))},
        compiler_params=pltpu.CompilerParams(dimension_semantics=("arbitrary",), vmem_limit_bytes=60 * MIB),
        cost_estimate=pl.CostEstimate(flops=flops // share, bytes_accessed=nbytes, transcendentals=0),
        )(rank, *[arr for _, arr, *_ in ins], *hidden)

    if not parts:
        return list(run(None, (), after))
    sent = list(run(1, (), after))
    kept = list(run(0, sent[:n_out], [sent[-1]]))
    return kept[:n_out] + [sent[n_out], sent[n_out + 1], kept[n_out], kept[n_out + 1], kept[-1]]


def mlp_fwd(rank, x, w_in, layer):
    seqs, rows, width = x.shape
    inner = w_in.shape[2]

    def body(in_refs, out_refs):
        x_ref, win_ref = in_refs
        a_ref, slope_ref, act_ref = out_refs
        a = rms_norm(x_ref[...]).astype(BF)
        a_ref[...] = a
        hid = dot(a, win_ref[...])
        act, slope_ref[...] = gelu_both(hid)
        act_ref[...] = act.astype(BF)
        return ()

    mid = (seqs, rows, inner)
    outs = [("row", x.shape, BF), ("row", mid, F32), ("row", mid, BF)]
    return seq_call(body, rank, [("row", x), ("layer", w_in, layer)], outs, [], 2 * seqs * rows * width * inner)


def mlp_back(rank, d, w_out, slope, w_in, layer, after=()):
    seqs, rows, width = d.shape
    inner = w_out.shape[1]

    def body(in_refs, out_refs):
        d_ref, wout_ref, slope_ref, win_ref = in_refs
        dbf_ref, dh_ref = out_refs
        d_bf = d_ref[...].astype(BF)
        dbf_ref[...] = d_bf
        dh = (dot_nt(d_bf, wout_ref[...]) * slope_ref[...]).astype(BF)
        dh_ref[...] = dh
        yield dot_nt(dh, win_ref[...])

    ins = [("row", d), ("layer", w_out, layer), ("row", slope), ("layer", w_in, layer)]
    outs = [("row", d.shape, BF), ("row", slope.shape, BF)]
    return seq_call(body, rank, ins, outs, [(rows, width, BF)], 4 * seqs * rows * width * inner, after)


def mlp_out(rank, act, w_out, layer, after=()):
    rows, width = act.shape[1], w_out.shape[2]

    def body(in_refs, out_refs):
        yield dot(in_refs[0][...], in_refs[1][...])

    return seq_call(body, rank, [("row", act), ("layer", w_out, layer)], [], [(rows, width, F32)], 2 * act.size * width, after)


def mlp_pair_fwd(rank, x, w_in, hi, lo, after=()):
    seqs, rows, width = x.shape
    inner = w_in.shape[2]

    def body(in_refs, out_refs):
        x_ref, whi_ref, wlo_ref = in_refs
        a_ref, shi_ref, acthi_ref, slo_ref, actlo_ref = out_refs
        a = rms_norm(x_ref[...]).astype(BF)
        a_ref[...] = a
        for w_ref, slope_ref, act_ref in ((wlo_ref, slo_ref, actlo_ref), (whi_ref, shi_ref, acthi_ref)):
            hid = dot(a, w_ref[...])
            act, slope_ref[...] = gelu_both(hid)
            act_ref[...] = act.astype(BF)
        return ()

    mid = (seqs, rows, inner)
    outs = [("row", x.shape, BF), ("row", mid, F32), ("row", mid, BF), ("row", mid, F32), ("row", mid, BF)]
    ins = [("row", x), ("layer", w_in, hi), ("layer", w_in, lo)]
    return seq_call(body, rank, ins, outs, [], 4 * seqs * rows * width * inner, after)


def mlp_dhid(rank, d, w_out, layer, slope, after=()):
    seqs, rows, width = d.shape
    inner = w_out.shape[1]

    def body(in_refs, out_refs):
        d_ref, w_ref, slope_ref = in_refs
        out_refs[0][...] = (dot_nt(d_ref[...], w_ref[...]) * slope_ref[...]).astype(BF)
        return ()

    ins = [("row", d), ("layer", w_out, layer), ("row", slope)]
    return seq_call(body, rank, ins, [("row", slope.shape, BF)], [], 2 * seqs * rows * width * inner, after)


def mlp_pair_back(rank, d, w_out, slope, dh_hi, w_in, hi, lo, after=()):
    seqs, rows, width = d.shape
    inner = w_out.shape[1]

    def body(in_refs, out_refs):
        d_ref, w_ref, slope_ref, dshi_ref, whi_ref, wlo_ref = in_refs
        dh = (dot_nt(d_ref[...], w_ref[...]) * slope_ref[...]).astype(BF)
        out_refs[0][...] = dh
        yield dot_nt(dshi_ref[...], whi_ref[...]) + dot_nt(dh, wlo_ref[...])

    ins = [("row", d), ("layer", w_out, lo), ("row", slope), ("row", dh_hi), ("layer", w_in, hi), ("layer", w_in, lo)]
    return seq_call(body, rank, ins, [("row", slope.shape, BF)], [(rows, width, BF)], 6 * seqs * rows * width * inner, after)


def attn(rank, head_dim, w_qkv, w_o, layer, x=None, minus=None, norm=False, qkv=None, d=None, after=()):
    seqs, rows, width = (x if x is not None else d).shape
    cols, inner = w_qkv.shape[1], w_o.shape[1]
    heads = inner // head_dim
    scale = head_dim ** -0.5
    forward, backward = x is not None, d is not None
    ins, outs = [("layer", w_qkv, layer)], []
    if forward:
        ins.append(("row", x))
        if minus is not None:
            ins.append(("row", minus))
            outs.append(("row", x.shape, F32))
        if norm:
            outs.append(("row", x.shape, BF))
        outs.append(("col", (inner, seqs * rows), BF))
        if not backward:
            outs.append(("col", (cols, seqs * rows), BF))
    else:
        ins.append(("col", qkv))
    if backward:
        ins += [("layer", w_o, layer), ("row", d)]
        outs.append(("col", (cols, seqs * rows), BF))

    def body(in_refs, out_refs):
        in_refs, out_refs = list(in_refs), list(out_refs)
        wqkv_ref = in_refs.pop(0)
        if forward:
            value = in_refs.pop(0)[...]
            if minus is not None:
                value = value - in_refs.pop(0)[...]
                out_refs.pop(0)[...] = value
            if norm:
                value = rms_norm(value).astype(BF)
                out_refs.pop(0)[...] = value
            o_ref = out_refs.pop(0)
            qkv_t = dot_nt(wqkv_ref[...], value).astype(BF)
            if not backward:
                out_refs.pop(0)[...] = qkv_t
        else:
            qkv_t = in_refs.pop(0)[...]
        if backward:
            wo_ref, d_ref = in_refs
            dqkv_ref = out_refs.pop(0)
            dheads = dot_nt(wo_ref[...], d_ref[...]).astype(BF)
        pieces = [[], [], []]
        for n in range(heads):
            lo = n * head_dim
            q_t, k_t, v_t = (qkv_t[part * inner + lo:part * inner + lo + head_dim] for part in range(3))
            scores = dot_tn(k_t, q_t) * scale
            expd = jnp.exp(scores - jnp.max(scores, axis=0, keepdims=True))
            probs = expd / jnp.sum(expd, axis=0, keepdims=True)
            probs_bf = probs.astype(BF)
            if forward:
                o_ref[pl.ds(lo, head_dim), :] = dot(v_t, probs_bf).astype(BF)
            if backward:
                dhead = dheads[lo:lo + head_dim]
                d_v = dot_nt(dhead, probs_bf)
                d_probs = dot_tn(v_t, dhead)
                d_scores = (probs * (d_probs - jnp.sum(d_probs * probs, axis=0, keepdims=True)) * scale).astype(BF)
                for part, piece in enumerate((dot(k_t, d_scores), dot_nt(q_t, d_scores), d_v)):
                    pieces[part].append(piece.astype(BF))
        if backward:
            dqkv = jnp.concatenate(pieces[0] + pieces[1] + pieces[2], axis=0)
            dqkv_ref[...] = dqkv
            yield dot_tn(dqkv, wqkv_ref[...])

    flops = 2 * seqs * rows * (width * (cols * (forward + backward) + inner * backward) + rows * inner * (2 * forward + 5 * backward))
    return seq_call(body, rank, ins, outs, [(rows, width, BF)] if backward else [], flops, after)


def attn_value(rank, base, o_all, wo_all, after=()):
    def body(in_refs, out_refs):
        base_ref, o_ref, w_ref = in_refs
        out_refs[0][...] = base_ref[...] - dot_tn(o_ref[...], w_ref[...])
        return ()

    ins = [("row", base), ("col", o_all), ("all", wo_all)]
    return seq_call(body, rank, ins, [("row", base.shape, F32)], [], 2 * base.size * wo_all.shape[0], after)


def assemble(rank, pieces, after=()):
    rows, width = pieces[0].shape
    half = width // 2

    def kernel(rank_ref, *refs):
        out_ref, token_ref = refs[-2:]
        token_ref[...] = jnp.zeros((8, 128), F32)
        step = pl.program_id(0)
        for place in range(6):

            @pl.when(step == place)
            def _(place=place):
                out_ref[...] = refs[place][...]

        for place in range(2):

            @pl.when(step == 6 + place)
            def _(place=place):
                out_ref[:, :half] = refs[6 + 2 * place][...]
                out_ref[:, half:] = refs[7 + 2 * place][...]

    return pl.pallas_call(
        kernel,
        grid_spec=pltpu.PrefetchScalarGridSpec(
            num_scalar_prefetch=1,
            grid=(8,),
            in_specs=[pl.BlockSpec(piece.shape, lambda g, rk: (0, 0)) for piece in pieces]
            + [pl.BlockSpec(memory_space=pl.ANY)] * len(after),
            out_specs=[
                pl.BlockSpec((None, rows, width), lambda g, rk: (g ^ rk[0], 0, 0)),
                pl.BlockSpec((8, 128), lambda g, rk: (0, 0)),
            ],
        ),
        out_shape=[jax.ShapeDtypeStruct((8, rows, width), F32), jax.ShapeDtypeStruct((8, 128), F32)],
        compiler_params=pltpu.CompilerParams(dimension_semantics=("arbitrary",), vmem_limit_bytes=60 * MIB),
        cost_estimate=pl.CostEstimate(flops=2 * 10**9, bytes_accessed=64 * rows * width, transcendentals=0),
    )(rank, *pieces, *after)


def weight_grads(stacks, layers, layer, jobs, after=()):
    steps = 5
    in_specs, out_specs, out_shape, args, flops, vmem = [], [], [], [], 0, 0
    for left, right, split in jobs:
        tokens, n_cols = right.shape
        if split == "rows":
            n_rows = left.shape[1]
            in_specs.append(pl.BlockSpec((tokens, n_rows // steps), lambda g: (0, g)))
            in_specs.append(pl.BlockSpec((tokens, n_cols), lambda g: (0, 0)))
            out_specs.append(pl.BlockSpec((None, n_rows // steps, n_cols), lambda g: (layer, g, 0)))
        else:
            n_rows = left.shape[0]
            in_specs.append(pl.BlockSpec((n_rows, tokens), lambda g: (0, 0)))
            in_specs.append(pl.BlockSpec((tokens, n_cols // steps), lambda g: (0, g)))
            out_specs.append(pl.BlockSpec((None, n_rows, n_cols // steps), lambda g: (layer, 0, g)))
        out_shape.append(jax.ShapeDtypeStruct((layers, n_rows, n_cols), F32))
        args += [left, right]
        flops += 2 * tokens * n_rows * n_cols
        vmem += 4 * (left.size + right.size) + 2 * n_rows * n_cols
    n_jobs = len(jobs)
    aliases = {}
    if stacks[0] is not None:
        aliases = {len(args) + index: index for index in range(n_jobs)}
        args += stacks
    args += list(after)
    in_specs += [pl.BlockSpec(memory_space=pl.ANY)] * (len(args) - 2 * n_jobs)
    out_specs.append(pl.BlockSpec((8, 128), lambda g: (0, 0)))
    out_shape.append(jax.ShapeDtypeStruct((8, 128), F32))

    def kernel(*refs):
        outs = refs[len(args):]
        for index, (_, _, split) in enumerate(jobs):
            left_ref, right_ref = refs[2 * index:2 * index + 2]
            outs[index][...] = (dot_tn if split == "rows" else dot)(left_ref[...], right_ref[...])
        outs[-1][...] = jnp.zeros((8, 128), F32)

    call = pl.pallas_call(
        kernel,
        grid=(steps,),
        in_specs=in_specs,
        out_specs=out_specs,
        out_shape=out_shape,
        input_output_aliases=aliases,
        compiler_params=pltpu.CompilerParams(dimension_semantics=("arbitrary",), vmem_limit_bytes=60 * MIB),
        cost_estimate=pl.CostEstimate(flops=flops, bytes_accessed=vmem, transcendentals=0),
    )
    *stacks, token = call(*args)
    return stacks, token


def permute(array, bit):
    return lax.ppermute(array, "tp", [(idx, idx ^ bit) for idx in range(8)])


def tie(value, tokens):
    return lax.optimization_barrier((value, *tokens))[0] if tokens else value


def sum_cores(parts):
    halves = []
    for send, keep, order in ((parts[0], parts[2], (2, 4)), (parts[1], parts[3], (4, 2))):
        grid = (2, 2) + keep.shape[1:]
        halves.append((keep.reshape(grid), permute(send, 1).reshape(grid), order))
    return halves


def sum_first(halves, begin=()):
    moving, sent = [], []
    for keep, recv, order in halves:
        recv = tie(recv, begin)
        pick = (lambda arr, pos: arr[:, pos]) if order[0] == 2 else (lambda arr, pos: arr[pos])
        away = pick(keep, 1) + pick(recv, 1)
        sent.append(away)
        moving.append((pick(keep, 0) + pick(recv, 0), permute(away, order[0]), order))
    return moving, sent


def received(halves):
    return [recv for _, recv, _ in halves]


def sum_second(moving, fill=()):
    value, sent, final = [], [], []
    for here, recv, order in moving:
        recv = tie(recv, fill)
        sent.append(here[1] + recv[1])
        value.append(here[0] + recv[0])
        final.append(permute(sent[-1], order[1]))
    return value, sent, final


def sum_end(value, final, fill=()):
    halves = [here.astype(F32) + tie(recv, fill).astype(F32) for here, recv in zip(value, final)]
    return jnp.concatenate(halves, axis=-1)[None]


def gather(shard):
    return lax.all_gather(shard, "tp", axis=0, tiled=True)


def spread_first(shard):
    return [permute(shard, bit) for bit in (1, 2, 4)]


def spread_second(near, fill):
    _, near_x, near_y = near
    near_x, near_y = tie(near_x, fill), tie(near_y, fill)
    half = near_x.shape[-1] // 2
    halves = (permute(near_y[:, :half], 2), permute(near_x[:, half:], 4))
    return halves, (permute(near_x, 1), permute(near_y, 1))


def spread_last(shard, near, halves, cross, fill):
    left, right = (tie(half, fill) for half in halves)
    cross_halves = [permute(half, 1) for half in (left, right)]
    return [shard, near[0], near[1], cross[0], near[2], cross[1], left, right, *cross_halves]


def solution(mesh):
    act_spec = P("dp", None, None)
    saved_spec = P(None, "dp", None, None)
    weight_specs = (P(None, None, None, "tp", None), P(None, "tp", None, None), P(None, None, "tp"), P(None, "tp", None))
    grad_specs = (P("dp", None, None, "tp", None), P("dp", "tp", None, None), P("dp", None, "tp"), P("dp", "tp", None))

    def per_device(y_one, y_two, dy_one, dy_two, saved_one, saved_two, w_qkv, w_o, w_in, w_out):
        index = lax.axis_index("tp")
        rank = index.astype(jnp.int32).reshape((1,))
        n_layers, width, _, n_heads, head_dim = w_qkv.shape
        tokens = y_one.shape[0] * y_one.shape[1]
        qkv_w = w_qkv.transpose(0, 2, 3, 4, 1).reshape(n_layers, 3 * n_heads * head_dim, width)
        o_w = w_o.reshape(n_layers, n_heads * head_dim, width)

        def shard(full):
            return lax.dynamic_slice_in_dim(full, index, 1, axis=0)

        def flat(full):
            return full.reshape(tokens, full.shape[-1])

        stacks = {"attn": [None] * 2, "in": [None], "out": [None]}

        def attn_grads(layer, a, o_t, dqkv_t, d_bf, after=()):
            jobs = [(dqkv_t, flat(a), "cols"), (o_t, flat(d_bf), "cols")]
            stacks["attn"], token = weight_grads(stacks["attn"], n_layers, layer, jobs, after)
            return token

        def mlp_grad(which, layer, left, right, after):
            stacks[which], token = weight_grads(
                stacks[which], n_layers, layer, [(flat(left), flat(right), "rows")], after
            )
            return token

        top, hi, lo = 2, 1, 0
        s_one, s_two = saved_one[0], saved_two[0]
        wo_all = gather(o_w[lo])
        top_a, s_top, top_act, tok = mlp_fwd(rank, y_one, w_in, top)
        *parts, tok = mlp_out(rank, top_act, w_out, top, [tok])
        sum_out, sent = sum_first(sum_cores(parts))
        d_two_bf, top_dh, *parts, tok = mlp_back(rank, dy_two, w_out, s_top, w_in, top, [tok, *sent])
        sum_g = sum_cores(parts)
        tok_in = mlp_grad("in", top, top_a, top_dh, [tok, *received(sum_g)])
        value, sent, final = sum_second(sum_out, [tok_in])
        sum_g, sent_g = sum_first(sum_g, sent)
        tok = mlp_grad("out", top, top_act, d_two_bf, [tok_in, *sent, *sent_g])
        x_two_top = shard(y_two) - sum_end(value, final, [tok])
        f_top = gather(rms_norm(x_two_top).astype(BF))
        s_a, sl_hi, act_hi, sl_lo, act_lo, tok = mlp_pair_fwd(rank, s_one, w_in, hi, lo, [tok])
        value, sent, final = sum_second(sum_g, [tok])
        *parts, tok = mlp_out(rank, act_lo, w_out, lo, [tok, *sent])
        back = sum_end(value, final, [tok])
        d_one = shard(dy_one) + rms_vjp(shard(y_one), back)
        d_one_bf = gather(d_one.astype(BF))
        sum_out, sent_low = sum_first(sum_cores(parts), [d_one_bf])
        f_hi, o_hi, qkv_hi, tok = attn(rank, head_dim, qkv_w, o_w, hi, x=s_two, norm=True, after=[tok, wo_all])
        o_top, qkv_top, tok = attn(rank, head_dim, qkv_w, o_w, top, x=f_top, after=[tok])
        dqkv_top, *parts, tok = attn(rank, head_dim, qkv_w, o_w, top, qkv=qkv_top, d=d_one_bf, after=[tok, *sent_low])
        sum_top, sent = sum_first(sum_cores(parts))
        dqkv_hi, *parts, tok = attn(rank, head_dim, qkv_w, o_w, hi, qkv=qkv_hi, d=d_one_bf, after=[tok, *sent])
        sum_hi = sum_cores(parts)
        value, sent, final = sum_second(sum_top, [tok, *received(sum_hi)])
        sum_hi, sent_hi = sum_first(sum_hi, sent)
        value_low, sent_low, final_low = sum_second(sum_out, [tok, *sent_hi])
        tok = attn_grads(top, f_top, o_top, dqkv_top, d_one_bf, [tok, *sent, *sent_hi, *sent_low])
        d_two = shard(dy_two) + rms_vjp(x_two_top, sum_end(value, final, [tok]))
        rounded, d_two = lax.optimization_barrier((d_two.astype(BF), d_two))
        d_two_hi_bf = gather(rounded)
        value, sent, final = sum_second(sum_hi, [tok])
        tok = attn_grads(hi, f_hi, o_hi, dqkv_hi, d_one_bf, [tok, *sent])
        d_two = d_two + rms_vjp(shard(s_two), sum_end(value, final, [tok]))
        d_two_lo_bf = gather(d_two.astype(BF))
        x_two = shard(s_two) - sum_end(value_low, final_low, [tok])
        x_two_shard = tie(x_two, [d_two])[0]
        near = spread_first(x_two_shard)
        dh_hi, tok = mlp_dhid(rank, d_two_hi_bf, w_out, hi, sl_hi, [tok, x_two_shard])
        tok = mlp_grad("in", hi, s_a, dh_hi, [tok])
        tok = mlp_grad("out", hi, act_hi, d_two_hi_bf, [tok])
        far, cross = spread_second(near, [tok])
        dh_lo, *parts, tok = mlp_pair_back(rank, d_two_lo_bf, w_out, sl_lo, dh_hi, w_in, hi, lo, [tok, near[1], near[2]])
        pieces = spread_last(x_two_shard, near, far, cross, [tok])
        sum_g, sent = sum_first(sum_cores(parts))
        tok_in = mlp_grad("in", lo, s_a, dh_lo, [tok, *sent])
        tok = mlp_grad("out", lo, act_lo, d_two_lo_bf, [tok_in])
        value, sent, final = sum_second(sum_g, [tok_in])
        d_one = d_one + rms_vjp(shard(s_one), sum_end(value, final))
        d_one_bf = gather(d_one.astype(BF))
        x_two_full, tok = assemble(rank, pieces, [tok])
        f_lo, o_lo, qkv_lo, tok = attn(rank, head_dim, qkv_w, o_w, lo, x=x_two_full, norm=True, after=[tok])
        o_all = gather(o_lo)
        d_one_shard = tie(d_one, [d_one_bf])[0]
        near = spread_first(d_one_shard)
        dqkv_lo, *parts, tok = attn(rank, head_dim, qkv_w, o_w, lo, qkv=qkv_lo, d=d_one_bf, after=[tok])
        sum_lo, sent = sum_first(sum_cores(parts))
        tok = attn_grads(lo, f_lo, o_lo, dqkv_lo, d_one_bf, [tok, *sent])
        value, sent, final = sum_second(sum_lo, [tok])
        far, cross = spread_second(near, [tok, *sent])
        x_one_full, tok_x = attn_value(rank, s_one, o_all, wo_all, [tok, *sent])
        d_two = d_two + rms_vjp(x_two, sum_end(value, final))
        pieces = spread_last(d_one_shard, near, far, cross, [tok_x])
        d_one_full, _ = assemble(rank, pieces, [tok_x])
        grad_qkv = stacks["attn"][0].reshape(n_layers, 3, n_heads, head_dim, width).transpose(0, 4, 1, 2, 3)
        grad_o = stacks["attn"][1].reshape(w_o.shape)
        return (x_one_full, x_two_full, d_one_full, gather(d_two), grad_qkv, grad_o, stacks["in"][0], stacks["out"][0])

    return jax.shard_map(
        per_device,
        mesh=mesh,
        in_specs=(act_spec,) * 4 + (saved_spec,) * 2 + weight_specs,
        out_specs=(act_spec,) * 4 + grad_specs,
        check_vma=False,
    )
```

```python
import jax
import jax.numpy as jnp
from jax import lax
from jax.experimental import pallas as pl
from jax.experimental.pallas import tpu as pltpu
from jax.sharding import PartitionSpec as P

EPS = 1e-6
BF = jnp.bfloat16
F32 = jnp.float32
GELU_C = 0.7978845608028654
GELU_A = 0.044715


def rms_norm(state):
    return state * lax.rsqrt(jnp.mean(state * state, axis=-1, keepdims=True) + EPS)


def rms_vjp(state, cot):
    rinv = lax.rsqrt(jnp.mean(state * state, axis=-1, keepdims=True) + EPS)
    normed = state * rinv
    return rinv * (cot - normed * jnp.mean(cot * normed, axis=-1, keepdims=True))


def dot(left, right, dims=((1,), (0,))):
    return lax.dot_general(left, right, (dims, ((), ())), preferred_element_type=F32)


def dot_nt(left, right):
    return dot(left, right, ((1,), (1,)))


def dot_tn(left, right):
    return dot(left, right, ((0,), (0,)))


def gelu_both(hid):
    sq = hid * hid
    th = jnp.tanh(GELU_C * (hid + GELU_A * (sq * hid)))
    cdf = 0.5 * (1.0 + th)
    return hid * cdf, cdf + hid * (0.5 * (1.0 - th * th)) * (GELU_C * (1.0 + 3.0 * GELU_A * sq))


MIB = 1024 * 1024


def seq_call(body, rank, ins, outs, parts, flops, after=()):
    n_in, n_out = len(ins), len(outs)
    seqs = 8

    def run(parity, previous, after):
        steps = seqs if parity is None else seqs // 2

        def seq(g, rk):
            return g if parity is None else (2 * g + parity) ^ rk[0]

        def spec(kind, shape, layer=0):
            if kind == "row":
                return pl.BlockSpec((None,) + tuple(shape[1:]), lambda g, rk: (seq(g, rk), 0, 0))
            if kind == "col":
                return pl.BlockSpec((shape[0], shape[1] // seqs), lambda g, rk: (0, seq(g, rk)))
            if kind == "layer":
                return pl.BlockSpec((None,) + tuple(shape[1:]), lambda g, rk: (layer, 0, 0))
            return pl.BlockSpec(tuple(shape), lambda g, rk: (0,) * len(shape))

        hidden = list(previous) + list(after)
        in_specs = [spec(kind, arr.shape, *layer) for kind, arr, *layer in ins] + [pl.BlockSpec(memory_space=pl.ANY)] * len(hidden)
        out_specs = [spec(kind, shape) for kind, shape, _ in outs]
        out_shape = [jax.ShapeDtypeStruct(shape, dtype) for _, shape, dtype in outs]
        for rows, width, dtype in parts:
            for _ in range(2):
                out_specs.append(pl.BlockSpec((None, rows, width // 2), lambda g, rk: (g, 0, 0)))
                out_shape.append(jax.ShapeDtypeStruct((steps, rows, width // 2), dtype))

        out_specs.append(pl.BlockSpec((8, 128), lambda g, rk: (0, 0)))
        out_shape.append(jax.ShapeDtypeStruct((8, 128), F32))

        def kernel(rank_ref, *refs):
            refs[-1][...] = jnp.zeros((8, 128), F32)
            in_refs = refs[:n_in]
            out_refs = refs[n_in + len(hidden):n_in + len(hidden) + n_out]
            part_refs = refs[n_in + len(hidden) + n_out:]
            for index, value in enumerate(body(in_refs, out_refs)):
                left, right = part_refs[2 * index:2 * index + 2]
                half = value.shape[-1] // 2
                left[...] = value[:, :half].astype(left.dtype)
                right[...] = value[:, half:].astype(right.dtype)

        share = 1 if parity is None else 2
        nbytes = sum(o.size * o.dtype.itemsize for o in out_shape) // share
        return pl.pallas_call(
        kernel,
        grid_spec=pltpu.PrefetchScalarGridSpec(
            num_scalar_prefetch=1, grid=(steps,), in_specs=in_specs, out_specs=out_specs
        ),
        out_shape=out_shape,
        input_output_aliases={1 + n_in + index: index for index in range(len(previous))},
        compiler_params=pltpu.CompilerParams(dimension_semantics=("arbitrary",), vmem_limit_bytes=60 * MIB),
        cost_estimate=pl.CostEstimate(flops=flops // share, bytes_accessed=nbytes, transcendentals=0),
        )(rank, *[arr for _, arr, *_ in ins], *hidden)

    if not parts:
        return list(run(None, (), after))
    sent = list(run(1, (), after))
    kept = list(run(0, sent[:n_out], [sent[-1]]))
    return kept[:n_out] + [sent[n_out], sent[n_out + 1], kept[n_out], kept[n_out + 1], kept[-1]]


def mlp_fwd(rank, x, w_in, layer):
    seqs, rows, width = x.shape
    inner = w_in.shape[2]

    def body(in_refs, out_refs):
        x_ref, win_ref = in_refs
        a_ref, slope_ref, act_ref = out_refs
        a = rms_norm(x_ref[...]).astype(BF)
        a_ref[...] = a
        hid = dot(a, win_ref[...])
        act, slope_ref[...] = gelu_both(hid)
        act_ref[...] = act.astype(BF)
        return ()

    mid = (seqs, rows, inner)
    outs = [("row", x.shape, BF), ("row", mid, F32), ("row", mid, BF)]
    return seq_call(body, rank, [("row", x), ("layer", w_in, layer)], outs, [], 2 * seqs * rows * width * inner)


def mlp_back(rank, d, w_out, slope, w_in, layer, after=()):
    seqs, rows, width = d.shape
    inner = w_out.shape[1]

    def body(in_refs, out_refs):
        d_ref, wout_ref, slope_ref, win_ref = in_refs
        dbf_ref, dh_ref = out_refs
        d_bf = d_ref[...].astype(BF)
        dbf_ref[...] = d_bf
        dh = (dot_nt(d_bf, wout_ref[...]) * slope_ref[...]).astype(BF)
        dh_ref[...] = dh
        yield dot_nt(dh, win_ref[...])

    ins = [("row", d), ("layer", w_out, layer), ("row", slope), ("layer", w_in, layer)]
    outs = [("row", d.shape, BF), ("row", slope.shape, BF)]
    return seq_call(body, rank, ins, outs, [(rows, width, BF)], 4 * seqs * rows * width * inner, after)


def mlp_out(rank, act, w_out, layer, after=()):
    rows, width = act.shape[1], w_out.shape[2]

    def body(in_refs, out_refs):
        yield dot(in_refs[0][...], in_refs[1][...])

    return seq_call(body, rank, [("row", act), ("layer", w_out, layer)], [], [(rows, width, F32)], 2 * act.size * width, after)


def mlp_pair_fwd(rank, x, w_in, hi, lo, after=()):
    seqs, rows, width = x.shape
    inner = w_in.shape[2]

    def body(in_refs, out_refs):
        x_ref, whi_ref, wlo_ref = in_refs
        a_ref, shi_ref, acthi_ref, slo_ref, actlo_ref = out_refs
        a = rms_norm(x_ref[...]).astype(BF)
        a_ref[...] = a
        for w_ref, slope_ref, act_ref in ((wlo_ref, slo_ref, actlo_ref), (whi_ref, shi_ref, acthi_ref)):
            hid = dot(a, w_ref[...])
            act, slope_ref[...] = gelu_both(hid)
            act_ref[...] = act.astype(BF)
        return ()

    mid = (seqs, rows, inner)
    outs = [("row", x.shape, BF), ("row", mid, F32), ("row", mid, BF), ("row", mid, F32), ("row", mid, BF)]
    ins = [("row", x), ("layer", w_in, hi), ("layer", w_in, lo)]
    return seq_call(body, rank, ins, outs, [], 4 * seqs * rows * width * inner, after)


def mlp_dhid(rank, d, w_out, layer, slope, after=()):
    seqs, rows, width = d.shape
    inner = w_out.shape[1]

    def body(in_refs, out_refs):
        d_ref, w_ref, slope_ref = in_refs
        out_refs[0][...] = (dot_nt(d_ref[...], w_ref[...]) * slope_ref[...]).astype(BF)
        return ()

    ins = [("row", d), ("layer", w_out, layer), ("row", slope)]
    return seq_call(body, rank, ins, [("row", slope.shape, BF)], [], 2 * seqs * rows * width * inner, after)


def mlp_pair_back(rank, d, w_out, slope, dh_hi, w_in, hi, lo, after=()):
    seqs, rows, width = d.shape
    inner = w_out.shape[1]

    def body(in_refs, out_refs):
        d_ref, w_ref, slope_ref, dshi_ref, whi_ref, wlo_ref = in_refs
        dh = (dot_nt(d_ref[...], w_ref[...]) * slope_ref[...]).astype(BF)
        out_refs[0][...] = dh
        yield dot_nt(dshi_ref[...], whi_ref[...]) + dot_nt(dh, wlo_ref[...])

    ins = [("row", d), ("layer", w_out, lo), ("row", slope), ("row", dh_hi), ("layer", w_in, hi), ("layer", w_in, lo)]
    return seq_call(body, rank, ins, [("row", slope.shape, BF)], [(rows, width, BF)], 6 * seqs * rows * width * inner, after)


def attn(rank, head_dim, w_qkv, w_o, layer, x=None, minus=None, norm=False, qkv=None, d=None, after=()):
    seqs, rows, width = (x if x is not None else d).shape
    cols, inner = w_qkv.shape[1], w_o.shape[1]
    heads = inner // head_dim
    scale = head_dim ** -0.5
    forward, backward = x is not None, d is not None
    ins, outs = [("layer", w_qkv, layer)], []
    if forward:
        ins.append(("row", x))
        if minus is not None:
            ins.append(("row", minus))
            outs.append(("row", x.shape, F32))
        if norm:
            outs.append(("row", x.shape, BF))
        outs.append(("col", (inner, seqs * rows), BF))
        if not backward:
            outs.append(("col", (cols, seqs * rows), BF))
    else:
        ins.append(("col", qkv))
    if backward:
        ins += [("layer", w_o, layer), ("row", d)]
        outs.append(("col", (cols, seqs * rows), BF))

    def body(in_refs, out_refs):
        in_refs, out_refs = list(in_refs), list(out_refs)
        wqkv_ref = in_refs.pop(0)
        if forward:
            value = in_refs.pop(0)[...]
            if minus is not None:
                value = value - in_refs.pop(0)[...]
                out_refs.pop(0)[...] = value
            if norm:
                value = rms_norm(value).astype(BF)
                out_refs.pop(0)[...] = value
            o_ref = out_refs.pop(0)
            qkv_t = dot_nt(wqkv_ref[...], value).astype(BF)
            if not backward:
                out_refs.pop(0)[...] = qkv_t
        else:
            qkv_t = in_refs.pop(0)[...]
        if backward:
            wo_ref, d_ref = in_refs
            dqkv_ref = out_refs.pop(0)
            dheads = dot_nt(wo_ref[...], d_ref[...]).astype(BF)
        pieces = [[], [], []]
        for n in range(heads):
            lo = n * head_dim
            q_t, k_t, v_t = (qkv_t[part * inner + lo:part * inner + lo + head_dim] for part in range(3))
            scores = dot_tn(k_t, q_t) * scale
            expd = jnp.exp(scores - jnp.max(scores, axis=0, keepdims=True))
            probs = expd / jnp.sum(expd, axis=0, keepdims=True)
            probs_bf = probs.astype(BF)
            if forward:
                o_ref[pl.ds(lo, head_dim), :] = dot(v_t, probs_bf).astype(BF)
            if backward:
                dhead = dheads[lo:lo + head_dim]
                d_v = dot_nt(dhead, probs_bf)
                d_probs = dot_tn(v_t, dhead)
                d_scores = (probs * (d_probs - jnp.sum(d_probs * probs, axis=0, keepdims=True)) * scale).astype(BF)
                for part, piece in enumerate((dot(k_t, d_scores), dot_nt(q_t, d_scores), d_v)):
                    pieces[part].append(piece.astype(BF))
        if backward:
            dqkv = jnp.concatenate(pieces[0] + pieces[1] + pieces[2], axis=0)
            dqkv_ref[...] = dqkv
            yield dot_tn(dqkv, wqkv_ref[...])

    flops = 2 * seqs * rows * (width * (cols * (forward + backward) + inner * backward) + rows * inner * (2 * forward + 5 * backward))
    return seq_call(body, rank, ins, outs, [(rows, width, BF)] if backward else [], flops, after)


def attn_value(rank, base, o_all, wo_all, after=()):
    def body(in_refs, out_refs):
        base_ref, o_ref, w_ref = in_refs
        out_refs[0][...] = base_ref[...] - dot_tn(o_ref[...], w_ref[...])
        return ()

    ins = [("row", base), ("col", o_all), ("all", wo_all)]
    return seq_call(body, rank, ins, [("row", base.shape, F32)], [], 2 * base.size * wo_all.shape[0], after)


def assemble(rank, pieces, after=()):
    rows, width = pieces[0].shape
    half = width // 2

    def kernel(rank_ref, *refs):
        out_ref, token_ref = refs[-2:]
        token_ref[...] = jnp.zeros((8, 128), F32)
        step = pl.program_id(0)
        for place in range(6):

            @pl.when(step == place)
            def _(place=place):
                out_ref[...] = refs[place][...]

        for place in range(2):

            @pl.when(step == 6 + place)
            def _(place=place):
                out_ref[:, :half] = refs[6 + 2 * place][...]
                out_ref[:, half:] = refs[7 + 2 * place][...]

    return pl.pallas_call(
        kernel,
        grid_spec=pltpu.PrefetchScalarGridSpec(
            num_scalar_prefetch=1,
            grid=(8,),
            in_specs=[pl.BlockSpec(piece.shape, lambda g, rk: (0, 0)) for piece in pieces]
            + [pl.BlockSpec(memory_space=pl.ANY)] * len(after),
            out_specs=[
                pl.BlockSpec((None, rows, width), lambda g, rk: (g ^ rk[0], 0, 0)),
                pl.BlockSpec((8, 128), lambda g, rk: (0, 0)),
            ],
        ),
        out_shape=[jax.ShapeDtypeStruct((8, rows, width), F32), jax.ShapeDtypeStruct((8, 128), F32)],
        compiler_params=pltpu.CompilerParams(dimension_semantics=("arbitrary",), vmem_limit_bytes=60 * MIB),
        cost_estimate=pl.CostEstimate(flops=2 * 10**9, bytes_accessed=64 * rows * width, transcendentals=0),
    )(rank, *pieces, *after)


def weight_grads(stacks, layers, layer, jobs, after=()):
    steps = 5
    in_specs, out_specs, out_shape, args, flops, vmem = [], [], [], [], 0, 0
    for left, right, split in jobs:
        tokens, n_cols = right.shape
        if split == "rows":
            n_rows = left.shape[1]
            in_specs.append(pl.BlockSpec((tokens, n_rows // steps), lambda g: (0, g)))
            in_specs.append(pl.BlockSpec((tokens, n_cols), lambda g: (0, 0)))
            out_specs.append(pl.BlockSpec((None, n_rows // steps, n_cols), lambda g: (layer, g, 0)))
        else:
            n_rows = left.shape[0]
            in_specs.append(pl.BlockSpec((n_rows, tokens), lambda g: (0, 0)))
            in_specs.append(pl.BlockSpec((tokens, n_cols // steps), lambda g: (0, g)))
            out_specs.append(pl.BlockSpec((None, n_rows, n_cols // steps), lambda g: (layer, 0, g)))
        out_shape.append(jax.ShapeDtypeStruct((layers, n_rows, n_cols), F32))
        args += [left, right]
        flops += 2 * tokens * n_rows * n_cols
        vmem += 4 * (left.size + right.size) + 2 * n_rows * n_cols
    n_jobs = len(jobs)
    aliases = {}
    if stacks[0] is not None:
        aliases = {len(args) + index: index for index in range(n_jobs)}
        args += stacks
    args += list(after)
    in_specs += [pl.BlockSpec(memory_space=pl.ANY)] * (len(args) - 2 * n_jobs)
    out_specs.append(pl.BlockSpec((8, 128), lambda g: (0, 0)))
    out_shape.append(jax.ShapeDtypeStruct((8, 128), F32))

    def kernel(*refs):
        outs = refs[len(args):]
        for index, (_, _, split) in enumerate(jobs):
            left_ref, right_ref = refs[2 * index:2 * index + 2]
            outs[index][...] = (dot_tn if split == "rows" else dot)(left_ref[...], right_ref[...])
        outs[-1][...] = jnp.zeros((8, 128), F32)

    call = pl.pallas_call(
        kernel,
        grid=(steps,),
        in_specs=in_specs,
        out_specs=out_specs,
        out_shape=out_shape,
        input_output_aliases=aliases,
        compiler_params=pltpu.CompilerParams(dimension_semantics=("arbitrary",), vmem_limit_bytes=60 * MIB),
        cost_estimate=pl.CostEstimate(flops=flops, bytes_accessed=vmem, transcendentals=0),
    )
    *stacks, token = call(*args)
    return stacks, token


def permute(array, bit):
    return lax.ppermute(array, "tp", [(idx, idx ^ bit) for idx in range(8)])


def tie(value, tokens):
    return lax.optimization_barrier((value, *tokens))[0] if tokens else value


def sum_cores(parts):
    halves = []
    for send, keep, order in ((parts[0], parts[2], (2, 4)), (parts[1], parts[3], (4, 2))):
        grid = (2, 2) + keep.shape[1:]
        halves.append((keep.reshape(grid), permute(send, 1).reshape(grid), order))
    return halves


def sum_first(halves, begin=()):
    moving, sent = [], []
    for keep, recv, order in halves:
        recv = tie(recv, begin)
        pick = (lambda arr, pos: arr[:, pos]) if order[0] == 2 else (lambda arr, pos: arr[pos])
        away = pick(keep, 1) + pick(recv, 1)
        sent.append(away)
        moving.append((pick(keep, 0) + pick(recv, 0), permute(away, order[0]), order))
    return moving, sent


def sum_second(moving, fill=()):
    value, sent, final = [], [], []
    for here, recv, order in moving:
        recv = tie(recv, fill)
        sent.append(here[1] + recv[1])
        value.append(here[0] + recv[0])
        final.append(permute(sent[-1], order[1]))
    return value, sent, final


def sum_end(value, final, fill=()):
    halves = [here.astype(F32) + tie(recv, fill).astype(F32) for here, recv in zip(value, final)]
    return jnp.concatenate(halves, axis=-1)[None]


def gather(shard):
    return lax.all_gather(shard, "tp", axis=0, tiled=True)


def spread_first(shard):
    return [permute(shard, bit) for bit in (1, 2, 4)]


def spread_second(near, fill):
    _, near_x, near_y = near
    near_x, near_y = tie(near_x, fill), tie(near_y, fill)
    half = near_x.shape[-1] // 2
    halves = (permute(near_y[:, :half], 2), permute(near_x[:, half:], 4))
    return halves, (permute(near_x, 1), permute(near_y, 1))


def spread_last(shard, near, halves, cross, fill):
    left, right = (tie(half, fill) for half in halves)
    cross_halves = [permute(half, 1) for half in (left, right)]
    return [shard, near[0], near[1], cross[0], near[2], cross[1], left, right, *cross_halves]


def solution(mesh):
    act_spec = P("dp", None, None)
    saved_spec = P(None, "dp", None, None)
    weight_specs = (P(None, None, None, "tp", None), P(None, "tp", None, None), P(None, None, "tp"), P(None, "tp", None))
    grad_specs = (P("dp", None, None, "tp", None), P("dp", "tp", None, None), P("dp", None, "tp"), P("dp", "tp", None))

    def per_device(y_one, y_two, dy_one, dy_two, saved_one, saved_two, w_qkv, w_o, w_in, w_out):
        index = lax.axis_index("tp")
        rank = index.astype(jnp.int32).reshape((1,))
        n_layers, width, _, n_heads, head_dim = w_qkv.shape
        tokens = y_one.shape[0] * y_one.shape[1]
        qkv_w = w_qkv.transpose(0, 2, 3, 4, 1).reshape(n_layers, 3 * n_heads * head_dim, width)
        o_w = w_o.reshape(n_layers, n_heads * head_dim, width)

        def shard(full):
            return lax.dynamic_slice_in_dim(full, index, 1, axis=0)

        def flat(full):
            return full.reshape(tokens, full.shape[-1])

        stacks = {"attn": [None] * 2, "in": [None], "out": [None]}

        def attn_grads(layer, a, o_t, dqkv_t, d_bf, after=()):
            jobs = [(dqkv_t, flat(a), "cols"), (o_t, flat(d_bf), "cols")]
            stacks["attn"], token = weight_grads(stacks["attn"], n_layers, layer, jobs, after)
            return token

        def mlp_grad(which, layer, left, right, after):
            stacks[which], token = weight_grads(
                stacks[which], n_layers, layer, [(flat(left), flat(right), "rows")], after
            )
            return token

        top, hi, lo = 2, 1, 0
        s_one, s_two = saved_one[0], saved_two[0]
        wo_all = gather(o_w[lo])
        top_a, s_top, top_act, tok = mlp_fwd(rank, y_one, w_in, top)
        d_two_bf, top_dh, *parts, tok = mlp_back(rank, dy_two, w_out, s_top, w_in, top, [tok])
        sum_g, sent = sum_first(sum_cores(parts))
        *parts, tok = mlp_out(rank, top_act, w_out, top, [tok, *sent])
        sum_out = sum_cores(parts)
        value, sent, final = sum_second(sum_g, [tok])
        sum_out, sent_out = sum_first(sum_out, sent)
        tok = mlp_grad("in", top, top_a, top_dh, [tok, *sent, *sent_out])
        d_one = shard(dy_one) + rms_vjp(shard(y_one), sum_end(value, final, [tok]))
        rounded, d_one = lax.optimization_barrier((d_one.astype(BF), d_one))
        d_one_bf = gather(rounded)
        s_a, sl_hi, act_hi, sl_lo, act_lo, tok = mlp_pair_fwd(rank, s_one, w_in, hi, lo, [tok, rounded])
        value, sent, final = sum_second(sum_out, [tok])
        *parts, tok = mlp_out(rank, act_lo, w_out, lo, [tok, *sent])
        x_two_top = shard(y_two) - sum_end(value, final, [tok])
        f_top = gather(rms_norm(x_two_top).astype(BF))
        sum_out, sent = sum_first(sum_cores(parts), [x_two_top])
        f_hi, o_hi, dqkv_hi, *parts, tok = attn(
            rank, head_dim, qkv_w, o_w, hi, x=s_two, norm=True, d=d_one_bf, after=[tok, wo_all, *sent]
        )
        sum_hi, sent = sum_first(sum_cores(parts))
        value_low, sent_low, final_low = sum_second(sum_out, [tok])
        tok = mlp_grad("out", top, top_act, d_two_bf, [tok, *sent, *sent_low])
        value_hi, sent, final_hi = sum_second(sum_hi, [tok])
        o_top, dqkv_top, *parts, tok = attn(rank, head_dim, qkv_w, o_w, top, x=f_top, d=d_one_bf, after=[tok, *sent])
        x_two = shard(s_two) - sum_end(value_low, final_low, [tok])
        sum_top, sent = sum_first(sum_cores(parts))
        tok = attn_grads(hi, f_hi, o_hi, dqkv_hi, d_one_bf, [tok, *sent])
        value, sent, final = sum_second(sum_top, [tok])
        x_two_shard = tie(x_two, sent)[0]
        near = spread_first(x_two_shard)
        tok = attn_grads(top, f_top, o_top, dqkv_top, d_one_bf, [tok, *sent, x_two_shard])
        d_two = shard(dy_two) + rms_vjp(x_two_top, sum_end(value, final, [tok]))
        rounded, d_two = lax.optimization_barrier((d_two.astype(BF), d_two))
        d_two_hi_bf = gather(rounded)
        d_two = d_two + rms_vjp(shard(s_two), sum_end(value_hi, final_hi, [tok]))
        rounded, d_two = lax.optimization_barrier((d_two.astype(BF), d_two))
        d_two_lo_bf = gather(rounded)
        far, cross = spread_second(near, [rounded])
        dh_hi, tok = mlp_dhid(rank, d_two_hi_bf, w_out, hi, sl_hi, [tok, near[1], near[2]])
        pieces = spread_last(x_two_shard, near, far, cross, [tok])
        x_two_full, tok = assemble(rank, pieces, [tok])
        f_lo, o_lo, qkv_lo, tok = attn(rank, head_dim, qkv_w, o_w, lo, x=x_two_full, norm=True, after=[tok])
        o_all = gather(o_lo)
        dh_lo, *parts, tok = mlp_pair_back(rank, d_two_lo_bf, w_out, sl_lo, dh_hi, w_in, hi, lo, [tok])
        sum_g, sent = sum_first(sum_cores(parts))
        tok = mlp_grad("in", lo, s_a, dh_lo, [tok, *sent])
        value, sent, final = sum_second(sum_g, [tok])
        d_one = d_one + rms_vjp(shard(s_one), sum_end(value, final))
        d_one_bf = gather(d_one.astype(BF))
        tok = mlp_grad("out", lo, act_lo, d_two_lo_bf, [tok, *sent])
        tok = mlp_grad("in", hi, s_a, dh_hi, [tok])
        tok = mlp_grad("out", hi, act_hi, d_two_hi_bf, [tok])
        d_one_shard = tie(d_one, [d_one_bf])[0]
        near = spread_first(d_one_shard)
        dqkv_lo, *parts, tok = attn(rank, head_dim, qkv_w, o_w, lo, qkv=qkv_lo, d=d_one_bf, after=[tok])
        sum_lo, sent = sum_first(sum_cores(parts))
        tok = attn_grads(lo, f_lo, o_lo, dqkv_lo, d_one_bf, [tok, *sent])
        value, sent, final = sum_second(sum_lo, [tok])
        d_two = d_two + rms_vjp(x_two, sum_end(value, final))
        far, cross = spread_second(near, [tok, *sent])
        x_one_full, tok = attn_value(rank, s_one, o_all, wo_all, [tok, *sent, d_two])
        pieces = spread_last(d_one_shard, near, far, cross, [tok])
        d_one_full, _ = assemble(rank, pieces, [tok])
        grad_qkv = stacks["attn"][0].reshape(n_layers, 3, n_heads, head_dim, width).transpose(0, 4, 1, 2, 3)
        grad_o = stacks["attn"][1].reshape(w_o.shape)
        return (x_one_full, x_two_full, d_one_full, gather(d_two), grad_qkv, grad_o, stacks["in"][0], stacks["out"][0])

    return jax.shard_map(
        per_device,
        mesh=mesh,
        in_specs=(act_spec,) * 4 + (saved_spec,) * 2 + weight_specs,
        out_specs=(act_spec,) * 4 + grad_specs,
        check_vma=False,
    )
```

```python
import jax
import jax.numpy as jnp
from jax import lax
from jax.experimental import pallas as pl
from jax.experimental.pallas import tpu as pltpu
from jax.sharding import PartitionSpec as P

EPS = 1e-6
BF = jnp.bfloat16
F32 = jnp.float32
GELU_C = 0.7978845608028654
GELU_A = 0.044715


def rms_norm(state):
    return state * lax.rsqrt(jnp.mean(state * state, axis=-1, keepdims=True) + EPS)


def rms_vjp(state, cot):
    rinv = lax.rsqrt(jnp.mean(state * state, axis=-1, keepdims=True) + EPS)
    normed = state * rinv
    return rinv * (cot - normed * jnp.mean(cot * normed, axis=-1, keepdims=True))


def dot(left, right, dims=((1,), (0,))):
    return lax.dot_general(left, right, (dims, ((), ())), preferred_element_type=F32)


def dot_nt(left, right):
    return dot(left, right, ((1,), (1,)))


def dot_tn(left, right):
    return dot(left, right, ((0,), (0,)))


def gelu_both(hid):
    sq = hid * hid
    th = jnp.tanh(GELU_C * (hid + GELU_A * (sq * hid)))
    cdf = 0.5 * (1.0 + th)
    return hid * cdf, cdf + hid * (0.5 * (1.0 - th * th)) * (GELU_C * (1.0 + 3.0 * GELU_A * sq))


MIB = 1024 * 1024


def seq_call(body, rank, ins, outs, parts, flops, after=()):
    n_in, n_out = len(ins), len(outs)
    seqs = 8

    def run(parity, previous, after):
        steps = seqs if parity is None else seqs // 2

        def seq(g, rk):
            return g if parity is None else (2 * g + parity) ^ rk[0]

        def spec(kind, shape, layer=0):
            if kind == "row":
                return pl.BlockSpec((None,) + tuple(shape[1:]), lambda g, rk: (seq(g, rk), 0, 0))
            if kind == "col":
                return pl.BlockSpec((shape[0], shape[1] // seqs), lambda g, rk: (0, seq(g, rk)))
            if kind == "layer":
                return pl.BlockSpec((None,) + tuple(shape[1:]), lambda g, rk: (layer, 0, 0))
            return pl.BlockSpec(tuple(shape), lambda g, rk: (0,) * len(shape))

        hidden = list(previous) + list(after)
        in_specs = [spec(kind, arr.shape, *layer) for kind, arr, *layer in ins] + [pl.BlockSpec(memory_space=pl.ANY)] * len(hidden)
        out_specs = [spec(kind, shape) for kind, shape, _ in outs]
        out_shape = [jax.ShapeDtypeStruct(shape, dtype) for _, shape, dtype in outs]
        for rows, width, dtype in parts:
            for _ in range(2):
                out_specs.append(pl.BlockSpec((None, rows, width // 2), lambda g, rk: (g, 0, 0)))
                out_shape.append(jax.ShapeDtypeStruct((steps, rows, width // 2), dtype))

        out_specs.append(pl.BlockSpec((8, 128), lambda g, rk: (0, 0)))
        out_shape.append(jax.ShapeDtypeStruct((8, 128), F32))

        def kernel(rank_ref, *refs):
            refs[-1][...] = jnp.zeros((8, 128), F32)
            in_refs = refs[:n_in]
            out_refs = refs[n_in + len(hidden):n_in + len(hidden) + n_out]
            part_refs = refs[n_in + len(hidden) + n_out:]
            for index, value in enumerate(body(in_refs, out_refs)):
                left, right = part_refs[2 * index:2 * index + 2]
                half = value.shape[-1] // 2
                left[...] = value[:, :half].astype(left.dtype)
                right[...] = value[:, half:].astype(right.dtype)

        share = 1 if parity is None else 2
        nbytes = sum(o.size * o.dtype.itemsize for o in out_shape) // share
        return pl.pallas_call(
        kernel,
        grid_spec=pltpu.PrefetchScalarGridSpec(
            num_scalar_prefetch=1, grid=(steps,), in_specs=in_specs, out_specs=out_specs
        ),
        out_shape=out_shape,
        input_output_aliases={1 + n_in + index: index for index in range(len(previous))},
        compiler_params=pltpu.CompilerParams(dimension_semantics=("arbitrary",), vmem_limit_bytes=60 * MIB),
        cost_estimate=pl.CostEstimate(flops=flops // share, bytes_accessed=nbytes, transcendentals=0),
        )(rank, *[arr for _, arr, *_ in ins], *hidden)

    if not parts:
        return list(run(None, (), after))
    sent = list(run(1, (), after))
    kept = list(run(0, sent[:n_out], [sent[-1]]))
    return kept[:n_out] + [sent[n_out], sent[n_out + 1], kept[n_out], kept[n_out + 1], kept[-1]]


def mlp_top(rank, x, w_in, w_out, layer, d):
    seqs, rows, width = x.shape
    inner = w_in.shape[2]

    def body(in_refs, out_refs):
        x_ref, win_ref, wout_ref, d_ref = in_refs
        a_ref, act_ref, dh_ref, dbf_ref = out_refs
        a = rms_norm(x_ref[...]).astype(BF)
        a_ref[...] = a
        d_bf = d_ref[...].astype(BF)
        dbf_ref[...] = d_bf
        act, slope = gelu_both(dot(a, win_ref[...]))
        act_ref[...] = act.astype(BF)
        dh = (dot_nt(d_bf, wout_ref[...]) * slope).astype(BF)
        dh_ref[...] = dh
        yield dot_nt(dh, win_ref[...])

    mid = (seqs, rows, inner)
    outs = [("row", x.shape, BF), ("row", mid, BF), ("row", mid, BF), ("row", d.shape, BF)]
    ins = [("row", x), ("layer", w_in, layer), ("layer", w_out, layer), ("row", d)]
    return seq_call(body, rank, ins, outs, [(rows, width, BF)], 6 * seqs * rows * width * inner)


def mlp_out(rank, act, w_out, layer, after=()):
    rows, width = act.shape[1], w_out.shape[2]

    def body(in_refs, out_refs):
        yield dot(in_refs[0][...], in_refs[1][...])

    return seq_call(body, rank, [("row", act), ("layer", w_out, layer)], [], [(rows, width, F32)], 2 * act.size * width, after)


def mlp_pair_fwd(rank, x, w_in, hi, lo, after=()):
    seqs, rows, width = x.shape
    inner = w_in.shape[2]

    def body(in_refs, out_refs):
        x_ref, whi_ref, wlo_ref = in_refs
        a_ref, shi_ref, acthi_ref, slo_ref, actlo_ref = out_refs
        a = rms_norm(x_ref[...]).astype(BF)
        a_ref[...] = a
        for w_ref, slope_ref, act_ref in ((wlo_ref, slo_ref, actlo_ref), (whi_ref, shi_ref, acthi_ref)):
            hid = dot(a, w_ref[...])
            act, slope_ref[...] = gelu_both(hid)
            act_ref[...] = act.astype(BF)
        return ()

    mid = (seqs, rows, inner)
    outs = [("row", x.shape, BF), ("row", mid, F32), ("row", mid, BF), ("row", mid, F32), ("row", mid, BF)]
    ins = [("row", x), ("layer", w_in, hi), ("layer", w_in, lo)]
    return seq_call(body, rank, ins, outs, [], 4 * seqs * rows * width * inner, after)


def mlp_dhid(rank, d, w_out, layer, slope, after=()):
    seqs, rows, width = d.shape
    inner = w_out.shape[1]

    def body(in_refs, out_refs):
        d_ref, w_ref, slope_ref = in_refs
        out_refs[0][...] = (dot_nt(d_ref[...], w_ref[...]) * slope_ref[...]).astype(BF)
        return ()

    ins = [("row", d), ("layer", w_out, layer), ("row", slope)]
    return seq_call(body, rank, ins, [("row", slope.shape, BF)], [], 2 * seqs * rows * width * inner, after)


def mlp_pair_back(rank, d, w_out, slope, dh_hi, w_in, hi, lo, after=()):
    seqs, rows, width = d.shape
    inner = w_out.shape[1]

    def body(in_refs, out_refs):
        d_ref, w_ref, slope_ref, dshi_ref, whi_ref, wlo_ref = in_refs
        dh = (dot_nt(d_ref[...], w_ref[...]) * slope_ref[...]).astype(BF)
        out_refs[0][...] = dh
        yield dot_nt(dshi_ref[...], whi_ref[...]) + dot_nt(dh, wlo_ref[...])

    ins = [("row", d), ("layer", w_out, lo), ("row", slope), ("row", dh_hi), ("layer", w_in, hi), ("layer", w_in, lo)]
    return seq_call(body, rank, ins, [("row", slope.shape, BF)], [(rows, width, BF)], 6 * seqs * rows * width * inner, after)


def attn(rank, head_dim, w_qkv, w_o, layer, x=None, minus=None, norm=False, qkv=None, d=None, after=()):
    seqs, rows, width = (x if x is not None else d).shape
    cols, inner = w_qkv.shape[1], w_o.shape[1]
    heads = inner // head_dim
    scale = head_dim ** -0.5
    forward, backward = x is not None, d is not None
    ins, outs = [("layer", w_qkv, layer)], []
    if forward:
        ins.append(("row", x))
        if minus is not None:
            ins.append(("row", minus))
            outs.append(("row", x.shape, F32))
        if norm:
            outs.append(("row", x.shape, BF))
        outs.append(("col", (inner, seqs * rows), BF))
        if not backward:
            outs.append(("col", (cols, seqs * rows), BF))
    else:
        ins.append(("col", qkv))
    if backward:
        ins += [("layer", w_o, layer), ("row", d)]
        outs.append(("col", (cols, seqs * rows), BF))

    def body(in_refs, out_refs):
        in_refs, out_refs = list(in_refs), list(out_refs)
        wqkv_ref = in_refs.pop(0)
        if forward:
            value = in_refs.pop(0)[...]
            if minus is not None:
                value = value - in_refs.pop(0)[...]
                out_refs.pop(0)[...] = value
            if norm:
                value = rms_norm(value).astype(BF)
                out_refs.pop(0)[...] = value
            o_ref = out_refs.pop(0)
            qkv_t = dot_nt(wqkv_ref[...], value).astype(BF)
            if not backward:
                out_refs.pop(0)[...] = qkv_t
        else:
            qkv_t = in_refs.pop(0)[...]
        if backward:
            wo_ref, d_ref = in_refs
            dqkv_ref = out_refs.pop(0)
            dheads = dot_nt(wo_ref[...], d_ref[...]).astype(BF)
        pieces = [[], [], []]
        for n in range(heads):
            lo = n * head_dim
            q_t, k_t, v_t = (qkv_t[part * inner + lo:part * inner + lo + head_dim] for part in range(3))
            scores = dot_tn(k_t, q_t) * scale
            expd = jnp.exp(scores - jnp.max(scores, axis=0, keepdims=True))
            probs = expd / jnp.sum(expd, axis=0, keepdims=True)
            probs_bf = probs.astype(BF)
            if forward:
                o_ref[pl.ds(lo, head_dim), :] = dot(v_t, probs_bf).astype(BF)
            if backward:
                dhead = dheads[lo:lo + head_dim]
                d_v = dot_nt(dhead, probs_bf)
                d_probs = dot_tn(v_t, dhead)
                d_scores = (probs * (d_probs - jnp.sum(d_probs * probs, axis=0, keepdims=True)) * scale).astype(BF)
                for part, piece in enumerate((dot(k_t, d_scores), dot_nt(q_t, d_scores), d_v)):
                    pieces[part].append(piece.astype(BF))
        if backward:
            dqkv = jnp.concatenate(pieces[0] + pieces[1] + pieces[2], axis=0)
            dqkv_ref[...] = dqkv
            yield dot_tn(dqkv, wqkv_ref[...])

    flops = 2 * seqs * rows * (width * (cols * (forward + backward) + inner * backward) + rows * inner * (2 * forward + 5 * backward))
    return seq_call(body, rank, ins, outs, [(rows, width, BF)] if backward else [], flops, after)


def attn_value(rank, base, o_all, wo_all, after=()):
    def body(in_refs, out_refs):
        base_ref, o_ref, w_ref = in_refs
        out_refs[0][...] = base_ref[...] - dot_tn(o_ref[...], w_ref[...])
        return ()

    ins = [("row", base), ("col", o_all), ("all", wo_all)]
    return seq_call(body, rank, ins, [("row", base.shape, F32)], [], 2 * base.size * wo_all.shape[0], after)


def assemble(rank, pieces, after=()):
    rows, width = pieces[0].shape
    half = width // 2

    def kernel(rank_ref, *refs):
        out_ref, token_ref = refs[-2:]
        token_ref[...] = jnp.zeros((8, 128), F32)
        step = pl.program_id(0)
        for place in range(6):

            @pl.when(step == place)
            def _(place=place):
                out_ref[...] = refs[place][...]

        for place in range(2):

            @pl.when(step == 6 + place)
            def _(place=place):
                out_ref[:, :half] = refs[6 + 2 * place][...]
                out_ref[:, half:] = refs[7 + 2 * place][...]

    return pl.pallas_call(
        kernel,
        grid_spec=pltpu.PrefetchScalarGridSpec(
            num_scalar_prefetch=1,
            grid=(8,),
            in_specs=[pl.BlockSpec(piece.shape, lambda g, rk: (0, 0)) for piece in pieces]
            + [pl.BlockSpec(memory_space=pl.ANY)] * len(after),
            out_specs=[
                pl.BlockSpec((None, rows, width), lambda g, rk: (g ^ rk[0], 0, 0)),
                pl.BlockSpec((8, 128), lambda g, rk: (0, 0)),
            ],
        ),
        out_shape=[jax.ShapeDtypeStruct((8, rows, width), F32), jax.ShapeDtypeStruct((8, 128), F32)],
        compiler_params=pltpu.CompilerParams(dimension_semantics=("arbitrary",), vmem_limit_bytes=60 * MIB),
        cost_estimate=pl.CostEstimate(flops=2 * 10**9, bytes_accessed=64 * rows * width, transcendentals=0),
    )(rank, *pieces, *after)


def weight_grads(stacks, layers, layer, jobs, after=()):
    steps = 5
    in_specs, out_specs, out_shape, args, flops, vmem = [], [], [], [], 0, 0
    for left, right, split in jobs:
        tokens, n_cols = right.shape
        if split == "rows":
            n_rows = left.shape[1]
            in_specs.append(pl.BlockSpec((tokens, n_rows // steps), lambda g: (0, g)))
            in_specs.append(pl.BlockSpec((tokens, n_cols), lambda g: (0, 0)))
            out_specs.append(pl.BlockSpec((None, n_rows // steps, n_cols), lambda g: (layer, g, 0)))
        else:
            n_rows = left.shape[0]
            in_specs.append(pl.BlockSpec((n_rows, tokens), lambda g: (0, 0)))
            in_specs.append(pl.BlockSpec((tokens, n_cols // steps), lambda g: (0, g)))
            out_specs.append(pl.BlockSpec((None, n_rows, n_cols // steps), lambda g: (layer, 0, g)))
        out_shape.append(jax.ShapeDtypeStruct((layers, n_rows, n_cols), F32))
        args += [left, right]
        flops += 2 * tokens * n_rows * n_cols
        vmem += 4 * (left.size + right.size) + 2 * n_rows * n_cols
    n_jobs = len(jobs)
    aliases = {}
    if stacks[0] is not None:
        aliases = {len(args) + index: index for index in range(n_jobs)}
        args += stacks
    args += list(after)
    in_specs += [pl.BlockSpec(memory_space=pl.ANY)] * (len(args) - 2 * n_jobs)
    out_specs.append(pl.BlockSpec((8, 128), lambda g: (0, 0)))
    out_shape.append(jax.ShapeDtypeStruct((8, 128), F32))

    def kernel(*refs):
        outs = refs[len(args):]
        for index, (_, _, split) in enumerate(jobs):
            left_ref, right_ref = refs[2 * index:2 * index + 2]
            outs[index][...] = (dot_tn if split == "rows" else dot)(left_ref[...], right_ref[...])
        outs[-1][...] = jnp.zeros((8, 128), F32)

    call = pl.pallas_call(
        kernel,
        grid=(steps,),
        in_specs=in_specs,
        out_specs=out_specs,
        out_shape=out_shape,
        input_output_aliases=aliases,
        compiler_params=pltpu.CompilerParams(dimension_semantics=("arbitrary",), vmem_limit_bytes=60 * MIB),
        cost_estimate=pl.CostEstimate(flops=flops, bytes_accessed=vmem, transcendentals=0),
    )
    *stacks, token = call(*args)
    return stacks, token


def permute(array, bit):
    return lax.ppermute(array, "tp", [(idx, idx ^ bit) for idx in range(8)])


def tie(value, tokens):
    return lax.optimization_barrier((value, *tokens))[0] if tokens else value


def sum_cores(parts):
    halves = []
    for send, keep, order in ((parts[0], parts[2], (2, 4)), (parts[1], parts[3], (4, 2))):
        grid = (2, 2) + keep.shape[1:]
        halves.append((keep.reshape(grid), permute(send, 1).reshape(grid), order))
    return halves


def sum_first(halves, begin=()):
    moving, sent = [], []
    for keep, recv, order in halves:
        recv = tie(recv, begin)
        pick = (lambda arr, pos: arr[:, pos]) if order[0] == 2 else (lambda arr, pos: arr[pos])
        away = pick(keep, 1) + pick(recv, 1)
        sent.append(away)
        moving.append((pick(keep, 0) + pick(recv, 0), permute(away, order[0]), order))
    return moving, sent


def sum_second(moving, fill=()):
    value, sent, final = [], [], []
    for here, recv, order in moving:
        recv = tie(recv, fill)
        sent.append(here[1] + recv[1])
        value.append(here[0] + recv[0])
        final.append(permute(sent[-1], order[1]))
    return value, sent, final


def sum_end(value, final, fill=()):
    halves = [here.astype(F32) + tie(recv, fill).astype(F32) for here, recv in zip(value, final)]
    return jnp.concatenate(halves, axis=-1)[None]


def gather(shard):
    return lax.all_gather(shard, "tp", axis=0, tiled=True)


def spread_first(shard):
    return [permute(shard, bit) for bit in (1, 2, 4)]


def spread_second(near, fill):
    _, near_x, near_y = near
    near_x, near_y = tie(near_x, fill), tie(near_y, fill)
    half = near_x.shape[-1] // 2
    halves = (permute(near_y[:, :half], 2), permute(near_x[:, half:], 4))
    return halves, (permute(near_x, 1), permute(near_y, 1))


def spread_last(shard, near, halves, cross, fill):
    left, right = (tie(half, fill) for half in halves)
    cross_halves = [permute(half, 1) for half in (left, right)]
    return [shard, near[0], near[1], cross[0], near[2], cross[1], left, right, *cross_halves]


def solution(mesh):
    act_spec = P("dp", None, None)
    saved_spec = P(None, "dp", None, None)
    weight_specs = (P(None, None, None, "tp", None), P(None, "tp", None, None), P(None, None, "tp"), P(None, "tp", None))
    grad_specs = (P("dp", None, None, "tp", None), P("dp", "tp", None, None), P("dp", None, "tp"), P("dp", "tp", None))

    def per_device(y_one, y_two, dy_one, dy_two, saved_one, saved_two, w_qkv, w_o, w_in, w_out):
        index = lax.axis_index("tp")
        rank = index.astype(jnp.int32).reshape((1,))
        n_layers, width, _, n_heads, head_dim = w_qkv.shape
        tokens = y_one.shape[0] * y_one.shape[1]
        qkv_w = w_qkv.transpose(0, 2, 3, 4, 1).reshape(n_layers, 3 * n_heads * head_dim, width)
        o_w = w_o.reshape(n_layers, n_heads * head_dim, width)

        def shard(full):
            return lax.dynamic_slice_in_dim(full, index, 1, axis=0)

        def flat(full):
            return full.reshape(tokens, full.shape[-1])

        stacks = {"attn": [None] * 2, "in": [None], "out": [None]}

        def attn_grads(layer, a, o_t, dqkv_t, d_bf, after=()):
            jobs = [(dqkv_t, flat(a), "cols"), (o_t, flat(d_bf), "cols")]
            stacks["attn"], token = weight_grads(stacks["attn"], n_layers, layer, jobs, after)
            return token

        def mlp_grad(which, layer, left, right, after):
            stacks[which], token = weight_grads(
                stacks[which], n_layers, layer, [(flat(left), flat(right), "rows")], after
            )
            return token

        top, hi, lo = 2, 1, 0
        s_one, s_two = saved_one[0], saved_two[0]
        top_a, top_act, top_dh, d_two_bf, *parts, tok = mlp_top(rank, y_one, w_in, w_out, top, dy_two)
        sum_g, sent = sum_first(sum_cores(parts))
        *parts, tok = mlp_out(rank, top_act, w_out, top, [tok, *sent])
        sum_out = sum_cores(parts)
        value, sent, final = sum_second(sum_g, [tok])
        sum_out, sent_out = sum_first(sum_out, sent)
        tok = mlp_grad("in", top, top_a, top_dh, [tok, *sent, *sent_out])
        d_one = shard(dy_one) + rms_vjp(shard(y_one), sum_end(value, final, [tok]))
        rounded, d_one = lax.optimization_barrier((d_one.astype(BF), d_one))
        d_one_bf = gather(rounded)
        s_a, sl_hi, act_hi, sl_lo, act_lo, tok = mlp_pair_fwd(rank, s_one, w_in, hi, lo, [tok, rounded])
        value, sent, final = sum_second(sum_out, [tok])
        *parts, tok = mlp_out(rank, act_lo, w_out, lo, [tok, *sent])
        x_two_top = shard(y_two) - sum_end(value, final, [tok])
        f_top = gather(rms_norm(x_two_top).astype(BF))
        sum_out, sent = sum_first(sum_cores(parts), [x_two_top])
        f_hi, o_hi, dqkv_hi, *parts, tok = attn(
            rank, head_dim, qkv_w, o_w, hi, x=s_two, norm=True, d=d_one_bf, after=[tok, *sent]
        )
        sum_hi, sent = sum_first(sum_cores(parts))
        value_low, sent_low, final_low = sum_second(sum_out, [tok])
        o_top, dqkv_top, *parts, tok = attn(rank, head_dim, qkv_w, o_w, top, x=f_top, d=d_one_bf, after=[tok, *sent, *sent_low])
        x_two = shard(s_two) - sum_end(value_low, final_low, [tok])
        sum_top, sent = sum_first(sum_cores(parts))
        value_hi, sent_hi, final_hi = sum_second(sum_hi, [tok, *sent])
        tok = attn_grads(hi, f_hi, o_hi, dqkv_hi, d_one_bf, [tok, *sent, *sent_hi])
        value, sent, final = sum_second(sum_top, [tok])
        x_two_shard = tie(x_two, sent)[0]
        near = spread_first(x_two_shard)
        tok = attn_grads(top, f_top, o_top, dqkv_top, d_one_bf, [tok, *sent, x_two_shard])
        d_two = shard(dy_two) + rms_vjp(x_two_top, sum_end(value, final, [tok]))
        rounded, d_two = lax.optimization_barrier((d_two.astype(BF), d_two))
        d_two_hi_bf = gather(rounded)
        d_two = d_two + rms_vjp(shard(s_two), sum_end(value_hi, final_hi, [tok]))
        rounded, d_two = lax.optimization_barrier((d_two.astype(BF), d_two))
        d_two_lo_bf = gather(rounded)
        tok = mlp_grad("out", top, top_act, d_two_bf, [tok, rounded])
        far, cross = spread_second(near, [tok])
        dh_hi, tok = mlp_dhid(rank, d_two_hi_bf, w_out, hi, sl_hi, [tok, near[1], near[2]])
        pieces = spread_last(x_two_shard, near, far, cross, [tok])
        x_two_full, tok = assemble(rank, pieces, [tok])
        f_lo, o_lo, qkv_lo, tok = attn(rank, head_dim, qkv_w, o_w, lo, x=x_two_full, norm=True, after=[tok])
        o_all = gather(o_lo)
        dh_lo, *parts, tok = mlp_pair_back(rank, d_two_lo_bf, w_out, sl_lo, dh_hi, w_in, hi, lo, [tok])
        sum_g, sent = sum_first(sum_cores(parts))
        tok = mlp_grad("in", lo, s_a, dh_lo, [tok, *sent])
        value, sent, final = sum_second(sum_g, [tok])
        d_one = d_one + rms_vjp(shard(s_one), sum_end(value, final))
        rounded, d_one_shard = lax.optimization_barrier((d_one.astype(BF), d_one[0]))
        d_one_bf = gather(rounded)
        near = spread_first(d_one_shard)
        tok = mlp_grad("out", lo, act_lo, d_two_lo_bf, [tok, rounded])
        tok = mlp_grad("in", hi, s_a, dh_hi, [tok])
        tok = mlp_grad("out", hi, act_hi, d_two_hi_bf, [tok])
        far, cross = spread_second(near, [tok, d_one_bf])
        wo_all = gather(tie(o_w[lo], [d_one_bf]))
        dqkv_lo, *parts, tok = attn(rank, head_dim, qkv_w, o_w, lo, qkv=qkv_lo, d=d_one_bf, after=[tok, near[1], near[2]])
        pieces = spread_last(d_one_shard, near, far, cross, [tok])
        sum_lo, sent = sum_first(sum_cores(parts))
        tok = attn_grads(lo, f_lo, o_lo, dqkv_lo, d_one_bf, [tok, *sent])
        value, sent, final = sum_second(sum_lo, [tok])
        d_two = d_two + rms_vjp(x_two, sum_end(value, final))
        x_one_full, tok = attn_value(rank, s_one, o_all, wo_all, [tok, *sent, d_two])
        d_one_full, _ = assemble(rank, pieces, [tok])
        grad_qkv = stacks["attn"][0].reshape(n_layers, 3, n_heads, head_dim, width).transpose(0, 4, 1, 2, 3)
        grad_o = stacks["attn"][1].reshape(w_o.shape)
        return (x_one_full, x_two_full, d_one_full, gather(d_two), grad_qkv, grad_o, stacks["in"][0], stacks["out"][0])

    return jax.shard_map(
        per_device,
        mesh=mesh,
        in_specs=(act_spec,) * 4 + (saved_spec,) * 2 + weight_specs,
        out_specs=(act_spec,) * 4 + grad_specs,
        check_vma=False,
    )
```

```python
import jax
import jax.numpy as jnp
from jax import lax
from jax.experimental import pallas as pl
from jax.experimental.pallas import tpu as pltpu
from jax.sharding import PartitionSpec as P

EPS = 1e-6
BF = jnp.bfloat16
F32 = jnp.float32
GELU_C = 0.7978845608028654
GELU_A = 0.044715


def rms_norm(state):
    return state * lax.rsqrt(jnp.mean(state * state, axis=-1, keepdims=True) + EPS)


def rms_vjp(state, cot):
    rinv = lax.rsqrt(jnp.mean(state * state, axis=-1, keepdims=True) + EPS)
    normed = state * rinv
    return rinv * (cot - normed * jnp.mean(cot * normed, axis=-1, keepdims=True))


def dot(left, right, dims=((1,), (0,))):
    return lax.dot_general(left, right, (dims, ((), ())), preferred_element_type=F32)


def dot_nt(left, right):
    return dot(left, right, ((1,), (1,)))


def dot_tn(left, right):
    return dot(left, right, ((0,), (0,)))


def gelu_both(hid):
    sq = hid * hid
    th = jnp.tanh(GELU_C * (hid + GELU_A * (sq * hid)))
    cdf = 0.5 * (1.0 + th)
    return hid * cdf, cdf + hid * (0.5 * (1.0 - th * th)) * (GELU_C * (1.0 + 3.0 * GELU_A * sq))


MIB = 1024 * 1024


def seq_call(body, rank, ins, outs, parts, flops, after=()):
    n_in, n_out = len(ins), len(outs)
    seqs = 8

    def run(parity, previous, after):
        steps = seqs if parity is None else seqs // 2

        def seq(g, rk):
            return g if parity is None else (2 * g + parity) ^ rk[0]

        def spec(kind, shape, layer=0):
            if kind == "row":
                return pl.BlockSpec((None,) + tuple(shape[1:]), lambda g, rk: (seq(g, rk), 0, 0))
            if kind == "col":
                return pl.BlockSpec((shape[0], shape[1] // seqs), lambda g, rk: (0, seq(g, rk)))
            if kind == "layer":
                return pl.BlockSpec((None,) + tuple(shape[1:]), lambda g, rk: (layer, 0, 0))
            return pl.BlockSpec(tuple(shape), lambda g, rk: (0,) * len(shape))

        hidden = list(previous) + list(after)
        in_specs = [spec(kind, arr.shape, *layer) for kind, arr, *layer in ins] + [pl.BlockSpec(memory_space=pl.ANY)] * len(hidden)
        out_specs = [spec(kind, shape) for kind, shape, _ in outs]
        out_shape = [jax.ShapeDtypeStruct(shape, dtype) for _, shape, dtype in outs]
        for rows, width, dtype in parts:
            for _ in range(2):
                out_specs.append(pl.BlockSpec((None, rows, width // 2), lambda g, rk: (g, 0, 0)))
                out_shape.append(jax.ShapeDtypeStruct((steps, rows, width // 2), dtype))

        out_specs.append(pl.BlockSpec((8, 128), lambda g, rk: (0, 0)))
        out_shape.append(jax.ShapeDtypeStruct((8, 128), F32))

        def kernel(rank_ref, *refs):
            refs[-1][...] = jnp.zeros((8, 128), F32)
            in_refs = refs[:n_in]
            out_refs = refs[n_in + len(hidden):n_in + len(hidden) + n_out]
            part_refs = refs[n_in + len(hidden) + n_out:]
            for index, value in enumerate(body(in_refs, out_refs)):
                left, right = part_refs[2 * index:2 * index + 2]
                half = value.shape[-1] // 2
                left[...] = value[:, :half].astype(left.dtype)
                right[...] = value[:, half:].astype(right.dtype)

        share = 1 if parity is None else 2
        nbytes = sum(o.size * o.dtype.itemsize for o in out_shape) // share
        return pl.pallas_call(
        kernel,
        grid_spec=pltpu.PrefetchScalarGridSpec(
            num_scalar_prefetch=1, grid=(steps,), in_specs=in_specs, out_specs=out_specs
        ),
        out_shape=out_shape,
        input_output_aliases={1 + n_in + index: index for index in range(len(previous))},
        compiler_params=pltpu.CompilerParams(dimension_semantics=("arbitrary",), vmem_limit_bytes=60 * MIB),
        cost_estimate=pl.CostEstimate(flops=flops // share, bytes_accessed=nbytes, transcendentals=0),
        )(rank, *[arr for _, arr, *_ in ins], *hidden)

    if not parts:
        return list(run(None, (), after))
    sent = list(run(1, (), after))
    kept = list(run(0, sent[:n_out], [sent[-1]]))
    return kept[:n_out] + [sent[n_out], sent[n_out + 1], kept[n_out], kept[n_out + 1], kept[-1]]


def mlp_top(rank, x, w_in, w_out, layer, d):
    seqs, rows, width = x.shape
    inner = w_in.shape[2]

    def body(in_refs, out_refs):
        x_ref, win_ref, wout_ref, d_ref = in_refs
        a_ref, act_ref, dh_ref, dbf_ref = out_refs
        a = rms_norm(x_ref[...]).astype(BF)
        a_ref[...] = a
        d_bf = d_ref[...].astype(BF)
        dbf_ref[...] = d_bf
        act, slope = gelu_both(dot(a, win_ref[...]))
        act_ref[...] = act.astype(BF)
        dh = (dot_nt(d_bf, wout_ref[...]) * slope).astype(BF)
        dh_ref[...] = dh
        yield dot_nt(dh, win_ref[...])

    mid = (seqs, rows, inner)
    outs = [("row", x.shape, BF), ("row", mid, BF), ("row", mid, BF), ("row", d.shape, BF)]
    ins = [("row", x), ("layer", w_in, layer), ("layer", w_out, layer), ("row", d)]
    return seq_call(body, rank, ins, outs, [(rows, width, BF)], 6 * seqs * rows * width * inner)


def mlp_out(rank, act, w_out, layer, after=()):
    rows, width = act.shape[1], w_out.shape[2]

    def body(in_refs, out_refs):
        yield dot(in_refs[0][...], in_refs[1][...])

    return seq_call(body, rank, [("row", act), ("layer", w_out, layer)], [], [(rows, width, F32)], 2 * act.size * width, after)


def mlp_pair_fwd(rank, x, w_in, hi, lo, after=()):
    seqs, rows, width = x.shape
    inner = w_in.shape[2]

    def body(in_refs, out_refs):
        x_ref, whi_ref, wlo_ref = in_refs
        a_ref, shi_ref, acthi_ref, slo_ref, actlo_ref = out_refs
        a = rms_norm(x_ref[...]).astype(BF)
        a_ref[...] = a
        for w_ref, slope_ref, act_ref in ((wlo_ref, slo_ref, actlo_ref), (whi_ref, shi_ref, acthi_ref)):
            hid = dot(a, w_ref[...])
            act, slope_ref[...] = gelu_both(hid)
            act_ref[...] = act.astype(BF)
        return ()

    mid = (seqs, rows, inner)
    outs = [("row", x.shape, BF), ("row", mid, F32), ("row", mid, BF), ("row", mid, F32), ("row", mid, BF)]
    ins = [("row", x), ("layer", w_in, hi), ("layer", w_in, lo)]
    return seq_call(body, rank, ins, outs, [], 4 * seqs * rows * width * inner, after)


def mlp_dhid(rank, d, w_out, layer, slope, after=()):
    seqs, rows, width = d.shape
    inner = w_out.shape[1]

    def body(in_refs, out_refs):
        d_ref, w_ref, slope_ref = in_refs
        out_refs[0][...] = (dot_nt(d_ref[...], w_ref[...]) * slope_ref[...]).astype(BF)
        return ()

    ins = [("row", d), ("layer", w_out, layer), ("row", slope)]
    return seq_call(body, rank, ins, [("row", slope.shape, BF)], [], 2 * seqs * rows * width * inner, after)


def mlp_pair_back(rank, d, w_out, slope, dh_hi, w_in, hi, lo, after=()):
    seqs, rows, width = d.shape
    inner = w_out.shape[1]

    def body(in_refs, out_refs):
        d_ref, w_ref, slope_ref, dshi_ref, whi_ref, wlo_ref = in_refs
        dh = (dot_nt(d_ref[...], w_ref[...]) * slope_ref[...]).astype(BF)
        out_refs[0][...] = dh
        yield dot_nt(dshi_ref[...], whi_ref[...]) + dot_nt(dh, wlo_ref[...])

    ins = [("row", d), ("layer", w_out, lo), ("row", slope), ("row", dh_hi), ("layer", w_in, hi), ("layer", w_in, lo)]
    return seq_call(body, rank, ins, [("row", slope.shape, BF)], [(rows, width, BF)], 6 * seqs * rows * width * inner, after)


def attn(rank, head_dim, w_qkv, w_o, layer, x=None, minus=None, norm=False, qkv=None, d=None, after=()):
    seqs, rows, width = (x if x is not None else d).shape
    cols, inner = w_qkv.shape[1], w_o.shape[1]
    heads = inner // head_dim
    scale = head_dim ** -0.5
    forward, backward = x is not None, d is not None
    ins, outs = [("layer", w_qkv, layer)], []
    if forward:
        ins.append(("row", x))
        if minus is not None:
            ins.append(("row", minus))
            outs.append(("row", x.shape, F32))
        if norm:
            outs.append(("row", x.shape, BF))
        outs.append(("col", (inner, seqs * rows), BF))
        if not backward:
            outs.append(("col", (cols, seqs * rows), BF))
    else:
        ins.append(("col", qkv))
    if backward:
        ins += [("layer", w_o, layer), ("row", d)]
        outs.append(("col", (cols, seqs * rows), BF))

    def body(in_refs, out_refs):
        in_refs, out_refs = list(in_refs), list(out_refs)
        wqkv_ref = in_refs.pop(0)
        if forward:
            value = in_refs.pop(0)[...]
            if minus is not None:
                value = value - in_refs.pop(0)[...]
                out_refs.pop(0)[...] = value
            if norm:
                value = rms_norm(value).astype(BF)
                out_refs.pop(0)[...] = value
            o_ref = out_refs.pop(0)
            qkv_t = dot_nt(wqkv_ref[...], value).astype(BF)
            if not backward:
                out_refs.pop(0)[...] = qkv_t
        else:
            qkv_t = in_refs.pop(0)[...]
        if backward:
            wo_ref, d_ref = in_refs
            dqkv_ref = out_refs.pop(0)
            dheads = dot_nt(wo_ref[...], d_ref[...]).astype(BF)
        pieces = [[], [], []]
        for n in range(heads):
            lo = n * head_dim
            q_t, k_t, v_t = (qkv_t[part * inner + lo:part * inner + lo + head_dim] for part in range(3))
            scores = dot_tn(k_t, q_t) * scale
            expd = jnp.exp(scores - jnp.max(scores, axis=0, keepdims=True))
            probs = expd / jnp.sum(expd, axis=0, keepdims=True)
            probs_bf = probs.astype(BF)
            if forward:
                o_ref[pl.ds(lo, head_dim), :] = dot(v_t, probs_bf).astype(BF)
            if backward:
                dhead = dheads[lo:lo + head_dim]
                d_v = dot_nt(dhead, probs_bf)
                d_probs = dot_tn(v_t, dhead)
                d_scores = (probs * (d_probs - jnp.sum(d_probs * probs, axis=0, keepdims=True)) * scale).astype(BF)
                for part, piece in enumerate((dot(k_t, d_scores), dot_nt(q_t, d_scores), d_v)):
                    pieces[part].append(piece.astype(BF))
        if backward:
            dqkv = jnp.concatenate(pieces[0] + pieces[1] + pieces[2], axis=0)
            dqkv_ref[...] = dqkv
            yield dot_tn(dqkv, wqkv_ref[...])

    flops = 2 * seqs * rows * (width * (cols * (forward + backward) + inner * backward) + rows * inner * (2 * forward + 5 * backward))
    return seq_call(body, rank, ins, outs, [(rows, width, BF)] if backward else [], flops, after)


def attn_value(rank, base, o_all, wo_all, after=()):
    def body(in_refs, out_refs):
        base_ref, o_ref, w_ref = in_refs
        out_refs[0][...] = base_ref[...] - dot_tn(o_ref[...], w_ref[...])
        return ()

    ins = [("row", base), ("col", o_all), ("all", wo_all)]
    return seq_call(body, rank, ins, [("row", base.shape, F32)], [], 2 * base.size * wo_all.shape[0], after)


def assemble(rank, pieces, after=()):
    rows, width = pieces[0].shape
    half = width // 2

    def kernel(rank_ref, *refs):
        out_ref, token_ref = refs[-2:]
        token_ref[...] = jnp.zeros((8, 128), F32)
        step = pl.program_id(0)
        for place in range(6):

            @pl.when(step == place)
            def _(place=place):
                out_ref[...] = refs[place][...]

        for place in range(2):

            @pl.when(step == 6 + place)
            def _(place=place):
                out_ref[:, :half] = refs[6 + 2 * place][...]
                out_ref[:, half:] = refs[7 + 2 * place][...]

    return pl.pallas_call(
        kernel,
        grid_spec=pltpu.PrefetchScalarGridSpec(
            num_scalar_prefetch=1,
            grid=(8,),
            in_specs=[pl.BlockSpec(piece.shape, lambda g, rk: (0, 0)) for piece in pieces]
            + [pl.BlockSpec(memory_space=pl.ANY)] * len(after),
            out_specs=[
                pl.BlockSpec((None, rows, width), lambda g, rk: (g ^ rk[0], 0, 0)),
                pl.BlockSpec((8, 128), lambda g, rk: (0, 0)),
            ],
        ),
        out_shape=[jax.ShapeDtypeStruct((8, rows, width), F32), jax.ShapeDtypeStruct((8, 128), F32)],
        compiler_params=pltpu.CompilerParams(dimension_semantics=("arbitrary",), vmem_limit_bytes=60 * MIB),
        cost_estimate=pl.CostEstimate(flops=2 * 10**9, bytes_accessed=64 * rows * width, transcendentals=0),
    )(rank, *pieces, *after)


def weight_grads(stacks, layers, layer, jobs, after=()):
    steps = 5
    in_specs, out_specs, out_shape, args, flops, vmem = [], [], [], [], 0, 0
    for left, right, split in jobs:
        tokens, n_cols = right.shape
        if split == "rows":
            n_rows = left.shape[1]
            in_specs.append(pl.BlockSpec((tokens, n_rows // steps), lambda g: (0, g)))
            in_specs.append(pl.BlockSpec((tokens, n_cols), lambda g: (0, 0)))
            out_specs.append(pl.BlockSpec((None, n_rows // steps, n_cols), lambda g: (layer, g, 0)))
        else:
            n_rows = left.shape[0]
            in_specs.append(pl.BlockSpec((n_rows, tokens), lambda g: (0, 0)))
            in_specs.append(pl.BlockSpec((tokens, n_cols // steps), lambda g: (0, g)))
            out_specs.append(pl.BlockSpec((None, n_rows, n_cols // steps), lambda g: (layer, 0, g)))
        out_shape.append(jax.ShapeDtypeStruct((layers, n_rows, n_cols), F32))
        args += [left, right]
        flops += 2 * tokens * n_rows * n_cols
        vmem += 4 * (left.size + right.size) + 2 * n_rows * n_cols
    n_jobs = len(jobs)
    aliases = {}
    if stacks[0] is not None:
        aliases = {len(args) + index: index for index in range(n_jobs)}
        args += stacks
    args += list(after)
    in_specs += [pl.BlockSpec(memory_space=pl.ANY)] * (len(args) - 2 * n_jobs)
    out_specs.append(pl.BlockSpec((8, 128), lambda g: (0, 0)))
    out_shape.append(jax.ShapeDtypeStruct((8, 128), F32))

    def kernel(*refs):
        outs = refs[len(args):]
        for index, (_, _, split) in enumerate(jobs):
            left_ref, right_ref = refs[2 * index:2 * index + 2]
            outs[index][...] = (dot_tn if split == "rows" else dot)(left_ref[...], right_ref[...])
        outs[-1][...] = jnp.zeros((8, 128), F32)

    call = pl.pallas_call(
        kernel,
        grid=(steps,),
        in_specs=in_specs,
        out_specs=out_specs,
        out_shape=out_shape,
        input_output_aliases=aliases,
        compiler_params=pltpu.CompilerParams(dimension_semantics=("arbitrary",), vmem_limit_bytes=60 * MIB),
        cost_estimate=pl.CostEstimate(flops=flops, bytes_accessed=vmem, transcendentals=0),
    )
    *stacks, token = call(*args)
    return stacks, token


def permute(array, bit):
    return lax.ppermute(array, "tp", [(idx, idx ^ bit) for idx in range(8)])


def tie(value, tokens):
    return lax.optimization_barrier((value, *tokens))[0] if tokens else value


def sum_cores(parts):
    halves = []
    for send, keep, order in ((parts[0], parts[2], (2, 4)), (parts[1], parts[3], (4, 2))):
        grid = (2, 2) + keep.shape[1:]
        halves.append((keep.reshape(grid), permute(send, 1).reshape(grid), order))
    return halves


def sum_first(halves, begin=()):
    moving, sent = [], []
    for keep, recv, order in halves:
        recv = tie(recv, begin)
        pick = (lambda arr, pos: arr[:, pos]) if order[0] == 2 else (lambda arr, pos: arr[pos])
        away = pick(keep, 1) + pick(recv, 1)
        sent.append(away)
        moving.append((pick(keep, 0) + pick(recv, 0), permute(away, order[0]), order))
    return moving, sent


def sum_second(moving, fill=()):
    value, sent, final = [], [], []
    for here, recv, order in moving:
        recv = tie(recv, fill)
        sent.append(here[1] + recv[1])
        value.append(here[0] + recv[0])
        final.append(permute(sent[-1], order[1]))
    return value, sent, final


def sum_end(value, final, fill=()):
    halves = [here.astype(F32) + tie(recv, fill).astype(F32) for here, recv in zip(value, final)]
    return jnp.concatenate(halves, axis=-1)[None]


def gather(shard):
    return lax.all_gather(shard, "tp", axis=0, tiled=True)


def spread_first(shard):
    return [permute(shard, bit) for bit in (1, 2, 4)]


def spread_second(near, fill):
    _, near_x, near_y = near
    near_x, near_y = tie(near_x, fill), tie(near_y, fill)
    half = near_x.shape[-1] // 2
    halves = (permute(near_y[:, :half], 2), permute(near_x[:, half:], 4))
    return halves, (permute(near_x, 1), permute(near_y, 1))


def spread_last(shard, near, halves, cross, fill):
    left, right = (tie(half, fill) for half in halves)
    cross_halves = [permute(half, 1) for half in (left, right)]
    return [shard, near[0], near[1], cross[0], near[2], cross[1], left, right, *cross_halves]


def solution(mesh):
    act_spec = P("dp", None, None)
    saved_spec = P(None, "dp", None, None)
    weight_specs = (P(None, None, None, "tp", None), P(None, "tp", None, None), P(None, None, "tp"), P(None, "tp", None))
    grad_specs = (P("dp", None, None, "tp", None), P("dp", "tp", None, None), P("dp", None, "tp"), P("dp", "tp", None))

    def per_device(y_one, y_two, dy_one, dy_two, saved_one, saved_two, w_qkv, w_o, w_in, w_out):
        index = lax.axis_index("tp")
        rank = index.astype(jnp.int32).reshape((1,))
        n_layers, width, _, n_heads, head_dim = w_qkv.shape
        tokens = y_one.shape[0] * y_one.shape[1]
        qkv_w = w_qkv.transpose(0, 2, 3, 4, 1).reshape(n_layers, 3 * n_heads * head_dim, width)
        o_w = w_o.reshape(n_layers, n_heads * head_dim, width)

        def shard(full):
            return lax.dynamic_slice_in_dim(full, index, 1, axis=0)

        def flat(full):
            return full.reshape(tokens, full.shape[-1])

        stacks = {"attn": [None] * 2, "in": [None], "out": [None]}

        def attn_grads(layer, a, o_t, dqkv_t, d_bf, after=()):
            jobs = [(dqkv_t, flat(a), "cols"), (o_t, flat(d_bf), "cols")]
            stacks["attn"], token = weight_grads(stacks["attn"], n_layers, layer, jobs, after)
            return token

        def mlp_grad(which, layer, left, right, after):
            stacks[which], token = weight_grads(
                stacks[which], n_layers, layer, [(flat(left), flat(right), "rows")], after
            )
            return token

        top, hi, lo = 2, 1, 0
        s_one, s_two = saved_one[0], saved_two[0]
        top_a, top_act, top_dh, d_two_bf, *parts, tok = mlp_top(rank, y_one, w_in, w_out, top, dy_two)
        sum_g, sent = sum_first(sum_cores(parts))
        *parts, tok = mlp_out(rank, top_act, w_out, top, [tok, *sent])
        sum_out = sum_cores(parts)
        value, sent, final = sum_second(sum_g, [tok])
        sum_out, sent_out = sum_first(sum_out, sent)
        d_one = shard(dy_one) + rms_vjp(shard(y_one), sum_end(value, final, sent_out))
        rounded, d_one = lax.optimization_barrier((d_one.astype(BF), d_one))
        d_one_bf = gather(rounded)
        s_a, sl_hi, act_hi, sl_lo, act_lo, tok = mlp_pair_fwd(rank, s_one, w_in, hi, lo, [tok, rounded, *sent_out])
        value, sent, final = sum_second(sum_out, [tok])
        *parts, tok = mlp_out(rank, act_lo, w_out, lo, [tok, *sent])
        x_two_top = shard(y_two) - sum_end(value, final, [tok])
        f_top = gather(rms_norm(x_two_top).astype(BF))
        sum_out, sent = sum_first(sum_cores(parts), [x_two_top])
        f_hi, o_hi, dqkv_hi, *parts, tok = attn(
            rank, head_dim, qkv_w, o_w, hi, x=s_two, norm=True, d=d_one_bf, after=[tok, *sent]
        )
        sum_hi, sent = sum_first(sum_cores(parts))
        value_low, sent_low, final_low = sum_second(sum_out, [tok, *sent])
        wo_all = gather(tie(o_w[lo], [f_top]))
        o_top, dqkv_top, *parts, tok = attn(rank, head_dim, qkv_w, o_w, top, x=f_top, d=d_one_bf, after=[tok, *sent, *sent_low])
        x_two = shard(s_two) - sum_end(value_low, final_low, [tok])
        sum_top, sent = sum_first(sum_cores(parts))
        value_hi, sent_hi, final_hi = sum_second(sum_hi, [tok, *sent])
        tok = attn_grads(hi, f_hi, o_hi, dqkv_hi, d_one_bf, [tok, *sent, *sent_hi])
        value, sent, final = sum_second(sum_top, [tok])
        x_two_shard = tie(x_two, sent)[0]
        near = spread_first(x_two_shard)
        d_two = shard(dy_two) + rms_vjp(x_two_top, sum_end(value, final, [x_two_shard]))
        rounded, d_two = lax.optimization_barrier((d_two.astype(BF), d_two))
        d_two_hi_bf = gather(rounded)
        tok = attn_grads(top, f_top, o_top, dqkv_top, d_one_bf, [tok, rounded])
        d_two = d_two + rms_vjp(shard(s_two), sum_end(value_hi, final_hi, [tok]))
        rounded, d_two = lax.optimization_barrier((d_two.astype(BF), d_two))
        d_two_lo_bf = gather(rounded)
        tok = mlp_grad("out", top, top_act, d_two_bf, [tok, rounded])
        far, cross = spread_second(near, [tok])
        tok = mlp_grad("in", top, top_a, top_dh, [tok, near[1], near[2]])
        dh_hi, tok = mlp_dhid(rank, d_two_hi_bf, w_out, hi, sl_hi, [tok, near[1], near[2]])
        pieces = spread_last(x_two_shard, near, far, cross, [tok])
        x_two_full, tok = assemble(rank, pieces, [tok])
        f_lo, o_lo, qkv_lo, tok = attn(rank, head_dim, qkv_w, o_w, lo, x=x_two_full, norm=True, after=[tok])
        o_all = gather(o_lo)
        dh_lo, *parts, tok = mlp_pair_back(rank, d_two_lo_bf, w_out, sl_lo, dh_hi, w_in, hi, lo, [tok])
        sum_g, sent = sum_first(sum_cores(parts))
        tok = mlp_grad("in", lo, s_a, dh_lo, [tok, *sent])
        value, sent, final = sum_second(sum_g, [tok])
        d_one = d_one + rms_vjp(shard(s_one), sum_end(value, final))
        rounded, d_one_shard = lax.optimization_barrier((d_one.astype(BF), d_one[0]))
        d_one_bf = gather(rounded)
        tok = mlp_grad("out", lo, act_lo, d_two_lo_bf, [tok, rounded])
        tok = mlp_grad("in", hi, s_a, dh_hi, [tok])
        tok = mlp_grad("out", hi, act_hi, d_two_hi_bf, [tok])
        d_one_shard = tie(d_one_shard, [d_one_bf])
        near = spread_first(d_one_shard)
        dqkv_lo, *parts, tok = attn(rank, head_dim, qkv_w, o_w, lo, qkv=qkv_lo, d=d_one_bf, after=[tok])
        sum_lo, sent = sum_first(sum_cores(parts))
        tok = attn_grads(lo, f_lo, o_lo, dqkv_lo, d_one_bf, [tok, *sent])
        value, sent, final = sum_second(sum_lo, [tok])
        d_two = d_two + rms_vjp(x_two, sum_end(value, final))
        far, cross = spread_second(near, [tok, *sent])
        x_one_full, tok = attn_value(rank, s_one, o_all, wo_all, [tok, *sent, d_two])
        pieces = spread_last(d_one_shard, near, far, cross, [tok])
        d_one_full, _ = assemble(rank, pieces, [tok])
        grad_qkv = stacks["attn"][0].reshape(n_layers, 3, n_heads, head_dim, width).transpose(0, 4, 1, 2, 3)
        grad_o = stacks["attn"][1].reshape(w_o.shape)
        return (x_one_full, x_two_full, d_one_full, gather(d_two), grad_qkv, grad_o, stacks["in"][0], stacks["out"][0])

    return jax.shard_map(
        per_device,
        mesh=mesh,
        in_specs=(act_spec,) * 4 + (saved_spec,) * 2 + weight_specs,
        out_specs=(act_spec,) * 4 + grad_specs,
        check_vma=False,
    )
```

```python
import jax
import jax.numpy as jnp
from jax import lax
from jax.experimental import pallas as pl
from jax.experimental.pallas import tpu as pltpu
from jax.sharding import PartitionSpec as P

EPS = 1e-6
BF = jnp.bfloat16
F32 = jnp.float32
GELU_C = 0.7978845608028654
GELU_A = 0.044715


def rms_norm(state):
    return state * lax.rsqrt(jnp.mean(state * state, axis=-1, keepdims=True) + EPS)


def rms_vjp(state, cot):
    rinv = lax.rsqrt(jnp.mean(state * state, axis=-1, keepdims=True) + EPS)
    normed = state * rinv
    return rinv * (cot - normed * jnp.mean(cot * normed, axis=-1, keepdims=True))


def dot(left, right, dims=((1,), (0,))):
    return lax.dot_general(left, right, (dims, ((), ())), preferred_element_type=F32)


def dot_nt(left, right):
    return dot(left, right, ((1,), (1,)))


def dot_tn(left, right):
    return dot(left, right, ((0,), (0,)))


def gelu_both(hid):
    sq = hid * hid
    th = jnp.tanh(GELU_C * (hid + GELU_A * (sq * hid)))
    cdf = 0.5 * (1.0 + th)
    return hid * cdf, cdf + hid * (0.5 * (1.0 - th * th)) * (GELU_C * (1.0 + 3.0 * GELU_A * sq))


MIB = 1024 * 1024


def seq_call(body, rank, ins, outs, parts, flops, after=()):
    n_in, n_out = len(ins), len(outs)
    seqs = 8

    def run(parity, previous, after):
        steps = seqs if parity is None else seqs // 2

        def seq(g, rk):
            return g if parity is None else (2 * g + parity) ^ rk[0]

        def spec(kind, shape, layer=0):
            if kind == "row":
                return pl.BlockSpec((None,) + tuple(shape[1:]), lambda g, rk: (seq(g, rk), 0, 0))
            if kind == "col":
                return pl.BlockSpec((shape[0], shape[1] // seqs), lambda g, rk: (0, seq(g, rk)))
            if kind == "layer":
                return pl.BlockSpec((None,) + tuple(shape[1:]), lambda g, rk: (layer, 0, 0))
            if kind == "tail":
                return pl.BlockSpec((shape[0], layer), lambda g, rk: (0, shape[1] // layer - seqs + seq(g, rk)))
            return pl.BlockSpec((shape[0], layer), lambda g, rk: (0, 0))

        hidden = list(previous) + list(after)
        in_specs = [spec(kind, arr.shape, *layer) for kind, arr, *layer in ins] + [pl.BlockSpec(memory_space=pl.ANY)] * len(hidden)
        out_specs = [spec(kind, shape) for kind, shape, _ in outs]
        out_shape = [jax.ShapeDtypeStruct(shape, dtype) for _, shape, dtype in outs]
        for rows, width, dtype in parts:
            for _ in range(2):
                out_specs.append(pl.BlockSpec((None, rows, width // 2), lambda g, rk: (g, 0, 0)))
                out_shape.append(jax.ShapeDtypeStruct((steps, rows, width // 2), dtype))

        out_specs.append(pl.BlockSpec((8, 128), lambda g, rk: (0, 0)))
        out_shape.append(jax.ShapeDtypeStruct((8, 128), F32))

        def kernel(rank_ref, *refs):
            refs[-1][...] = jnp.zeros((8, 128), F32)
            in_refs = refs[:n_in]
            out_refs = refs[n_in + len(hidden):n_in + len(hidden) + n_out]
            part_refs = refs[n_in + len(hidden) + n_out:]
            for index, value in enumerate(body(in_refs, out_refs)):
                left, right = part_refs[2 * index:2 * index + 2]
                half = value.shape[-1] // 2
                left[...] = value[:, :half].astype(left.dtype)
                right[...] = value[:, half:].astype(right.dtype)

        share = 1 if parity is None else 2
        nbytes = sum(o.size * o.dtype.itemsize for o in out_shape) // share
        return pl.pallas_call(
        kernel,
        grid_spec=pltpu.PrefetchScalarGridSpec(
            num_scalar_prefetch=1, grid=(steps,), in_specs=in_specs, out_specs=out_specs
        ),
        out_shape=out_shape,
        input_output_aliases={1 + n_in + index: index for index in range(len(previous))},
        compiler_params=pltpu.CompilerParams(dimension_semantics=("arbitrary",), vmem_limit_bytes=60 * MIB),
        cost_estimate=pl.CostEstimate(flops=flops // share, bytes_accessed=nbytes, transcendentals=0),
        )(rank, *[arr for _, arr, *_ in ins], *hidden)

    if not parts:
        return list(run(None, (), after))
    sent = list(run(1, (), after))
    kept = list(run(0, sent[:n_out], [sent[-1]]))
    return kept[:n_out] + [sent[n_out], sent[n_out + 1], kept[n_out], kept[n_out + 1], kept[-1]]


def mlp_top(rank, x, w_in, w_out, layer, d):
    seqs, rows, width = x.shape
    inner = w_in.shape[2]

    def body(in_refs, out_refs):
        x_ref, win_ref, wout_ref, d_ref = in_refs
        a_ref, act_ref, dh_ref, dbf_ref = out_refs
        a = rms_norm(x_ref[...]).astype(BF)
        a_ref[...] = a
        d_bf = d_ref[...].astype(BF)
        dbf_ref[...] = d_bf
        act, slope = gelu_both(dot(a, win_ref[...]))
        act_ref[...] = act.astype(BF)
        dh = (dot_nt(d_bf, wout_ref[...]) * slope).astype(BF)
        dh_ref[...] = dh
        yield dot_nt(dh, win_ref[...])

    mid = (seqs, rows, inner)
    outs = [("row", x.shape, BF), ("row", mid, BF), ("row", mid, BF), ("row", d.shape, BF)]
    ins = [("row", x), ("layer", w_in, layer), ("layer", w_out, layer), ("row", d)]
    return seq_call(body, rank, ins, outs, [(rows, width, BF)], 6 * seqs * rows * width * inner)


def mlp_out(rank, act, w_out, layer, after=()):
    rows, width = act.shape[1], w_out.shape[2]

    def body(in_refs, out_refs):
        yield dot(in_refs[0][...], in_refs[1][...])

    return seq_call(body, rank, [("row", act), ("layer", w_out, layer)], [], [(rows, width, F32)], 2 * act.size * width, after)


def mlp_pair_fwd(rank, x, w_in, hi, lo, after=()):
    seqs, rows, width = x.shape
    inner = w_in.shape[2]

    def body(in_refs, out_refs):
        x_ref, whi_ref, wlo_ref = in_refs
        a_ref, shi_ref, acthi_ref, slo_ref, actlo_ref = out_refs
        a = rms_norm(x_ref[...]).astype(BF)
        a_ref[...] = a
        for w_ref, slope_ref, act_ref in ((wlo_ref, slo_ref, actlo_ref), (whi_ref, shi_ref, acthi_ref)):
            hid = dot(a, w_ref[...])
            act, slope_ref[...] = gelu_both(hid)
            act_ref[...] = act.astype(BF)
        return ()

    mid = (seqs, rows, inner)
    outs = [("row", x.shape, BF), ("row", mid, F32), ("row", mid, BF), ("row", mid, F32), ("row", mid, BF)]
    ins = [("row", x), ("layer", w_in, hi), ("layer", w_in, lo)]
    return seq_call(body, rank, ins, outs, [], 4 * seqs * rows * width * inner, after)


def mlp_dhid(rank, d, w_out, layer, slope, after=()):
    seqs, rows, width = d.shape
    inner = w_out.shape[1]

    def body(in_refs, out_refs):
        d_ref, w_ref, slope_ref = in_refs
        out_refs[0][...] = (dot_nt(d_ref[...], w_ref[...]) * slope_ref[...]).astype(BF)
        return ()

    ins = [("row", d), ("layer", w_out, layer), ("row", slope)]
    return seq_call(body, rank, ins, [("row", slope.shape, BF)], [], 2 * seqs * rows * width * inner, after)


def mlp_pair_back(rank, d, w_out, slope, dh_hi, w_in, hi, lo, after=()):
    seqs, rows, width = d.shape
    inner = w_out.shape[1]

    def body(in_refs, out_refs):
        d_ref, w_ref, slope_ref, dshi_ref, whi_ref, wlo_ref = in_refs
        dh = (dot_nt(d_ref[...], w_ref[...]) * slope_ref[...]).astype(BF)
        out_refs[0][...] = dh
        yield dot_nt(dshi_ref[...], whi_ref[...]) + dot_nt(dh, wlo_ref[...])

    ins = [("row", d), ("layer", w_out, lo), ("row", slope), ("row", dh_hi), ("layer", w_in, hi), ("layer", w_in, lo)]
    return seq_call(body, rank, ins, [("row", slope.shape, BF)], [(rows, width, BF)], 6 * seqs * rows * width * inner, after)


def attn(rank, head_dim, w_qkv, w_o, layer, x=None, minus=None, norm=False, qkv=None, d=None, after=()):
    seqs, rows, width = (x if x is not None else d).shape
    cols, inner = w_qkv.shape[1], w_o.shape[1]
    heads = inner // head_dim
    scale = head_dim ** -0.5
    forward, backward = x is not None, d is not None
    ins, outs = [("layer", w_qkv, layer)], []
    if forward:
        ins.append(("row", x))
        if minus is not None:
            ins.append(("row", minus))
            outs.append(("row", x.shape, F32))
        if norm:
            outs.append(("row", x.shape, BF))
        outs.append(("col", (inner, seqs * rows), BF))
        if not backward:
            outs.append(("col", (cols, seqs * rows), BF))
    else:
        ins.append(("col", qkv))
    if backward:
        ins += [("layer", w_o, layer), ("row", d)]
        outs.append(("col", (cols, seqs * rows), BF))

    def body(in_refs, out_refs):
        in_refs, out_refs = list(in_refs), list(out_refs)
        wqkv_ref = in_refs.pop(0)
        if forward:
            value = in_refs.pop(0)[...]
            if minus is not None:
                value = value - in_refs.pop(0)[...]
                out_refs.pop(0)[...] = value
            if norm:
                value = rms_norm(value).astype(BF)
                out_refs.pop(0)[...] = value
            o_ref = out_refs.pop(0)
            qkv_t = dot_nt(wqkv_ref[...], value).astype(BF)
            if not backward:
                out_refs.pop(0)[...] = qkv_t
        else:
            qkv_t = in_refs.pop(0)[...]
        if backward:
            wo_ref, d_ref = in_refs
            dqkv_ref = out_refs.pop(0)
            dheads = dot_nt(wo_ref[...], d_ref[...]).astype(BF)
        pieces = [[], [], []]
        for n in range(heads):
            lo = n * head_dim
            q_t, k_t, v_t = (qkv_t[part * inner + lo:part * inner + lo + head_dim] for part in range(3))
            scores = dot_tn(k_t, q_t) * scale
            expd = jnp.exp(scores - jnp.max(scores, axis=0, keepdims=True))
            probs = expd / jnp.sum(expd, axis=0, keepdims=True)
            probs_bf = probs.astype(BF)
            if forward:
                o_ref[pl.ds(lo, head_dim), :] = dot(v_t, probs_bf).astype(BF)
            if backward:
                dhead = dheads[lo:lo + head_dim]
                d_v = dot_nt(dhead, probs_bf)
                d_probs = dot_tn(v_t, dhead)
                d_scores = (probs * (d_probs - jnp.sum(d_probs * probs, axis=0, keepdims=True)) * scale).astype(BF)
                for part, piece in enumerate((dot(k_t, d_scores), dot_nt(q_t, d_scores), d_v)):
                    pieces[part].append(piece.astype(BF))
        if backward:
            dqkv = jnp.concatenate(pieces[0] + pieces[1] + pieces[2], axis=0)
            dqkv_ref[...] = dqkv
            yield dot_tn(dqkv, wqkv_ref[...])

    flops = 2 * seqs * rows * (width * (cols * (forward + backward) + inner * backward) + rows * inner * (2 * forward + 5 * backward))
    return seq_call(body, rank, ins, outs, [(rows, width, BF)] if backward else [], flops, after)


def attn_value(rank, base, both, after=()):
    _, rows, width = base.shape

    def body(in_refs, out_refs):
        base_ref, w_ref, o_ref = in_refs
        out_refs[0][...] = base_ref[...] - dot_tn(o_ref[...], w_ref[...])
        return ()

    ins = [("row", base), ("head", both, width), ("tail", both, rows)]
    return seq_call(body, rank, ins, [("row", base.shape, F32)], [], 2 * base.size * both.shape[0], after)


def assemble(rank, pieces, after=()):
    rows, width = pieces[0].shape
    half = width // 2

    def kernel(rank_ref, *refs):
        out_ref, token_ref = refs[-2:]
        token_ref[...] = jnp.zeros((8, 128), F32)
        step = pl.program_id(0)
        for place in range(6):

            @pl.when(step == place)
            def _(place=place):
                out_ref[...] = refs[place][...]

        for place in range(2):

            @pl.when(step == 6 + place)
            def _(place=place):
                out_ref[:, :half] = refs[6 + 2 * place][...]
                out_ref[:, half:] = refs[7 + 2 * place][...]

    return pl.pallas_call(
        kernel,
        grid_spec=pltpu.PrefetchScalarGridSpec(
            num_scalar_prefetch=1,
            grid=(8,),
            in_specs=[pl.BlockSpec(piece.shape, lambda g, rk: (0, 0)) for piece in pieces]
            + [pl.BlockSpec(memory_space=pl.ANY)] * len(after),
            out_specs=[
                pl.BlockSpec((None, rows, width), lambda g, rk: (g ^ rk[0], 0, 0)),
                pl.BlockSpec((8, 128), lambda g, rk: (0, 0)),
            ],
        ),
        out_shape=[jax.ShapeDtypeStruct((8, rows, width), F32), jax.ShapeDtypeStruct((8, 128), F32)],
        compiler_params=pltpu.CompilerParams(dimension_semantics=("arbitrary",), vmem_limit_bytes=60 * MIB),
        cost_estimate=pl.CostEstimate(flops=2 * 10**9, bytes_accessed=64 * rows * width, transcendentals=0),
    )(rank, *pieces, *after)


def weight_grads(stacks, layers, layer, jobs, after=()):
    steps = 5
    in_specs, out_specs, out_shape, args, flops, vmem = [], [], [], [], 0, 0
    for left, right, split in jobs:
        tokens, n_cols = right.shape
        if split == "rows":
            n_rows = left.shape[1]
            in_specs.append(pl.BlockSpec((tokens, n_rows // steps), lambda g: (0, g)))
            in_specs.append(pl.BlockSpec((tokens, n_cols), lambda g: (0, 0)))
            out_specs.append(pl.BlockSpec((None, n_rows // steps, n_cols), lambda g: (layer, g, 0)))
        else:
            n_rows = left.shape[0]
            in_specs.append(pl.BlockSpec((n_rows, tokens), lambda g: (0, 0)))
            in_specs.append(pl.BlockSpec((tokens, n_cols // steps), lambda g: (0, g)))
            out_specs.append(pl.BlockSpec((None, n_rows, n_cols // steps), lambda g: (layer, 0, g)))
        out_shape.append(jax.ShapeDtypeStruct((layers, n_rows, n_cols), F32))
        args += [left, right]
        flops += 2 * tokens * n_rows * n_cols
        vmem += 4 * (left.size + right.size) + 2 * n_rows * n_cols
    n_jobs = len(jobs)
    aliases = {}
    if stacks[0] is not None:
        aliases = {len(args) + index: index for index in range(n_jobs)}
        args += stacks
    args += list(after)
    in_specs += [pl.BlockSpec(memory_space=pl.ANY)] * (len(args) - 2 * n_jobs)
    out_specs.append(pl.BlockSpec((8, 128), lambda g: (0, 0)))
    out_shape.append(jax.ShapeDtypeStruct((8, 128), F32))

    def kernel(*refs):
        outs = refs[len(args):]
        for index, (_, _, split) in enumerate(jobs):
            left_ref, right_ref = refs[2 * index:2 * index + 2]
            outs[index][...] = (dot_tn if split == "rows" else dot)(left_ref[...], right_ref[...])
        outs[-1][...] = jnp.zeros((8, 128), F32)

    call = pl.pallas_call(
        kernel,
        grid=(steps,),
        in_specs=in_specs,
        out_specs=out_specs,
        out_shape=out_shape,
        input_output_aliases=aliases,
        compiler_params=pltpu.CompilerParams(dimension_semantics=("arbitrary",), vmem_limit_bytes=60 * MIB),
        cost_estimate=pl.CostEstimate(flops=flops, bytes_accessed=vmem, transcendentals=0),
    )
    *stacks, token = call(*args)
    return stacks, token


def permute(array, bit):
    return lax.ppermute(array, "tp", [(idx, idx ^ bit) for idx in range(8)])


def tie(value, tokens):
    return lax.optimization_barrier((value, *tokens))[0] if tokens else value


def sum_cores(parts):
    halves = []
    for send, keep, order in ((parts[0], parts[2], (2, 4)), (parts[1], parts[3], (4, 2))):
        grid = (2, 2) + keep.shape[1:]
        halves.append((keep.reshape(grid), permute(send, 1).reshape(grid), order))
    return halves


def sum_first(halves, begin=()):
    moving, sent = [], []
    for keep, recv, order in halves:
        recv = tie(recv, begin)
        pick = (lambda arr, pos: arr[:, pos]) if order[0] == 2 else (lambda arr, pos: arr[pos])
        away = pick(keep, 1) + pick(recv, 1)
        sent.append(away)
        moving.append((pick(keep, 0) + pick(recv, 0), permute(away, order[0]), order))
    return moving, sent


def sum_second(moving, fill=()):
    value, sent, final = [], [], []
    for here, recv, order in moving:
        recv = tie(recv, fill)
        sent.append(here[1] + recv[1])
        value.append(here[0] + recv[0])
        final.append(permute(sent[-1], order[1]))
    return value, sent, final


def sum_end(value, final, fill=()):
    halves = [here.astype(F32) + tie(recv, fill).astype(F32) for here, recv in zip(value, final)]
    return jnp.concatenate(halves, axis=-1)[None]


def gather(shard):
    return lax.all_gather(shard, "tp", axis=0, tiled=True)


def spread_first(shard):
    return [permute(shard, bit) for bit in (1, 2, 4)]


def spread_second(near, fill):
    _, near_x, near_y = near
    near_x, near_y = tie(near_x, fill), tie(near_y, fill)
    half = near_x.shape[-1] // 2
    halves = (permute(near_y[:, :half], 2), permute(near_x[:, half:], 4))
    return halves, (permute(near_x, 1), permute(near_y, 1))


def spread_last(shard, near, halves, cross, fill):
    left, right = (tie(half, fill) for half in halves)
    cross_halves = [permute(half, 1) for half in (left, right)]
    return [shard, near[0], near[1], cross[0], near[2], cross[1], left, right, *cross_halves]


def solution(mesh):
    act_spec = P("dp", None, None)
    saved_spec = P(None, "dp", None, None)
    weight_specs = (P(None, None, None, "tp", None), P(None, "tp", None, None), P(None, None, "tp"), P(None, "tp", None))
    grad_specs = (P("dp", None, None, "tp", None), P("dp", "tp", None, None), P("dp", None, "tp"), P("dp", "tp", None))

    def per_device(y_one, y_two, dy_one, dy_two, saved_one, saved_two, w_qkv, w_o, w_in, w_out):
        index = lax.axis_index("tp")
        rank = index.astype(jnp.int32).reshape((1,))
        n_layers, width, _, n_heads, head_dim = w_qkv.shape
        tokens = y_one.shape[0] * y_one.shape[1]
        qkv_w = w_qkv.transpose(0, 2, 3, 4, 1).reshape(n_layers, 3 * n_heads * head_dim, width)
        o_w = w_o.reshape(n_layers, n_heads * head_dim, width)

        def shard(full):
            return lax.dynamic_slice_in_dim(full, index, 1, axis=0)

        def flat(full):
            return full.reshape(tokens, full.shape[-1])

        stacks = {"attn": [None] * 2, "in": [None], "out": [None]}

        def attn_grads(layer, a, o_t, dqkv_t, d_bf, after=()):
            jobs = [(dqkv_t, flat(a), "cols"), (o_t, flat(d_bf), "cols")]
            stacks["attn"], token = weight_grads(stacks["attn"], n_layers, layer, jobs, after)
            return token

        def mlp_grad(which, layer, left, right, after):
            stacks[which], token = weight_grads(
                stacks[which], n_layers, layer, [(flat(left), flat(right), "rows")], after
            )
            return token

        top, hi, lo = 2, 1, 0
        s_one, s_two = saved_one[0], saved_two[0]
        top_a, top_act, top_dh, d_two_bf, *parts, tok = mlp_top(rank, y_one, w_in, w_out, top, dy_two)
        sum_g, sent = sum_first(sum_cores(parts))
        *parts, tok = mlp_out(rank, top_act, w_out, top, [tok, *sent])
        sum_out = sum_cores(parts)
        value, sent, final = sum_second(sum_g, [tok])
        sum_out, sent_out = sum_first(sum_out, sent)
        d_one = shard(dy_one) + rms_vjp(shard(y_one), sum_end(value, final, sent_out))
        rounded, d_one = lax.optimization_barrier((d_one.astype(BF), d_one))
        d_one_bf = gather(rounded)
        s_a, sl_hi, act_hi, sl_lo, act_lo, tok = mlp_pair_fwd(rank, s_one, w_in, hi, lo, [tok, rounded, *sent_out])
        value, sent, final = sum_second(sum_out, [tok])
        *parts, tok = mlp_out(rank, act_lo, w_out, lo, [tok, *sent])
        x_two_top = shard(y_two) - sum_end(value, final, [tok])
        f_top = gather(rms_norm(x_two_top).astype(BF))
        sum_out, sent = sum_first(sum_cores(parts), [x_two_top])
        f_hi, o_hi, dqkv_hi, *parts, tok = attn(
            rank, head_dim, qkv_w, o_w, hi, x=s_two, norm=True, d=d_one_bf, after=[tok, *sent]
        )
        sum_hi, sent = sum_first(sum_cores(parts))
        value_low, sent_low, final_low = sum_second(sum_out, [tok, *sent])
        o_top, dqkv_top, *parts, tok = attn(rank, head_dim, qkv_w, o_w, top, x=f_top, d=d_one_bf, after=[tok, *sent, *sent_low])
        x_two = shard(s_two) - sum_end(value_low, final_low, [tok])
        sum_top, sent = sum_first(sum_cores(parts))
        value_hi, sent_hi, final_hi = sum_second(sum_hi, [tok, *sent])
        tok = attn_grads(hi, f_hi, o_hi, dqkv_hi, d_one_bf, [tok, *sent, *sent_hi])
        value, sent, final = sum_second(sum_top, [tok])
        x_two_shard = tie(x_two, sent)[0]
        near = spread_first(x_two_shard)
        d_two = shard(dy_two) + rms_vjp(x_two_top, sum_end(value, final, [x_two_shard]))
        rounded, d_two = lax.optimization_barrier((d_two.astype(BF), d_two))
        d_two_hi_bf = gather(rounded)
        tok = attn_grads(top, f_top, o_top, dqkv_top, d_one_bf, [tok, rounded])
        d_two = d_two + rms_vjp(shard(s_two), sum_end(value_hi, final_hi, [tok]))
        rounded, d_two = lax.optimization_barrier((d_two.astype(BF), d_two))
        d_two_lo_bf = gather(rounded)
        tok = mlp_grad("out", top, top_act, d_two_bf, [tok, rounded])
        far, cross = spread_second(near, [tok])
        tok = mlp_grad("in", top, top_a, top_dh, [tok, near[1], near[2]])
        dh_hi, tok = mlp_dhid(rank, d_two_hi_bf, w_out, hi, sl_hi, [tok, near[1], near[2]])
        pieces = spread_last(x_two_shard, near, far, cross, [tok])
        x_two_full, tok = assemble(rank, pieces, [tok])
        f_lo, o_lo, qkv_lo, tok = attn(rank, head_dim, qkv_w, o_w, lo, x=x_two_full, norm=True, after=[tok])
        both = gather(jnp.concatenate([o_w[lo], o_lo], axis=1))
        dh_lo, *parts, tok = mlp_pair_back(rank, d_two_lo_bf, w_out, sl_lo, dh_hi, w_in, hi, lo, [tok])
        sum_g, sent = sum_first(sum_cores(parts))
        tok = mlp_grad("in", lo, s_a, dh_lo, [tok, *sent])
        value, sent, final = sum_second(sum_g, [tok])
        d_one = d_one + rms_vjp(shard(s_one), sum_end(value, final))
        rounded, d_one_shard = lax.optimization_barrier((d_one.astype(BF), d_one[0]))
        d_one_bf = gather(rounded)
        tok = mlp_grad("out", lo, act_lo, d_two_lo_bf, [tok, rounded])
        tok = mlp_grad("in", hi, s_a, dh_hi, [tok])
        tok = mlp_grad("out", hi, act_hi, d_two_hi_bf, [tok])
        d_one_shard = tie(d_one_shard, [d_one_bf])
        near = spread_first(d_one_shard)
        dqkv_lo, *parts, tok = attn(rank, head_dim, qkv_w, o_w, lo, qkv=qkv_lo, d=d_one_bf, after=[tok])
        sum_lo, sent = sum_first(sum_cores(parts))
        tok = attn_grads(lo, f_lo, o_lo, dqkv_lo, d_one_bf, [tok, *sent])
        value, sent, final = sum_second(sum_lo, [tok])
        d_two = d_two + rms_vjp(x_two, sum_end(value, final))
        far, cross = spread_second(near, [tok, *sent])
        x_one_full, tok = attn_value(rank, s_one, both, [tok, *sent, d_two])
        pieces = spread_last(d_one_shard, near, far, cross, [tok])
        d_one_full, _ = assemble(rank, pieces, [tok])
        grad_qkv = stacks["attn"][0].reshape(n_layers, 3, n_heads, head_dim, width).transpose(0, 4, 1, 2, 3)
        grad_o = stacks["attn"][1].reshape(w_o.shape)
        return (x_one_full, x_two_full, d_one_full, gather(d_two), grad_qkv, grad_o, stacks["in"][0], stacks["out"][0])

    return jax.shard_map(
        per_device,
        mesh=mesh,
        in_specs=(act_spec,) * 4 + (saved_spec,) * 2 + weight_specs,
        out_specs=(act_spec,) * 4 + grad_specs,
        check_vma=False,
    )
```
